512 devices in a mesh: inter: 64 (over y, z_hi, core), intra: 8 (over x, z_lo).
Axes of the slice: x: 4, y: 8, z: 8 (z_hi: 4, z_lo: 2; z = z_hi * 2 + z_lo), core: 2. Of those that a mesh axis runs over, the one named last changes fastest.
Arguments:
- hidden_in: bfloat16 [64, 1024, 4096], P('inter', 'intra'), may hold values from -120 to 120, as said below
- norm_gain: bfloat16 [4096], P(('inter', 'intra')), may hold values from 0.5 to 2, as said below
- qkv_weight: bfloat16 [4096, 768], P(('inter', 'intra')), may hold values from -0.09375 to 0.09375
- attn_cotangent: bfloat16 [64, 1024, 512], P('inter', 'intra'), may hold values from -6 to 6
Outputs:
- attn: bfloat16 [64, 1024, 512], P('inter', 'intra')
- grad_in: bfloat16 [64, 1024, 4096], P('inter', 'intra')
- weight_grad: float32 [4096, 768], P(('intra', 'inter'))
- gain_grad: float32 [4096], P(('intra', 'inter'))
The draws below stay inside these ranges and needn't reach their ends.
Inputs may be any that keep to these rules, and one draw needn't show every extreme that they name: `hidden_in`: activations with spread row and feature scales. `norm_gain`: positive gains.
All inputs are finite; a program needn't handle non-finite values.
Results may differ from the reference program's by a relative error of at most 0.015.
Values may be sent and summed in bfloat16 or wider, within the bound.
A program may use at most 64 MiB of HBM per device.

```python
import math
import jax
import jax.numpy as jnp
from jax import lax

D = 4096
HD = 128
HEADS = 4
SEQ = 1024
SEQS = 64


def draw_hidden_in(key, part):
    key_base, key_rows, key_cols = jax.random.split(jax.random.fold_in(key, 11), 3)
    shape = (SEQS, SEQ, D)
    row_scale = jnp.exp(jax.random.uniform(key_rows, (SEQS, SEQ, 1), minval=0.0, maxval=math.log(10.0)))
    col_scale = jnp.exp(jax.random.uniform(key_cols, (1, 1, D), minval=math.log(0.5), maxval=math.log(3.0)))
    base = jnp.clip(jax.random.normal(key_base, shape), -4.0, 4.0)
    return (base * row_scale * col_scale).astype(jnp.bfloat16)


def draw_norm_gain(key, part):
    key_gain = jax.random.fold_in(key, 23)
    values_out = jnp.exp(jax.random.uniform(key_gain, (D,), minval=math.log(0.5), maxval=math.log(2.0)))
    return values_out.astype(jnp.bfloat16)


def block_scale(key, shape, cuts, least, high):
    loudness, own = 1.0, jax.random.fold_in(key, 6)
    for position, blocks in cuts:
        draws = jnp.exp(jax.random.uniform(jax.random.fold_in(own, position), (blocks,), jnp.float32, least / len(cuts), high / len(cuts)))
        loudness = loudness * jnp.repeat(draws, shape[position] // blocks).reshape([-1 if axis == position else 1 for axis in range(len(shape))])
    return loudness


def centred(stream_key, extent, width, bound, pieces=(), held_as=jnp.bfloat16):
    entries = width * jax.random.normal(stream_key, extent, jnp.float32)
    if pieces:
        entries = entries * block_scale(stream_key, extent, pieces, -0.22, 0.18)
    return jnp.clip(entries, -bound, bound).astype(held_as)


def setup_inputs(seed: int = 0) -> dict:
    arg_keys = jax.random.split(jax.random.key(seed), 5)
    return {
        "hidden_in": draw_hidden_in(jax.random.fold_in(arg_keys[4], 71), 0),
        "norm_gain": draw_norm_gain(jax.random.fold_in(arg_keys[4], 71), 0),
        "qkv_weight": centred(arg_keys[2], (D, (HEADS + 2) * HD), D ** -0.5, 0.09375, ((0, 512),)),
        "attn_cotangent": centred(arg_keys[3], (SEQS, SEQ, HEADS * HD), 1.0, 6.0, ((0, 64), (1, 8))),
    }


eps_norm = 1e-05
rope_base = 500000.0

def rope_tables(positions, head_size):
    half_size = head_size // 2
    freqs = rope_base ** (-jnp.arange(half_size, dtype=jnp.float32) / half_size)
    angles = positions.astype(jnp.float32)[:, None] * freqs[None, :]
    return (jnp.cos(angles), jnp.sin(angles))

def rotate(values_in, cosine, sine):
    half_size = values_in.shape[-1] // 2
    first, second = (values_in[..., :half_size], values_in[..., half_size:])
    return jnp.concatenate([first * cosine - second * sine, second * cosine + first * sine], axis=-1)

def unrotate(grad_out, cosine, sine):
    half_size = grad_out.shape[-1] // 2
    first, second = (grad_out[..., :half_size], grad_out[..., half_size:])
    return jnp.concatenate([first * cosine + second * sine, second * cosine - first * sine], axis=-1)

def reference(hidden_in, norm_gain, qkv_weight, attn_cotangent):
    gain = norm_gain.astype(jnp.float32)
    positions = jnp.arange(SEQ, dtype=jnp.int32)
    cosine, sine = rope_tables(positions, HD)
    row_pos = jnp.arange(SEQ * HEADS, dtype=jnp.int32) // HEADS
    allowed = positions[None, :] <= row_pos[:, None]
    scale = HD ** (-0.5)
    qcols = HEADS * HD

    def one_sequence(carry, items):
        weight_acc, gain_acc = carry
        rows_in, grad_attn = items
        wide_rows = rows_in.astype(jnp.float32)
        inv_rms = lax.rsqrt(lax.optimization_barrier(jnp.mean(wide_rows * wide_rows, axis=1, keepdims=True)) + eps_norm)
        normed = (wide_rows * inv_rms * gain[None, :]).astype(jnp.bfloat16)
        mixed = jnp.dot(normed, qkv_weight, preferred_element_type=jnp.float32)
        query = (rotate(mixed[:, :qcols].reshape(SEQ, HEADS, HD), cosine[:, None, :], sine[:, None, :]) * scale).astype(jnp.bfloat16).reshape(SEQ * HEADS, HD)
        key_rows = rotate(mixed[:, qcols:qcols + HD], cosine, sine).astype(jnp.bfloat16)
        value_rows = mixed[:, qcols + HD:].astype(jnp.bfloat16)
        grad_flat = grad_attn.reshape(SEQ * HEADS, HD)
        scores = jnp.dot(query, key_rows.T, preferred_element_type=jnp.float32)
        scores = jnp.where(allowed, scores, -1e+30)
        row_top = lax.optimization_barrier(jnp.max(scores, axis=1))
        row_total = lax.optimization_barrier(jnp.sum(jnp.where(allowed, jnp.exp(scores - row_top[:, None]), 0.0), axis=1))
        log_total = row_top + jnp.log(row_total)
        probs = jnp.where(allowed, jnp.exp(scores - log_total[:, None]), 0.0)
        probs_low = probs.astype(jnp.bfloat16)
        attn_flat = jnp.dot(probs, value_rows.astype(jnp.float32), precision=lax.Precision.HIGHEST, preferred_element_type=jnp.float32).astype(jnp.bfloat16)
        row_delta = lax.optimization_barrier(jnp.sum(grad_flat.astype(jnp.float32) * attn_flat.astype(jnp.float32), axis=1))
        grad_probs = jnp.dot(grad_flat, value_rows.T, preferred_element_type=jnp.float32)
        grad_scores = (probs * (grad_probs - row_delta[:, None])).astype(jnp.bfloat16)
        grad_query = jnp.dot(grad_scores, key_rows, preferred_element_type=jnp.float32)
        grad_keys = jnp.dot(grad_scores.T, query, preferred_element_type=jnp.float32)
        grad_values = jnp.dot(probs_low.T, grad_flat, preferred_element_type=jnp.float32)
        query_back = (unrotate(grad_query.reshape(SEQ, HEADS, HD), cosine[:, None, :], sine[:, None, :]) * scale).reshape(SEQ, qcols)
        grad_mixed = jnp.concatenate([query_back, unrotate(grad_keys, cosine, sine), grad_values], axis=1).astype(jnp.bfloat16)
        grad_normed = jnp.dot(grad_mixed, qkv_weight.T, preferred_element_type=jnp.float32)
        inner = lax.optimization_barrier(jnp.sum(grad_normed * gain[None, :] * wide_rows, axis=1, keepdims=True))
        grad_rows = (gain[None, :] * grad_normed * inv_rms - wide_rows * inv_rms ** 3 / D * inner).astype(jnp.bfloat16)
        gain_acc = gain_acc + lax.optimization_barrier(jnp.sum(grad_normed * wide_rows * inv_rms, axis=0))
        term_low = jnp.dot(normed.T, grad_mixed, preferred_element_type=jnp.float32).astype(jnp.bfloat16)
        term_low = lax.optimization_barrier(term_low)
        weight_acc = weight_acc + term_low.astype(jnp.float32)
        return ((weight_acc, gain_acc), (attn_flat.reshape(SEQ, qcols), grad_rows))
    start = (jnp.zeros((D, (HEADS + 2) * HD), jnp.float32), jnp.zeros((D,), jnp.float32))
    (weight_grad, gain_grad), (attn, grad_in) = lax.scan(one_sequence, start, (hidden_in, attn_cotangent))
    return (attn, grad_in, weight_grad, gain_grad)
```

```python
import functools
import math

import jax
import jax.numpy as jnp
from jax import lax
from jax.experimental import pallas as pl
from jax.experimental.pallas import tpu as pltpu
from jax.sharding import PartitionSpec as P

HD = 128
HEADS = 4
TILES = HEADS + 2
MESH = pl.DeviceIdType.MESH
SIZES = {"x": 4, "y": 8, "z": 8}
ORDERS = (("z", "y", "x"), ("x", "z", "y"), ("y", "x", "z"))
HALVES = 2

eps_norm = 1e-05
rope_base = 500000.0


def place():
    i, j = lax.axis_index("inter"), lax.axis_index("intra")
    return {"x": j // 2, "y": i // 8, "z": ((i // 2) % 4) * 2 + j % 2}, i % 2


def device(at, core):
    return ((at["y"] * 4 + at["z"] // 2) * 2 + core, at["x"] * 2 + at["z"] % 2)


def moved(at, dim, step):
    size = SIZES[dim]
    return {**at, dim: (at[dim] + step + size) % size}


def slab(ref, tile, at, cores=slice(None)):
    every = slice(None)
    y, x = at.get("y", every), at.get("x", every)
    high, low = (at["z"] // 2, at["z"] % 2) if "z" in at else (every, every)
    return ref.at[tile, y, high, cores, x, low]


def enter(at, core, barrier):
    peers = [device(at, 1 - core)]
    for dim, size in SIZES.items():
        peers += [device(moved(at, dim, step), core) for step in range(1, size)]
    for peer in peers:
        pl.semaphore_signal(barrier, inc=1, device_id=peer, device_id_type=MESH)
    pl.semaphore_wait(barrier, len(peers))


def gather_kernel(
    mine_ref, full_ref, swap_send, swap_recv, send_1, recv_1, send_2, recv_2, ring_send, ring_recv, pass_send, pass_recv, own_sem
):
    at, core = place()
    partner = device(at, 1 - core)
    enter(at, core, pltpu.get_barrier_semaphore())

    def remote(src, dst, send, recv, peer):
        return pltpu.make_async_remote_copy(
            src_ref=src, dst_ref=dst, send_sem=send, recv_sem=recv, device_id=peer, device_id_type=MESH
        )

    mine = [3 * core + p for p in range(3)]
    theirs = [3 * (1 - core) + p for p in range(3)]
    swaps, owns = [], []
    for p in range(3):
        swaps.append(
            remote(
                mine_ref.at[theirs[p]],
                slab(full_ref, theirs[p], at, core),
                swap_send.at[p],
                swap_recv.at[p],
                partner,
            )
        )
        swaps[-1].start()
        owns.append(
            pltpu.make_async_copy(mine_ref.at[mine[p]], slab(full_ref, mine[p], at, core), own_sem.at[p])
        )
        owns[-1].start()
    for p in range(3):
        owns[p].wait()
    swap_in = [
        remote(
            mine_ref.at[mine[p]],
            slab(full_ref, mine[p], at, 1 - core),
            swap_send.at[p],
            swap_recv.at[p],
            partner,
        )
        for p in range(3)
    ]

    def direct(p, dim, known, send, recv):
        src = slab(full_ref, mine[p], known)
        copies = []
        for step in range(1, SIZES[dim]):
            k = step - 1
            copies.append(remote(src, src, send.at[p, k], recv.at[p, k], device(moved(at, dim, step), core)))
            copies[-1].start()
        return copies

    def arrived(p, dim, known, send, recv):
        for step in range(1, SIZES[dim]):
            k = step - 1
            there = slab(full_ref, mine[p], moved(known, dim, -step))
            remote(there, there, send.at[p, k], recv.at[p, k], partner).wait_recv()

    sent = []
    first, second = [], []
    for p in range(3):
        swap_in[p].wait_recv()
        sent += direct(p, ORDERS[p][0], at, send_1, recv_1)
    for p in range(3):
        a, b, c = ORDERS[p]
        arrived(p, a, at, send_1, recv_1)
        known = {b: at[b], c: at[c]}
        sent += direct(p, b, known, send_2, recv_2)

    sign = 1 - 2 * core
    ways = ((0, sign), (1, -sign))

    def piece(p, where, h):
        return slab(full_ref, mine[p], {ORDERS[p][2]: where}, h)

    def hop(p, way, step, h):
        dim = ORDERS[p][2]
        direction = ways[way][1]
        return remote(
            piece(p, moved(at, dim, -direction * step)[dim], h),
            piece(p, moved(at, dim, -direction * step)[dim], h),
            ring_send.at[p, way, step, h],
            ring_recv.at[p, way, step, h],
            device(moved(at, dim, direction), core),
        )

    def arriving(p, way, step, h):
        dim = ORDERS[p][2]
        where = moved(at, dim, -ways[way][1] * (step + 1))[dim]
        return remote(
            piece(p, where, h), piece(p, where, h), ring_send.at[p, way, step, h], ring_recv.at[p, way, step, h], partner
        )

    def pass_on(p, where, slot):
        copy = remote(
            slab(full_ref, mine[p], {ORDERS[p][2]: where}),
            slab(full_ref, mine[p], {ORDERS[p][2]: where}),
            pass_send.at[p, slot],
            pass_recv.at[p, slot],
            partner,
        )
        copy.start()
        return copy

    def steps_of(p, way):
        return SIZES[ORDERS[p][2]] // 2 - way

    for p in range(3):
        a, b, c = ORDERS[p]
        arrived(p, b, {b: at[b], c: at[c]}, send_2, recv_2)
        for h in range(HALVES):
            for way in range(2):
                copy = hop(p, way, 0, h)
                copy.start()
                sent.append(copy)
        sent.append(pass_on(p, at[c], 0))
    for step in range(4):
        for h in range(HALVES):
            for p in range(3):
                for way in range(2):
                    if step >= steps_of(p, way):
                        continue
                    arriving(p, way, step, h).wait_recv()
                    if step + 1 < steps_of(p, way):
                        copy = hop(p, way, step + 1, h)
                        copy.start()
                        sent.append(copy)
                    if h == HALVES - 1:
                        dim = ORDERS[p][2]
                        where = moved(at, dim, -ways[way][1] * (step + 1))[dim]
                        sent.append(pass_on(p, where, (1 + step if way == 0 else -1 - step) % 8))
    for p in range(3):
        dim = ORDERS[p][2]
        size = SIZES[dim]
        for step in range(size // 2 + 1):
            for way in range(2):
                if (step == 0 and way == 1) or step > steps_of(p, way):
                    continue
                slot = 0 if step == 0 else (step if way == 0 else -step)
                where = moved(at, dim, (ways[way][1]) * step)[dim]
                there = slab(full_ref, theirs[p], {dim: where})
                remote(there, there, pass_send.at[p, slot % 8], pass_recv.at[p, slot % 8], partner).wait_recv()
    for copy in swaps + sent:
        copy.wait_send()


def gather_weights(tiles):
    dma = pltpu.SemaphoreType.DMA
    return pl.pallas_call(
        gather_kernel,
        out_shape=jax.ShapeDtypeStruct((TILES, 8, 4, 2, 4, 2, 8, HD), jnp.bfloat16),
        in_specs=[pl.BlockSpec(memory_space=pltpu.VMEM)],
        out_specs=pl.BlockSpec(memory_space=pltpu.VMEM),
        scratch_shapes=[
            dma((3,)),
            dma((3,)),
            dma((3, 7)),
            dma((3, 7)),
            dma((3, 7)),
            dma((3, 7)),
            dma((3, 2, 4, HALVES)),
            dma((3, 2, 4, HALVES)),
            dma((3, 8)),
            dma((3, 8)),
            dma((3,)),
        ],
        compiler_params=pltpu.CompilerParams(collective_id=0, has_side_effects=True, vmem_limit_bytes=48 * 2**20),
        name="gather_weights",
    )(tiles)


def in_one_piece(arrays, axis, dim, along):
    ends, at = ([], 0)
    for a in arrays[:-1]:
        at += a.shape[along]
        ends.append(at)
    both = jnp.concatenate(arrays, axis=along)
    return tuple(jnp.split(lax.all_gather(both, axis, axis=dim, tiled=True), ends, axis=along))


def gather_turned(arrays, axis, dims):
    turned = [jnp.moveaxis(a, dim, 0) for a, dim in zip(arrays, dims)]
    both = jnp.concatenate([t.reshape(len(t), -1) for t in turned], axis=1)
    filled, at, outs = (lax.all_gather(both, axis, axis=0, tiled=True), 0, [])
    for t, dim in zip(turned, dims):
        section = filled[:, at : at + t[0].size].reshape(-1, *t.shape[1:])
        outs.append(jnp.moveaxis(section, 0, dim))
        at += t[0].size
    return tuple(outs)


def in_order(tiles, dim):
    tiles = jnp.moveaxis(tiles, 0, dim)
    dims = tiles.shape
    return tiles.reshape(*dims[:dim], dims[dim] * dims[dim + 1], *dims[dim + 2 :])


def from_everyone(x, axis):
    copies = jnp.broadcast_to(x, (lax.axis_size(axis), *x.shape))
    return lax.all_to_all(copies, axis, split_axis=0, concat_axis=0, tiled=True)


def gather_directly(x, axis, dim):
    return in_order(from_everyone(x, axis), dim)


def split_up(x, dim, size):
    dims = x.shape
    tiles = x.reshape(*dims[:dim], size, dims[dim] // size, *dims[dim + 1 :])
    return jnp.moveaxis(tiles, dim, 0)


def summed_on_arrival(x, axis, dim):
    tiles = split_up(x, dim, lax.axis_size(axis))
    arrived = lax.all_to_all(tiles, axis, split_axis=0, concat_axis=0, tiled=True)
    return arrived.sum(axis=0)


def summed_on_arrival_2(x, axis, dim):
    size = lax.axis_size(axis)
    tiles = lax.all_to_all(split_up(x, dim, size), axis, 0, 0, tiled=True)
    return jnp.sum(tiles.astype(jnp.float32), axis=0)


def side_by_side(arrays, axis, dim, along):
    columns = [a.reshape(*a.shape[:along], -1) for a in arrays]
    both = jnp.concatenate(columns, axis=along)
    filled, at, outs = (summed_on_arrival_2(both, axis, dim), 0, [])
    for a, column in zip(arrays, columns):
        section = filled[..., at : at + column.shape[along]]
        outs.append(section.reshape(*section.shape[:along], *a.shape[along:]))
        at += column.shape[along]
    return tuple(outs)


def rope_tables(positions, head_size):
    half_size = head_size // 2
    freqs = rope_base ** (-jnp.arange(half_size, dtype=jnp.float32) / half_size)
    angles = positions.astype(jnp.float32)[:, None] * freqs[None, :]
    return (jnp.cos(angles), jnp.sin(angles))


def rotate(values_in, cosine, sine):
    half_size = values_in.shape[-1] // 2
    first, second = (values_in[..., :half_size], values_in[..., half_size:])
    return jnp.concatenate(
        [first * cosine - second * sine, second * cosine + first * sine], axis=-1
    )


def unrotate(grad_out, cosine, sine):
    half_size = grad_out.shape[-1] // 2
    first, second = (grad_out[..., :half_size], grad_out[..., half_size:])
    return jnp.concatenate(
        [first * cosine + second * sine, second * cosine - first * sine], axis=-1
    )


def forward_fold(query_rows, row_pos):

    def forward_advance(carry, piece, start):
        row_top, row_total, weighted = carry
        key_part, value_part = piece
        scores = jnp.einsum("qd,kd->qk", query_rows, key_part, preferred_element_type=jnp.float32)
        key_pos = start + jnp.arange(key_part.shape[0], dtype=jnp.int32)
        allowed = key_pos[None, :] <= row_pos[:, None]
        scores = jnp.where(allowed, scores, -1e30)
        new_top = jnp.maximum(row_top, jnp.max(scores, axis=1))
        numbers = jnp.where(allowed, jnp.exp(scores - new_top[:, None]), 0.0)
        row_total = jnp.sum(numbers, axis=1)
        weighted = jnp.dot(
            numbers,
            value_part.astype(jnp.float32),
            precision=lax.Precision.HIGHEST,
            preferred_element_type=jnp.float32,
        )
        return (new_top, row_total, weighted)

    return forward_advance


def query_grad_fold(query_rows, row_pos, grad_flat, log_total, row_delta):

    def query_advance(grad_query, piece, start):
        key_part, value_part = piece
        scores = jnp.einsum("qd,kd->qk", query_rows, key_part, preferred_element_type=jnp.float32)
        key_pos = start + jnp.arange(key_part.shape[0], dtype=jnp.int32)
        allowed = key_pos[None, :] <= row_pos[:, None]
        probs = jnp.where(
            allowed, jnp.exp(jnp.where(allowed, scores, -1e30) - log_total[:, None]), 0.0
        )
        grad_probs = jnp.einsum(
            "qd,kd->qk", grad_flat, value_part, preferred_element_type=jnp.float32
        )
        grad_scores = (probs * (grad_probs - row_delta[:, None])).astype(jnp.bfloat16)
        return jnp.dot(grad_scores, key_part, preferred_element_type=jnp.float32)

    return query_advance


def key_grad_fold(key_rows, value_rows, key_pos, log_all, delta_all, heads_count):

    def key_advance(carry, piece, start):
        query_part, attn_grad_part = piece
        count = query_part.shape[0]
        scores = jnp.einsum("qd,kd->qk", query_part, key_rows, preferred_element_type=jnp.float32)
        query_pos = jnp.arange(count, dtype=jnp.int32) // heads_count
        allowed = key_pos[None, :] <= query_pos[:, None]
        probs = jnp.where(
            allowed, jnp.exp(jnp.where(allowed, scores, -1e30) - log_all[:, None]), 0.0
        )
        grad_values = jnp.einsum(
            "qk,qd->kd",
            probs.astype(jnp.bfloat16),
            attn_grad_part,
            preferred_element_type=jnp.float32,
        )
        grad_probs = jnp.einsum(
            "qd,kd->qk", attn_grad_part, value_rows, preferred_element_type=jnp.float32
        )
        grad_scores = (probs * (grad_probs - delta_all[:, None])).astype(jnp.bfloat16)
        grad_keys = jnp.einsum(
            "qk,qd->kd", grad_scores, query_part, preferred_element_type=jnp.float32
        )
        return (grad_keys, grad_values)

    return key_advance


def gain_of_outputs(norm_gain):
    pairs = []
    for i in range(64):
        for j in range(8):
            row = (j * 512 + i * 8) // 8
            pairs.append((row, i * 8 + j))
    return lax.ppermute(norm_gain, ("inter", "intra"), pairs).astype(jnp.float32)


def local(hidden_in, norm_gain, qkv_weight, attn_cotangent):
    rows_in = hidden_in[0]
    grad_attn = attn_cotangent[0]
    tokens_here = rows_in.shape[0]
    width = rows_in.shape[1]
    head_size = HD
    heads_count = HEADS
    qcols = heads_count * head_size
    scale = head_size ** (-0.5)
    scaled = (qkv_weight.astype(jnp.float32) * norm_gain.astype(jnp.float32)[:, None]).astype(jnp.bfloat16)
    tiles = jnp.moveaxis(scaled.reshape(8, TILES, HD), 1, 0)
    weight_tiles = gather_weights(tiles).reshape(TILES, width, HD)
    weight_full = jnp.moveaxis(weight_tiles, 0, 1).reshape(width, TILES * HD)
    gain_here = gain_of_outputs(norm_gain)
    query_pos = lax.axis_index("intra") * tokens_here + jnp.arange(tokens_here, dtype=jnp.int32)
    row_pos = jnp.broadcast_to(query_pos[:, None], (tokens_here, heads_count)).reshape(
        tokens_here * heads_count
    )
    cosine, sine = rope_tables(query_pos, head_size)
    wide_rows = rows_in.astype(jnp.float32)
    inv_rms = lax.rsqrt(jnp.mean(wide_rows * wide_rows, axis=1, keepdims=True) + eps_norm)
    normed = (wide_rows * inv_rms).astype(jnp.bfloat16)
    mixed = jnp.dot(normed, weight_full, preferred_element_type=jnp.float32)
    query_rows = (
        (
            rotate(
                mixed[:, :qcols].reshape(tokens_here, heads_count, head_size),
                cosine[:, None, :],
                sine[:, None, :],
            )
            * scale
        )
        .astype(jnp.bfloat16)
        .reshape(tokens_here * heads_count, head_size)
    )
    key_rows = rotate(mixed[:, qcols : qcols + head_size], cosine, sine).astype(jnp.bfloat16)
    value_rows = mixed[:, qcols + head_size :].astype(jnp.bfloat16)
    grad_flat = grad_attn.reshape(tokens_here * heads_count, head_size)
    flat_rows = tokens_here * heads_count
    forward_step = forward_fold(query_rows, row_pos)
    start_carry = (
        jnp.full((flat_rows,), -1e30, jnp.float32),
        jnp.zeros((flat_rows,), jnp.float32),
        jnp.zeros((flat_rows, head_size), jnp.float32),
    )
    key_all, value_all = in_one_piece((key_rows, value_rows), "intra", 0, 1)
    row_top, row_total, weighted = forward_step(start_carry, (key_all, value_all), 0)
    attn_flat = (weighted / row_total[:, None]).astype(jnp.bfloat16)
    log_total = row_top + jnp.log(row_total)
    row_delta = jnp.sum(grad_flat.astype(jnp.float32) * attn_flat.astype(jnp.float32), axis=1)
    query_step = query_grad_fold(query_rows, row_pos, grad_flat, log_total, row_delta)
    grad_query = query_step(jnp.zeros((flat_rows, head_size), jnp.float32), (key_all, value_all), 0)
    log_all, delta_all = gather_turned((log_total, row_delta), "intra", (0, 0))
    key_step = key_grad_fold(key_rows, value_rows, query_pos, log_all, delta_all, heads_count)
    grad_keys, grad_values = key_step(
        (
            jnp.zeros((tokens_here, head_size), jnp.float32),
            jnp.zeros((tokens_here, head_size), jnp.float32),
        ),
        in_one_piece((query_rows, grad_flat), "intra", 0, 1),
        jnp.int32(0),
    )
    query_back = (
        unrotate(
            grad_query.reshape(tokens_here, heads_count, head_size),
            cosine[:, None, :],
            sine[:, None, :],
        )
        * scale
    ).reshape(tokens_here, qcols)
    grad_mixed = jnp.concatenate(
        [query_back, unrotate(grad_keys, cosine, sine), grad_values], axis=1
    ).astype(jnp.bfloat16)
    scaled_grad = jnp.einsum("tc,dc->td", grad_mixed, weight_full, preferred_element_type=jnp.float32)
    inner = jnp.sum(scaled_grad * wide_rows, axis=1, keepdims=True)
    grad_rows = (scaled_grad * inv_rms - wide_rows * inv_rms**3 / width * inner).astype(jnp.bfloat16)
    normed_cols = lax.all_to_all(normed, "intra", split_axis=1, concat_axis=0, tiled=True)
    group_term = lax.dot_general(
        normed_cols,
        gather_directly(grad_mixed, "intra", 0),
        (((0,), (0,)), ((), ())),
        preferred_element_type=jnp.float32,
    )
    term_low = lax.optimization_barrier(group_term.astype(jnp.bfloat16))
    plain_grad = summed_on_arrival_2(term_low, "inter", 0)
    start = lax.axis_index("intra") * 512 + lax.axis_index("inter") * 8
    weight_here = lax.dynamic_slice_in_dim(weight_full, start, 8, 0).astype(jnp.float32)
    weight_grad = plain_grad * gain_here[:, None]
    gain_grad = jnp.sum(plain_grad * weight_here, axis=1) / gain_here
    return (attn_flat.reshape(tokens_here, qcols)[None], grad_rows[None], weight_grad, gain_grad)


def solution(mesh):
    return jax.shard_map(
        local,
        mesh=mesh,
        in_specs=(
            P("inter", "intra", None),
            P(("inter", "intra")),
            P(("inter", "intra"), None),
            P("inter", "intra", None),
        ),
        out_specs=(
            P("inter", "intra", None),
            P("inter", "intra", None),
            P(("intra", "inter"), None),
            P(("intra", "inter")),
        ),
        check_vma=False,
    )
```

```python
import functools
import math

import jax
import jax.numpy as jnp
from jax import lax
from jax.experimental import pallas as pl
from jax.experimental.pallas import tpu as pltpu
from jax.sharding import PartitionSpec as P

HD = 128
HEADS = 4
TILES = HEADS + 2
MESH = pl.DeviceIdType.MESH
SIZES = {"x": 4, "y": 8, "z": 8}
ORDERS = (("z", "y", "x"), ("x", "z", "y"), ("y", "x", "z"))
HALVES = 2
GAIN_ORDER = ("z", "y", "x")

eps_norm = 1e-05
rope_base = 500000.0


def place():
    i, j = lax.axis_index("inter"), lax.axis_index("intra")
    return {"x": j // 2, "y": i // 8, "z": ((i // 2) % 4) * 2 + j % 2}, i % 2


def device(at, core):
    return ((at["y"] * 4 + at["z"] // 2) * 2 + core, at["x"] * 2 + at["z"] % 2)


def moved(at, dim, step):
    size = SIZES[dim]
    return {**at, dim: (at[dim] + step + size) % size}


def slab(ref, tile, at, cores=slice(None)):
    every = slice(None)
    y, x = at.get("y", every), at.get("x", every)
    high, low = (at["z"] // 2, at["z"] % 2) if "z" in at else (every, every)
    return ref.at[tile, y, high, cores, x, low]


def enter(at, core, barrier):
    peers = [device(at, 1 - core)]
    for dim, size in SIZES.items():
        peers += [device(moved(at, dim, step), core) for step in range(1, size)]
    for peer in peers:
        pl.semaphore_signal(barrier, inc=1, device_id=peer, device_id_type=MESH)
    pl.semaphore_wait(barrier, len(peers))


def gain_slab(ref, at, cores):
    every = slice(None)
    y, x = at.get("y", every), at.get("x", every)
    high, low = (at["z"] // 2, at["z"] % 2) if "z" in at else (every, every)
    return ref.at[y, high, cores, x, low]


def gather_kernel(
    mine_ref, gain_ref, full_ref, gain_full, swap_send, swap_recv, send_1, recv_1, send_2, recv_2, ring_send, ring_recv, pass_send, pass_recv, own_sem,
    gain_send, gain_recv,
):
    at, core = place()
    partner = device(at, 1 - core)
    enter(at, core, pltpu.get_barrier_semaphore())

    def remote(src, dst, send, recv, peer):
        return pltpu.make_async_remote_copy(
            src_ref=src, dst_ref=dst, send_sem=send, recv_sem=recv, device_id=peer, device_id_type=MESH
        )

    mine = [3 * core + p for p in range(3)]
    theirs = [3 * (1 - core) + p for p in range(3)]
    swaps, owns = [], []
    for p in range(3):
        swaps.append(
            remote(
                mine_ref.at[theirs[p]],
                slab(full_ref, theirs[p], at, core),
                swap_send.at[p],
                swap_recv.at[p],
                partner,
            )
        )
        swaps[-1].start()
        owns.append(
            pltpu.make_async_copy(mine_ref.at[mine[p]], slab(full_ref, mine[p], at, core), own_sem.at[p])
        )
        owns[-1].start()
    owns.append(pltpu.make_async_copy(gain_ref, gain_slab(gain_full, at, core), own_sem.at[3]))
    owns[-1].start()
    for own in owns:
        own.wait()

    def gain_out(phase):
        dim = GAIN_ORDER[phase]
        src = gain_slab(gain_full, {d: at[d] for d in GAIN_ORDER[phase:]}, core)
        for step in range(1, SIZES[dim]):
            k = step - 1
            peer = device(moved(at, dim, step), core)
            sent.append(remote(src, src, gain_send.at[phase, k], gain_recv.at[phase, k], peer))
            sent[-1].start()

    def gain_in(phase):
        dim = GAIN_ORDER[phase]
        for step in range(1, SIZES[dim]):
            k = step - 1
            known = {d: at[d] for d in GAIN_ORDER[phase:]}
            there = gain_slab(gain_full, moved(known, dim, -step), core)
            remote(there, there, gain_send.at[phase, k], gain_recv.at[phase, k], partner).wait_recv()

    swap_in = [
        remote(
            mine_ref.at[mine[p]],
            slab(full_ref, mine[p], at, 1 - core),
            swap_send.at[p],
            swap_recv.at[p],
            partner,
        )
        for p in range(3)
    ]

    def direct(p, dim, known, send, recv):
        src = slab(full_ref, mine[p], known)
        copies = []
        for step in range(1, SIZES[dim]):
            k = step - 1
            copies.append(remote(src, src, send.at[p, k], recv.at[p, k], device(moved(at, dim, step), core)))
            copies[-1].start()
        return copies

    def arrived(p, dim, known, send, recv):
        for step in range(1, SIZES[dim]):
            k = step - 1
            there = slab(full_ref, mine[p], moved(known, dim, -step))
            remote(there, there, send.at[p, k], recv.at[p, k], partner).wait_recv()

    sent = []
    gain_out(0)
    for p in range(3):
        swap_in[p].wait_recv()
        sent += direct(p, ORDERS[p][0], at, send_1, recv_1)
    for p in range(3):
        a, b, c = ORDERS[p]
        arrived(p, a, at, send_1, recv_1)
        known = {b: at[b], c: at[c]}
        sent += direct(p, b, known, send_2, recv_2)
    gain_in(0)
    gain_out(1)

    sign = 1 - 2 * core
    ways = ((0, sign), (1, -sign))

    def piece(p, where, h):
        return slab(full_ref, mine[p], {ORDERS[p][2]: where}, h)

    def hop(p, way, step, h):
        dim = ORDERS[p][2]
        direction = ways[way][1]
        return remote(
            piece(p, moved(at, dim, -direction * step)[dim], h),
            piece(p, moved(at, dim, -direction * step)[dim], h),
            ring_send.at[p, way, step, h],
            ring_recv.at[p, way, step, h],
            device(moved(at, dim, direction), core),
        )

    def arriving(p, way, step, h):
        dim = ORDERS[p][2]
        where = moved(at, dim, -ways[way][1] * (step + 1))[dim]
        return remote(
            piece(p, where, h), piece(p, where, h), ring_send.at[p, way, step, h], ring_recv.at[p, way, step, h], partner
        )

    def pass_on(p, where, slot):
        copy = remote(
            slab(full_ref, mine[p], {ORDERS[p][2]: where}),
            slab(full_ref, mine[p], {ORDERS[p][2]: where}),
            pass_send.at[p, slot],
            pass_recv.at[p, slot],
            partner,
        )
        copy.start()
        return copy

    def steps_of(p, way):
        return SIZES[ORDERS[p][2]] // 2 - way

    for p in range(3):
        a, b, c = ORDERS[p]
        arrived(p, b, {b: at[b], c: at[c]}, send_2, recv_2)
        for h in range(HALVES):
            for way in range(2):
                copy = hop(p, way, 0, h)
                copy.start()
                sent.append(copy)
        sent.append(pass_on(p, at[c], 0))
    gain_in(1)
    gain_out(2)
    for step in range(4):
        if step == 1:
            gain_in(2)
            mine_gain = gain_slab(gain_full, {}, core)
            sent.append(remote(mine_gain, mine_gain, gain_send.at[3, 0], gain_recv.at[3, 0], partner))
            sent[-1].start()
        for h in range(HALVES):
            for p in range(3):
                for way in range(2):
                    if step >= steps_of(p, way):
                        continue
                    arriving(p, way, step, h).wait_recv()
                    if step + 1 < steps_of(p, way):
                        copy = hop(p, way, step + 1, h)
                        copy.start()
                        sent.append(copy)
                    if h == HALVES - 1:
                        dim = ORDERS[p][2]
                        where = moved(at, dim, -ways[way][1] * (step + 1))[dim]
                        sent.append(pass_on(p, where, (1 + step if way == 0 else -1 - step) % 8))
    for p in range(3):
        dim = ORDERS[p][2]
        size = SIZES[dim]
        for step in range(size // 2 + 1):
            for way in range(2):
                if (step == 0 and way == 1) or step > steps_of(p, way):
                    continue
                slot = 0 if step == 0 else (step if way == 0 else -step)
                where = moved(at, dim, (ways[way][1]) * step)[dim]
                there = slab(full_ref, theirs[p], {dim: where})
                remote(there, there, pass_send.at[p, slot % 8], pass_recv.at[p, slot % 8], partner).wait_recv()
    their_gain = gain_slab(gain_full, {}, 1 - core)
    remote(their_gain, their_gain, gain_send.at[3, 0], gain_recv.at[3, 0], partner).wait_recv()
    for copy in swaps + sent:
        copy.wait_send()


def gather_weights(tiles, gain_row):
    dma = pltpu.SemaphoreType.DMA
    return pl.pallas_call(
        gather_kernel,
        out_shape=(
            jax.ShapeDtypeStruct((TILES, 8, 4, 2, 4, 2, 8, HD), jnp.bfloat16),
            jax.ShapeDtypeStruct((8, 4, 2, 4, 2, 1, 128), jnp.float32),
        ),
        in_specs=[pl.BlockSpec(memory_space=pltpu.VMEM)] * 2,
        out_specs=(pl.BlockSpec(memory_space=pltpu.VMEM),) * 2,
        scratch_shapes=[
            dma((3,)),
            dma((3,)),
            dma((3, 7)),
            dma((3, 7)),
            dma((3, 7)),
            dma((3, 7)),
            dma((3, 2, 4, HALVES)),
            dma((3, 2, 4, HALVES)),
            dma((3, 8)),
            dma((3, 8)),
            dma((4,)),
            dma((4, 7)),
            dma((4, 7)),
        ],
        compiler_params=pltpu.CompilerParams(collective_id=0, has_side_effects=True, vmem_limit_bytes=48 * 2**20),
        name="gather_weights",
    )(tiles, gain_row)


def remote(src, dst, send, recv, peer):
    return pltpu.make_async_remote_copy(
        src_ref=src, dst_ref=dst, send_sem=send, recv_sem=recv, device_id=peer, device_id_type=MESH
    )


def across(left, right, left_dim, right_dim):
    return lax.dot_general(
        left, right, (((left_dim,), (right_dim,)), ((), ())), preferred_element_type=jnp.float32
    )


CHUNK = 256
CHUNKS = 1024 // CHUNK
BLOCKS = CHUNK // 128


def attention_kernel(
    mixed_ref, cos_ref, sin_ref, cot_ref, attn_ref, back_ref,
    kv, probs, part_out, part_in, kv_send, kv_recv, part_send, part_recv,
):
    i, j = lax.axis_index("inter"), lax.axis_index("intra")
    for block in range(8):
        kv[block] = jnp.zeros((2, 128, HD), jnp.bfloat16)
    barrier = pltpu.get_barrier_semaphore()
    for step in range(1, 8):
        pl.semaphore_signal(barrier, inc=1, device_id=(i, (j + step) % 8), device_id_type=MESH)
    cosine, sine = cos_ref[...], sin_ref[...]

    def turned(x, sign):
        return x * cosine + sign * (pltpu.roll(x, 64, 1) * sine)

    kv[j, 0] = turned(mixed_ref[4], 1.0).astype(jnp.bfloat16)
    kv[j, 1] = mixed_ref[5].astype(jnp.bfloat16)
    scale = HD ** (-0.5)
    queries = [(turned(mixed_ref[h], 1.0) * scale).astype(jnp.bfloat16) for h in range(HEADS)]
    cots = [cot_ref[:, h * HD : (h + 1) * HD] for h in range(HEADS)]
    query = jnp.concatenate(queries, axis=0)
    query_t = jnp.concatenate([q.T for q in queries], axis=1)
    cot = jnp.concatenate(cots, axis=0)
    cot_t = jnp.concatenate([c.T for c in cots], axis=1)
    pl.semaphore_wait(barrier, 7)

    def kv_copy(owner, peer):
        return remote(kv.at[owner], kv.at[owner], kv_send.at[peer], kv_recv.at[owner], (i, peer))

    for peer in range(1, 8):
        @pl.when(j < peer)
        def _():
            kv_copy(j, peer).start()

    flat = HEADS * 128
    row_pos = j * 128 + lax.broadcasted_iota(jnp.int32, (CHUNK, flat), 1) % 128
    key_pos = lax.broadcasted_iota(jnp.int32, (CHUNK, flat), 0)

    def allowed(chunk):
        return key_pos + chunk * CHUNK <= row_pos

    def rows(chunk, which):
        return jnp.concatenate([kv[chunk * BLOCKS + b, which] for b in range(BLOCKS)], axis=0)

    top = jnp.full((1, flat), -1e30, jnp.float32)
    for chunk in range(CHUNKS):
        for b in range(BLOCKS):
            owner = chunk * BLOCKS + b

            @pl.when(owner < j)
            def _():
                kv_copy(owner, j).wait_recv()

        scores = jnp.where(allowed(chunk), across(rows(chunk, 0), query_t, 1, 0), -1e30)
        probs[chunk] = scores
        top = jnp.maximum(top, jnp.max(scores, axis=0, keepdims=True))
    total = jnp.zeros((1, flat), jnp.float32)
    out_t = jnp.zeros((HD, flat), jnp.float32)
    for chunk in range(CHUNKS):
        numbers = jnp.where(allowed(chunk), jnp.exp(probs[chunk] - top), 0.0)
        probs[chunk] = numbers
        total = total + jnp.sum(numbers, axis=0, keepdims=True)
        out_t = out_t + across(rows(chunk, 1), numbers.astype(jnp.bfloat16), 0, 0)
    share = 1.0 / total
    attn_t = (out_t * share).astype(jnp.bfloat16)
    for h in range(HEADS):
        attn_ref[:, h * HD : (h + 1) * HD] = attn_t[:, h * 128 : (h + 1) * 128].T
    delta = jnp.sum(cot_t.astype(jnp.float32) * attn_t.astype(jnp.float32), axis=0, keepdims=True)
    query_grad_t = jnp.zeros((HD, flat), jnp.float32)

    def part_copy(owner, maker):
        return remote(part_out.at[owner], part_in.at[maker], part_send.at[owner], part_recv.at[maker], (i, owner))

    def send_parts(chunk):
        for b in range(BLOCKS):
            owner = chunk * BLOCKS + b

            @pl.when(owner < j)
            def _():
                part_copy(owner, j).start()

    for chunk in range(CHUNKS):
        probs_t = probs[chunk] * share
        probs_grad = across(rows(chunk, 1), cot_t, 1, 0)
        scores_grad = (probs_t * (probs_grad - delta)).astype(jnp.bfloat16)
        query_grad_t = query_grad_t + across(rows(chunk, 0), scores_grad, 0, 0)
        keys_part = across(scores_grad, query, 1, 0).astype(jnp.bfloat16)
        values_part = across(probs_t.astype(jnp.bfloat16), cot, 1, 0).astype(jnp.bfloat16)
        for b in range(BLOCKS):
            part_out[chunk * BLOCKS + b, 0] = keys_part[b * 128 : (b + 1) * 128]
            part_out[chunk * BLOCKS + b, 1] = values_part[b * 128 : (b + 1) * 128]
        if chunk:
            send_parts(chunk - 1)
    send_parts(CHUNKS - 1)
    for h in range(HEADS):
        grad = query_grad_t[:, h * 128 : (h + 1) * 128].T
        back_ref[h] = (turned(grad, -1.0) * scale).astype(jnp.bfloat16)
    part_in[j] = part_out[j]
    keys_grad = jnp.zeros((128, HD), jnp.float32)
    values_grad = jnp.zeros((128, HD), jnp.float32)
    for maker in range(8):
        @pl.when(maker > j)
        def _():
            part_copy(j, maker).wait_recv()

        @pl.when(maker < j)
        def _():
            part_in[maker] = jnp.zeros((2, 128, HD), jnp.bfloat16)

        keys_grad = keys_grad + part_in[maker, 0].astype(jnp.float32)
        values_grad = values_grad + part_in[maker, 1].astype(jnp.float32)
    back_ref[4] = turned(keys_grad, -1.0).astype(jnp.bfloat16)
    back_ref[5] = values_grad.astype(jnp.bfloat16)
    for peer in range(1, 8):
        @pl.when(j < peer)
        def _():
            kv_copy(j, peer).wait_send()

    for owner in range(7):
        @pl.when(owner < j)
        def _():
            part_copy(owner, j).wait_send()


def attention(mixed, cosine, sine, cot):
    dma = pltpu.SemaphoreType.DMA
    vmem = pl.BlockSpec(memory_space=pltpu.VMEM)
    return pl.pallas_call(
        attention_kernel,
        out_shape=(
            jax.ShapeDtypeStruct((128, HEADS * HD), jnp.bfloat16),
            jax.ShapeDtypeStruct((TILES, 128, HD), jnp.bfloat16),
        ),
        in_specs=[vmem] * 4,
        out_specs=(vmem, vmem),
        scratch_shapes=[
            pltpu.VMEM((8, 2, 128, HD), jnp.bfloat16),
            pltpu.VMEM((CHUNKS, CHUNK, HEADS * 128), jnp.float32),
            pltpu.VMEM((8, 2, 128, HD), jnp.bfloat16),
            pltpu.VMEM((8, 2, 128, HD), jnp.bfloat16),
            dma((8,)),
            dma((8,)),
            dma((8,)),
            dma((8,)),
        ],
        compiler_params=pltpu.CompilerParams(collective_id=1, has_side_effects=True, vmem_limit_bytes=32 * 2**20),
        name="attention",
    )(mixed, cosine, sine, cot)


def out_slab(ref, tile, at, cores=slice(None)):
    every = slice(None)
    y, x = at.get("y", every), at.get("x", every)
    high, low = (at["z"] // 2, at["z"] % 2) if "z" in at else (every, every)
    return ref.at[tile, x, low, y, high, cores]


RING_SHAPES = {"x": (2, 8, 4, 8, HD), "y": (4, 2, 4, 8, HD), "z": (4, 8, 8, HD)}


def line_shape(p):
    dim = ORDERS[p][0]
    return {"x": (4, 2, 8, HD), "y": (8, 2, 8, HD), "z": (2, 4, 2, 8, HD)}[dim]


def scatter_kernel(
    turned_ref, back_ref, out_ref,
    other, other_back, part, ring_0, ring_1, ring_2, line_0, line_1, line_2, dot_in, final,
    swap_send, swap_recv, ring_send, ring_recv, send_2, recv_2, send_3, recv_3, last_send, last_recv,
):
    at, core = place()
    partner = device(at, 1 - core)
    enter(at, core, pltpu.get_barrier_semaphore())
    swap = remote(turned_ref, other, swap_send.at[0], swap_recv.at[0], partner)
    swap.start()
    swap_back = remote(back_ref.at[pl.ds(3 * (1 - core), 3)], other_back, swap_send.at[1], swap_recv.at[1], partner)
    swap_back.start()
    mine = [3 * core + p for p in range(3)]
    own = jnp.concatenate([back_ref[m] for m in mine], axis=1)
    swap.wait_recv()
    swap_back.wait_recv()
    theirs = jnp.concatenate([other_back[p] for p in range(3)], axis=1)

    @pl.loop(0, 8)
    def _(k):
        rows = pl.ds(k * 512, 512)
        sums = across(turned_ref[rows, :], own, 1, 0) + across(other[rows, :], theirs, 1, 0)
        for p in range(3):
            part[p, k // 2, k % 2] = (
                sums[:, p * HD : (p + 1) * HD].reshape(8, 4, 2, 8, HD).astype(jnp.bfloat16)
            )

    rings = (ring_0, ring_1, ring_2)
    lines = (line_0, line_1, line_2)
    sign = 1 - 2 * core
    ways = (sign, -sign)
    sent = [swap, swap_back]

    def steps_of(p, way):
        return SIZES[ORDERS[p][2]] // 2 - way

    def ring_copy(p, way, step, h):
        dim = ORDERS[p][2]
        target = moved(at, dim, ways[way] * (steps_of(p, way) - step))[dim]
        return remote(
            out_slab(part, p, {dim: target}, h),
            rings[p].at[way, step, h],
            ring_send.at[p, way, step, h],
            ring_recv.at[p, way, step, h],
            device(moved(at, dim, ways[way]), core),
        )

    def add_to(slab_ref, arrived_ref):
        slab_ref[...] = (slab_ref[...].astype(jnp.float32) + arrived_ref[...].astype(jnp.float32)).astype(jnp.bfloat16)

    for h in range(HALVES):
        for p in range(3):
            for way in range(2):
                sent.append(ring_copy(p, way, 0, h))
                sent[-1].start()
    for step in range(4):
        for h in range(HALVES):
            for p in range(3):
                for way in range(2):
                    if step >= steps_of(p, way):
                        continue
                    dim = ORDERS[p][2]
                    target = moved(at, dim, ways[way] * (steps_of(p, way) - step - 1))[dim]
                    ring_copy(p, way, step, h).wait_recv()
                    add_to(out_slab(part, p, {dim: target}, h), rings[p].at[way, step, h])
                    if step + 1 < steps_of(p, way):
                        sent.append(ring_copy(p, way, step + 1, h))
                        sent[-1].start()
    for p in range(3):
        a, b, c = ORDERS[p]
        for step in range(1, SIZES[b]):
            there = moved(at, b, step)
            sent.append(
                remote(
                    out_slab(part, p, {b: there[b], c: at[c]}),
                    lines[p].at[step - 1],
                    send_2.at[p, step - 1],
                    recv_2.at[p, step - 1],
                    device(there, core),
                )
            )
            sent[-1].start()
    for p in range(3):
        a, b, c = ORDERS[p]
        here = out_slab(part, p, {b: at[b], c: at[c]})
        total = here[...].astype(jnp.float32)
        for step in range(1, SIZES[b]):
            remote(here, lines[p].at[step - 1], send_2.at[p, step - 1], recv_2.at[p, step - 1], partner).wait_recv()
            total = total + lines[p][step - 1].astype(jnp.float32)
        here[...] = total.astype(jnp.bfloat16)
        for step in range(1, SIZES[a]):
            there = moved(at, a, step)
            sent.append(
                remote(
                    out_slab(part, p, there),
                    dot_in.at[p, step - 1],
                    send_3.at[p, step - 1],
                    recv_3.at[p, step - 1],
                    device(there, core),
                )
            )
            sent[-1].start()
    for p in range(3):
        a, b, c = ORDERS[p]
        here = out_slab(part, p, at)
        total = here[...].astype(jnp.float32)
        for step in range(1, SIZES[a]):
            remote(here, dot_in.at[p, step - 1], send_3.at[p, step - 1], recv_3.at[p, step - 1], partner).wait_recv()
            total = total + dot_in[p, step - 1].astype(jnp.float32)
        final[p] = total
    lasts = [
        remote(final.at[p, 1 - core], out_ref.at[mine[p]], last_send.at[p], last_recv.at[p], partner) for p in range(3)
    ]
    for p in range(3):
        lasts[p].start()
    for p in range(3):
        out_ref[mine[p]] = final[p, core]
    for p in range(3):
        tile = 3 * (1 - core) + p
        remote(final.at[p, core], out_ref.at[tile], last_send.at[p], last_recv.at[p], partner).wait_recv()
    for copy in sent + lasts:
        copy.wait_send()


def scatter_sums(turned, back):
    dma = pltpu.SemaphoreType.DMA
    vmem = pl.BlockSpec(memory_space=pltpu.VMEM)

    def rings(p):
        dim = ORDERS[p][2]
        return pltpu.VMEM((2, SIZES[dim] // 2, HALVES, *RING_SHAPES[dim]), jnp.bfloat16)

    def lines(p):
        return pltpu.VMEM((SIZES[ORDERS[p][1]] - 1, *line_shape(p)), jnp.bfloat16)

    return pl.pallas_call(
        scatter_kernel,
        out_shape=jax.ShapeDtypeStruct((TILES, 8, HD), jnp.float32),
        in_specs=[vmem] * 2,
        out_specs=vmem,
        scratch_shapes=[
            pltpu.VMEM((4096, 128), jnp.bfloat16),
            pltpu.VMEM((3, 128, HD), jnp.bfloat16),
            pltpu.VMEM((3, 4, 2, 8, 4, 2, 8, HD), jnp.bfloat16),
            *[rings(p) for p in range(3)],
            *[lines(p) for p in range(3)],
            pltpu.VMEM((3, 7, 2, 8, HD), jnp.bfloat16),
            pltpu.VMEM((3, 2, 8, HD), jnp.float32),
            dma((2,)),
            dma((2,)),
            dma((3, 2, 4, HALVES)),
            dma((3, 2, 4, HALVES)),
            dma((3, 7)),
            dma((3, 7)),
            dma((3, 7)),
            dma((3, 7)),
            dma((3,)),
            dma((3,)),
        ],
        compiler_params=pltpu.CompilerParams(collective_id=2, has_side_effects=True, vmem_limit_bytes=32 * 2**20),
        name="scatter_sums",
    )(turned, back)


def rope_tables(first_position):
    freqs = rope_base ** (-jnp.arange(HD // 2, dtype=jnp.float32) / (HD // 2))
    positions = first_position + jnp.arange(128, dtype=jnp.int32)
    angles = positions.astype(jnp.float32)[:, None] * freqs[None, :]
    cosine, sine = jnp.cos(angles), jnp.sin(angles)
    return jnp.concatenate([cosine, cosine], axis=1), jnp.concatenate([-sine, sine], axis=1)


def local(hidden_in, norm_gain, qkv_weight, attn_cotangent):
    rows_in = hidden_in[0]
    tokens, width = rows_in.shape
    i, j = lax.axis_index("inter"), lax.axis_index("intra")
    tiles = jnp.moveaxis(qkv_weight.reshape(8, TILES, HD), 1, 0)
    lane = jnp.arange(128)
    gain_row = jnp.where(lane // 8 == (i * 8 + j) % 16, jnp.tile(norm_gain.astype(jnp.float32), 16), 0.0)[None]
    weight, gain = gather_weights(tiles, gain_row)
    weight = weight.reshape(TILES, width, HD)
    gain = gain.reshape(32, 16, 128).sum(axis=1).reshape(width)
    cosine, sine = rope_tables(j * tokens)
    wide_rows = rows_in.astype(jnp.float32)
    inv_rms = lax.rsqrt(jnp.mean(wide_rows * wide_rows, axis=1, keepdims=True) + eps_norm)
    unit = (wide_rows * inv_rms * gain[None, :]).astype(jnp.bfloat16)
    mixed = jnp.stack([jnp.dot(unit, weight[n], preferred_element_type=jnp.float32) for n in range(TILES)])
    attn, back = attention(mixed, cosine, sine, attn_cotangent[0])
    unit_t = unit.T
    plain_grad = jnp.moveaxis(scatter_sums(unit_t, back), 0, 1).reshape(8, TILES * HD)
    scaled_grad = sum(
        lax.dot_general(back[n], weight[n], (((1,), (1,)), ((), ())), preferred_element_type=jnp.float32)
        for n in range(TILES)
    )
    scaled_grad = scaled_grad * gain[None, :]
    inner = jnp.sum(scaled_grad * wide_rows, axis=1, keepdims=True)
    grad_rows = (scaled_grad * inv_rms - wide_rows * inv_rms**3 / width * inner).astype(jnp.bfloat16)
    start = j * 512 + i * 8
    weight_here = lax.dynamic_slice_in_dim(weight, start, 8, 1).astype(jnp.float32)
    weight_here = jnp.moveaxis(weight_here, 0, 1).reshape(8, TILES * HD)
    gain_here = lax.dynamic_slice_in_dim(gain, start, 8, 0)
    gain_grad = jnp.sum(plain_grad * weight_here, axis=1) / gain_here
    return (attn[None], grad_rows[None], plain_grad, gain_grad)


def solution(mesh):
    return jax.shard_map(
        local,
        mesh=mesh,
        in_specs=(
            P("inter", "intra", None),
            P(("inter", "intra")),
            P(("inter", "intra"), None),
            P("inter", "intra", None),
        ),
        out_specs=(
            P("inter", "intra", None),
            P("inter", "intra", None),
            P(("intra", "inter"), None),
            P(("intra", "inter")),
        ),
        check_vma=False,
    )
```

```python
import functools

import jax
import jax.numpy as jnp
from jax import lax
from jax.experimental import pallas as pl
from jax.experimental.pallas import tpu as pltpu
from jax.sharding import PartitionSpec as P

HD = 128
HEADS = 4
TILES = HEADS + 2
WIDTH = 4096
MESH = pl.DeviceIdType.MESH
SIZES = {"x": 4, "y": 8, "z": 8}
ORDERS = (("z", "y", "x"), ("x", "z", "y"), ("y", "x", "z"))
HALVES = 2
GAIN_ORDER = ("z", "y", "x")
CHUNK = 256
CHUNKS = 1024 // CHUNK
BLOCKS = CHUNK // 128
FLAT = HEADS * 128

eps_norm = 1e-05
rope_base = 500000.0


def place():
    i, j = lax.axis_index("inter"), lax.axis_index("intra")
    return {"x": j // 2, "y": i // 8, "z": ((i // 2) % 4) * 2 + j % 2}, i % 2


def device(at, core):
    return ((at["y"] * 4 + at["z"] // 2) * 2 + core, at["x"] * 2 + at["z"] % 2)


def moved(at, dim, step):
    size = SIZES[dim]
    return {**at, dim: (at[dim] + step + size) % size}


def indices(at):
    every = slice(None)
    y, x = at.get("y", every), at.get("x", every)
    high, low = (at["z"] // 2, at["z"] % 2) if "z" in at else (every, every)
    return y, high, x, low


def slab(ref, tile, at, cores=slice(None)):
    y, high, x, low = indices(at)
    return ref.at[tile, y, high, cores, x, low]


def gain_slab(ref, at, cores):
    y, high, x, low = indices(at)
    return ref.at[y, high, cores, x, low]


def out_slab(ref, tile, at, cores=slice(None)):
    y, high, x, low = indices(at)
    return ref.at[tile, x, low, y, high, cores]


def remote(src, dst, send, recv, peer):
    return pltpu.make_async_remote_copy(
        src_ref=src, dst_ref=dst, send_sem=send, recv_sem=recv, device_id=peer, device_id_type=MESH
    )


def across(left, right, left_dim, right_dim):
    return lax.dot_general(
        left, right, (((left_dim,), (right_dim,)), ((), ())), preferred_element_type=jnp.float32
    )


def steps_of(p, way):
    return SIZES[ORDERS[p][2]] // 2 - way


def greet(at, core, barrier):
    i, j = lax.axis_index("inter"), lax.axis_index("intra")
    peers = [device(at, 1 - core)]
    for dim, size in SIZES.items():
        peers += [device(moved(at, dim, step), core) for step in range(1, size)]
    peers += [(i, (j + step) % 8) for step in range(1, 8)]
    for peer in peers:
        pl.semaphore_signal(barrier, inc=1, device_id=peer, device_id_type=MESH)
    return len(peers)


class Gather:
    def __init__(self, at, core, mine_ref, gain_ref, full, gain_full, sems, sent):
        self.at, self.core, self.partner = at, core, device(at, 1 - core)
        self.mine_ref, self.gain_ref, self.full, self.gain_full = mine_ref, gain_ref, full, gain_full
        (self.swap, self.one, self.two, self.ring, self.passing, self.gains, self.own) = sems
        self.mine = [3 * core + p for p in range(3)]
        self.theirs = [3 * (1 - core) + p for p in range(3)]
        sign = 1 - 2 * core
        self.ways = (sign, -sign)
        self.sent = sent

    def go(self, copy):
        copy.start()
        self.sent.append(copy)

    def begin(self):
        at, core, full = self.at, self.core, self.full
        owns = []
        for p in range(3):
            self.go(
                remote(
                    self.mine_ref.at[self.theirs[p]],
                    slab(full, self.theirs[p], at, core),
                    self.swap.at[0, p],
                    self.swap.at[1, p],
                    self.partner,
                )
            )
            owns.append(
                pltpu.make_async_copy(self.mine_ref.at[self.mine[p]], slab(full, self.mine[p], at, core), self.own.at[p])
            )
        owns.append(pltpu.make_async_copy(self.gain_ref, gain_slab(self.gain_full, at, core), self.own.at[3]))
        for own in owns:
            own.start()
        for own in owns:
            own.wait()
        for p in (1, 2, 0):
            there = slab(full, self.mine[p], at, 1 - core)
            remote(there, there, self.swap.at[0, p], self.swap.at[1, p], self.partner).wait_recv()
            self.direct(p, 0)
        self.gain_out(0)

    def direct(self, p, phase):
        dim = ORDERS[p][phase]
        sems = (self.one, self.two)[phase]
        src = slab(self.full, self.mine[p], {d: self.at[d] for d in ORDERS[p][phase:]})
        for step in range(1, SIZES[dim]):
            peer = device(moved(self.at, dim, step), self.core)
            self.go(remote(src, src, sems.at[0, p, step - 1], sems.at[1, p, step - 1], peer))

    def arrived(self, p, phase):
        dim = ORDERS[p][phase]
        sems = (self.one, self.two)[phase]
        known = {d: self.at[d] for d in ORDERS[p][phase:]}
        for step in range(1, SIZES[dim]):
            there = slab(self.full, self.mine[p], moved(known, dim, -step))
            remote(there, there, sems.at[0, p, step - 1], sems.at[1, p, step - 1], self.partner).wait_recv()

    def gain_out(self, phase):
        dim = GAIN_ORDER[phase]
        src = gain_slab(self.gain_full, {d: self.at[d] for d in GAIN_ORDER[phase:]}, self.core)
        for step in range(1, SIZES[dim]):
            peer = device(moved(self.at, dim, step), self.core)
            self.go(remote(src, src, self.gains.at[0, phase, step - 1], self.gains.at[1, phase, step - 1], peer))

    def gain_in(self, phase):
        dim = GAIN_ORDER[phase]
        known = {d: self.at[d] for d in GAIN_ORDER[phase:]}
        for step in range(1, SIZES[dim]):
            there = gain_slab(self.gain_full, moved(known, dim, -step), self.core)
            remote(
                there, there, self.gains.at[0, phase, step - 1], self.gains.at[1, phase, step - 1], self.partner
            ).wait_recv()

    def gain_pass(self):
        whole = gain_slab(self.gain_full, {}, self.core)
        self.go(remote(whole, whole, self.gains.at[0, 3, 0], self.gains.at[1, 3, 0], self.partner))

    def gain_passed(self):
        whole = gain_slab(self.gain_full, {}, 1 - self.core)
        remote(whole, whole, self.gains.at[0, 3, 0], self.gains.at[1, 3, 0], self.partner).wait_recv()

    def where(self, p, way, step):
        dim = ORDERS[p][2]
        return moved(self.at, dim, -self.ways[way] * step)[dim]

    def hop(self, p, way, step, h):
        dim = ORDERS[p][2]
        piece = slab(self.full, self.mine[p], {dim: self.where(p, way, step)}, h)
        peer = device(moved(self.at, dim, self.ways[way]), self.core)
        self.go(remote(piece, piece, self.ring.at[0, p, way, step, h], self.ring.at[1, p, way, step, h], peer))

    def pass_on(self, p, where, slot):
        piece = slab(self.full, self.mine[p], {ORDERS[p][2]: where})
        self.go(remote(piece, piece, self.passing.at[0, p, slot], self.passing.at[1, p, slot], self.partner))

    def ring_start(self, p):
        for h in range(HALVES):
            for way in range(2):
                self.hop(p, way, 0, h)
        self.pass_on(p, self.at[ORDERS[p][2]], 0)

    def ring_step(self, p, step):
        dim = ORDERS[p][2]
        for h in range(HALVES):
            for way in range(2):
                if step >= steps_of(p, way):
                    continue
                piece = slab(self.full, self.mine[p], {dim: self.where(p, way, step + 1)}, h)
                remote(
                    piece, piece, self.ring.at[0, p, way, step, h], self.ring.at[1, p, way, step, h], self.partner
                ).wait_recv()
                if step + 1 < steps_of(p, way):
                    self.hop(p, way, step + 1, h)
                if h == HALVES - 1:
                    self.pass_on(p, self.where(p, way, step + 1), 1 + step if way == 0 else 7 - step)

    def passed(self):
        for p in range(3):
            dim = ORDERS[p][2]
            for way in range(2):
                for step in range(way, steps_of(p, way) + 1):
                    slot = (step if way == 0 else 8 - step) % 8
                    where = moved(self.at, dim, self.ways[way] * step)[dim]
                    piece = slab(self.full, self.theirs[p], {dim: where})
                    remote(
                        piece, piece, self.passing.at[0, p, slot], self.passing.at[1, p, slot], self.partner
                    ).wait_recv()


RING_SHAPES = {"x": (2, 8, 4, 8, HD), "y": (4, 2, 4, 8, HD), "z": (4, 8, 8, HD)}
LINE_SHAPES = {"x": (4, 2, 8, HD), "y": (8, 2, 8, HD), "z": (2, 4, 2, 8, HD)}


class Scatter:
    def __init__(self, at, core, part, rings, lines, dot_in, final, total_ref, sems, sent):
        self.at, self.core, self.partner = at, core, device(at, 1 - core)
        self.part, self.rings, self.lines, self.dot_in = part, rings, lines, dot_in
        self.final, self.total_ref = final, total_ref
        self.ring, self.two, self.three, self.last = sems
        sign = 1 - 2 * core
        self.ways = (sign, -sign)
        self.sent = sent

    def go(self, copy):
        copy.start()
        self.sent.append(copy)

    def target(self, p, way, left):
        dim = ORDERS[p][2]
        return {dim: moved(self.at, dim, self.ways[way] * left)[dim]}

    def copy(self, p, way, step, h):
        dim = ORDERS[p][2]
        return remote(
            out_slab(self.part, p, self.target(p, way, steps_of(p, way) - step), h),
            self.rings[p].at[way, step, h],
            self.ring.at[0, p, way, step, h],
            self.ring.at[1, p, way, step, h],
            device(moved(self.at, dim, self.ways[way]), self.core),
        )

    def ring_start(self, p):
        for h in range(HALVES):
            for way in range(2):
                self.go(self.copy(p, way, 0, h))

    def ring_step(self, p, step):
        for h in range(HALVES):
            for way in range(2):
                if step >= steps_of(p, way):
                    continue
                self.copy(p, way, step, h).wait_recv()
                here = out_slab(self.part, p, self.target(p, way, steps_of(p, way) - step - 1), h)
                there = self.rings[p].at[way, step, h]
                here[...] = (here[...].astype(jnp.float32) + there[...].astype(jnp.float32)).astype(jnp.bfloat16)
                if step + 1 < steps_of(p, way):
                    self.go(self.copy(p, way, step + 1, h))

    def lines_out(self, p):
        a, b, c = ORDERS[p]
        for step in range(1, SIZES[b]):
            there = moved(self.at, b, step)
            self.go(
                remote(
                    out_slab(self.part, p, {b: there[b], c: self.at[c]}),
                    self.lines[p].at[step - 1],
                    self.two.at[0, p, step - 1],
                    self.two.at[1, p, step - 1],
                    device(there, self.core),
                )
            )

    def dots_out(self, p):
        a, b, c = ORDERS[p]
        here = out_slab(self.part, p, {b: self.at[b], c: self.at[c]})
        total = here[...].astype(jnp.float32)
        for step in range(1, SIZES[b]):
            remote(
                here, self.lines[p].at[step - 1], self.two.at[0, p, step - 1], self.two.at[1, p, step - 1], self.partner
            ).wait_recv()
            total = total + self.lines[p][step - 1].astype(jnp.float32)
        here[...] = total.astype(jnp.bfloat16)
        for step in range(1, SIZES[a]):
            there = moved(self.at, a, step)
            self.go(
                remote(
                    out_slab(self.part, p, there),
                    self.dot_in.at[p, step - 1],
                    self.three.at[0, p, step - 1],
                    self.three.at[1, p, step - 1],
                    device(there, self.core),
                )
            )

    def finish(self, p):
        a = ORDERS[p][0]
        here = out_slab(self.part, p, self.at)
        total = here[...].astype(jnp.float32)
        for step in range(1, SIZES[a]):
            remote(
                here, self.dot_in.at[p, step - 1], self.three.at[0, p, step - 1], self.three.at[1, p, step - 1], self.partner
            ).wait_recv()
            total = total + self.dot_in[p, step - 1].astype(jnp.float32)
        self.final[p] = total
        tile = 3 * self.core + p
        self.total_ref[tile] = self.final[p, self.core]
        self.go(
            remote(
                self.final.at[p, 1 - self.core], self.total_ref.at[tile], self.last.at[0, p], self.last.at[1, p], self.partner
            )
        )

    def finished(self, p):
        tile = 3 * (1 - self.core) + p
        remote(
            self.final.at[p, 0], self.total_ref.at[tile], self.last.at[0, p], self.last.at[1, p], self.partner
        ).wait_recv()


def whole_kernel(
    hidden_ref, mine_ref, gain_ref, cos_ref, sin_ref, cot_ref,
    attn_ref, grad_in_ref, weight_grad_ref, gain_grad_ref,
    full, gain_full, gain_row, normed, turned_own, turned_other,
    kv, probs, part_out, part_in, back, back_other, plain,
    part, ring_0, ring_1, ring_2, line_0, line_1, line_2, dot_in, final, total_ref,
    g_swap, g_one, g_two, g_ring, g_pass, g_gain, g_own,
    kv_sem, part_sem, swap_sem, s_ring, s_two, s_three, s_last,
):
    i, j = lax.axis_index("inter"), lax.axis_index("intra")
    at, core = place()
    partner = device(at, 1 - core)
    sent = []
    barrier = pltpu.get_barrier_semaphore()
    for block in range(8):
        kv[block] = jnp.zeros((2, 128, HD), jnp.bfloat16)
    count = greet(at, core, barrier)
    squares = jnp.zeros((128, 128), jnp.float32)
    for t in range(WIDTH // 128):
        tile = hidden_ref[:, t * 128 : (t + 1) * 128].astype(jnp.float32)
        squares = squares + tile * tile
    inv_rms = lax.rsqrt(jnp.sum(squares, axis=1, keepdims=True) / WIDTH + eps_norm)
    cosine, sine = cos_ref[...], sin_ref[...]
    cots = [cot_ref[:, h * HD : (h + 1) * HD] for h in range(HEADS)]
    pl.semaphore_wait(barrier, count)

    g = Gather(
        at, core, mine_ref, gain_ref, full, gain_full, (g_swap, g_one, g_two, g_ring, g_pass, g_gain, g_own), sent
    )
    g.begin()
    for p in (1, 2, 0):
        g.arrived(p, 0)
        g.direct(p, 1)
    g.gain_in(0)
    g.gain_out(1)
    for p in (2, 1):
        g.arrived(p, 1)
        g.ring_start(p)
    g.gain_in(1)
    g.gain_out(2)
    g.ring_step(2, 0)
    g.ring_step(1, 0)
    g.arrived(0, 1)
    g.ring_start(0)
    g.gain_in(2)
    g.gain_pass()
    g.ring_step(2, 1)
    g.ring_step(1, 1)
    g.gain_passed()
    for y in range(8):
        for z in range(4):
            t = y * 4 + z
            gain_row[:, t * 128 : (t + 1) * 128] = jnp.sum(gain_full[y, z], axis=(0, 1, 2))
    for t in range(WIDTH // 128):
        cols = slice(t * 128, (t + 1) * 128)
        unit = hidden_ref[:, cols].astype(jnp.float32) * inv_rms * gain_row[:, cols]
        normed[:, cols] = unit.astype(jnp.bfloat16)
    g.ring_step(0, 0)
    g.ring_step(2, 2)
    g.ring_step(1, 2)
    for t in range(WIDTH // 128):
        cols = slice(t * 128, (t + 1) * 128)
        turned_own[cols, :] = normed[:, cols].T
    g.ring_step(0, 1)
    g.ring_step(2, 3)
    g.ring_step(1, 3)
    swap = remote(turned_own, turned_other, swap_sem.at[0, 0], swap_sem.at[1, 0], partner)
    swap.start()
    g.passed()

    def weight_rows(pair, y):
        return jnp.concatenate([full[2 * pair + k, y].reshape(512, HD) for k in range(2)], axis=1)

    def mixed_pair(pair):
        total = jnp.zeros((128, 2 * HD), jnp.float32)
        for y in range(8):
            total = total + across(normed[:, y * 512 : (y + 1) * 512], weight_rows(pair, y), 1, 0)
        return total[:, :HD], total[:, HD:]

    def rotated(x, sign):
        return x * cosine + sign * (pltpu.roll(x, 64, 1) * sine)

    keys_in, values_in = mixed_pair(2)
    kv[j, 0] = rotated(keys_in, 1.0).astype(jnp.bfloat16)
    kv[j, 1] = values_in.astype(jnp.bfloat16)

    def kv_copy(owner, peer):
        return remote(kv.at[owner], kv.at[owner], kv_sem.at[0, peer], kv_sem.at[1, owner], (i, peer))

    for peer in range(1, 8):
        @pl.when(j < peer)
        def _():
            kv_copy(j, peer).start()

    scale = HD ** (-0.5)
    heads = [*mixed_pair(0), *mixed_pair(1)]
    queries = [(rotated(head, 1.0) * scale).astype(jnp.bfloat16) for head in heads]
    query = jnp.concatenate(queries, axis=0)
    query_t = jnp.concatenate([q.T for q in queries], axis=1)
    cot = jnp.concatenate(cots, axis=0)
    cot_t = jnp.concatenate([c.T for c in cots], axis=1)
    row_pos = j * 128 + lax.broadcasted_iota(jnp.int32, (CHUNK, FLAT), 1) % 128
    key_pos = lax.broadcasted_iota(jnp.int32, (CHUNK, FLAT), 0)

    def allowed(chunk):
        return key_pos + chunk * CHUNK <= row_pos

    def rows(chunk, which):
        return jnp.concatenate([kv[chunk * BLOCKS + b, which] for b in range(BLOCKS)], axis=0)

    top = jnp.full((1, FLAT), -1e30, jnp.float32)
    for chunk in range(CHUNKS):
        for b in range(BLOCKS):
            owner = chunk * BLOCKS + b

            @pl.when(owner < j)
            def _():
                kv_copy(owner, j).wait_recv()

        scores = jnp.where(allowed(chunk), across(rows(chunk, 0), query_t, 1, 0), -1e30)
        probs[chunk] = scores
        top = jnp.maximum(top, jnp.max(scores, axis=0, keepdims=True))
    total = jnp.zeros((1, FLAT), jnp.float32)
    out_t = jnp.zeros((HD, FLAT), jnp.float32)
    for chunk in range(CHUNKS):
        numbers = jnp.where(allowed(chunk), jnp.exp(probs[chunk] - top), 0.0)
        probs[chunk] = numbers
        total = total + jnp.sum(numbers, axis=0, keepdims=True)
        out_t = out_t + across(rows(chunk, 1), numbers.astype(jnp.bfloat16), 0, 0)
    share = 1.0 / total
    attn_t = (out_t * share).astype(jnp.bfloat16)
    delta = jnp.sum(cot_t.astype(jnp.float32) * attn_t.astype(jnp.float32), axis=0, keepdims=True)
    query_grad_t = jnp.zeros((HD, FLAT), jnp.float32)

    def part_copy(owner, maker):
        return remote(part_out.at[owner], part_in.at[maker], part_sem.at[0, owner], part_sem.at[1, maker], (i, owner))

    def send_parts(chunk):
        for b in range(BLOCKS):
            owner = chunk * BLOCKS + b

            @pl.when(owner < j)
            def _():
                part_copy(owner, j).start()

    for chunk in range(CHUNKS):
        probs_t = probs[chunk] * share
        probs_grad = across(rows(chunk, 1), cot_t, 1, 0)
        scores_grad = (probs_t * (probs_grad - delta)).astype(jnp.bfloat16)
        query_grad_t = query_grad_t + across(rows(chunk, 0), scores_grad, 0, 0)
        keys_part = across(scores_grad, query, 1, 0).astype(jnp.bfloat16)
        values_part = across(probs_t.astype(jnp.bfloat16), cot, 1, 0).astype(jnp.bfloat16)
        for b in range(BLOCKS):
            part_out[chunk * BLOCKS + b, 0] = keys_part[b * 128 : (b + 1) * 128]
            part_out[chunk * BLOCKS + b, 1] = values_part[b * 128 : (b + 1) * 128]
        if chunk:
            send_parts(chunk - 1)
    send_parts(CHUNKS - 1)
    for h in range(HEADS):
        attn_ref[:, h * HD : (h + 1) * HD] = attn_t[:, h * 128 : (h + 1) * 128].T
        grad = query_grad_t[:, h * 128 : (h + 1) * 128].T
        back[h] = (rotated(grad, -1.0) * scale).astype(jnp.bfloat16)
    part_in[j] = part_out[j]
    keys_grad = jnp.zeros((128, HD), jnp.float32)
    values_grad = jnp.zeros((128, HD), jnp.float32)
    for maker in range(8):
        @pl.when(maker > j)
        def _():
            part_copy(j, maker).wait_recv()

        @pl.when(maker < j)
        def _():
            part_in[maker] = jnp.zeros((2, 128, HD), jnp.bfloat16)

        keys_grad = keys_grad + part_in[maker, 0].astype(jnp.float32)
        values_grad = values_grad + part_in[maker, 1].astype(jnp.float32)
    back[4] = rotated(keys_grad, -1.0).astype(jnp.bfloat16)
    back[5] = values_grad.astype(jnp.bfloat16)

    swap_back = remote(
        back.at[pl.ds(3 * (1 - core), 3)], back_other, swap_sem.at[0, 1], swap_sem.at[1, 1], partner
    )
    swap_back.start()
    own = jnp.concatenate([back[3 * core + p] for p in range(3)], axis=1)
    swap.wait_recv()
    swap_back.wait_recv()
    theirs = jnp.concatenate([back_other[p] for p in range(3)], axis=1)

    @pl.loop(0, 8)
    def _(k):
        chosen = pl.ds(k * 512, 512)
        sums = across(turned_own[chosen, :], own, 1, 0) + across(turned_other[chosen, :], theirs, 1, 0)
        for p in range(3):
            part[p, k // 2, k % 2] = sums[:, p * HD : (p + 1) * HD].reshape(8, 4, 2, 8, HD).astype(jnp.bfloat16)

    s = Scatter(
        at, core, part, (ring_0, ring_1, ring_2), (line_0, line_1, line_2), dot_in, final, total_ref,
        (s_ring, s_two, s_three, s_last), sent,
    )
    for p in (0, 1, 2):
        s.ring_start(p)
    pairs = [jnp.concatenate([back[2 * pair], back[2 * pair + 1]], axis=1) for pair in range(3)]

    def plain_rows(y, inner):
        cols = slice(y * 512, (y + 1) * 512)
        grad = sum(across(pairs[pair], weight_rows(pair, y), 1, 1) for pair in range(3))
        grad = grad * gain_row[:, cols]
        plain[:, cols] = grad
        return inner + jnp.sum(grad * hidden_ref[:, cols].astype(jnp.float32), axis=1, keepdims=True)

    inner = jnp.zeros((128, 1), jnp.float32)
    for y in (0, 1, 2, 3):
        inner = plain_rows(y, inner)
    s.ring_step(1, 0)
    s.ring_step(2, 0)
    s.ring_step(0, 0)
    for y in (4, 5):
        inner = plain_rows(y, inner)
    s.ring_step(1, 1)
    s.ring_step(2, 1)
    for y in (6, 7):
        inner = plain_rows(y, inner)
    s.ring_step(0, 1)
    s.lines_out(0)
    s.ring_step(1, 2)
    s.ring_step(2, 2)
    fall = inv_rms * inv_rms * inv_rms * (1.0 / WIDTH) * inner
    for y in range(8):
        cols = slice(y * 512, (y + 1) * 512)
        grad_in_ref[:, cols] = (
            plain[:, cols] * inv_rms - hidden_ref[:, cols].astype(jnp.float32) * fall
        ).astype(jnp.bfloat16)
    s.ring_step(1, 3)
    s.lines_out(1)
    s.ring_step(2, 3)
    s.lines_out(2)
    for p in (0, 2, 1):
        s.dots_out(p)
    for p in (1, 0, 2):
        s.finish(p)
    for p in (1, 0, 2):
        s.finished(p)
    inside = (j, i // 16, (i // 8) % 2, (i // 2) % 4, i % 2)
    sums = jnp.zeros((8, HD), jnp.float32)
    for n in range(TILES):
        tile = total_ref[n]
        weight_grad_ref[:, n * HD : (n + 1) * HD] = tile
        sums = sums + tile * full[(n, *inside)].astype(jnp.float32)
    lane = lax.broadcasted_iota(jnp.int32, (8, 128), 1)
    row = lax.broadcasted_iota(jnp.int32, (8, 128), 0)
    gains = jnp.sum(jnp.where(lane % 8 == row, gain_full[inside], 0.0), axis=1, keepdims=True)
    answer = jnp.sum(sums, axis=1, keepdims=True) / gains
    gain_grad_ref[...] = jnp.sum(jnp.where(lane == row, answer, 0.0), axis=0, keepdims=True)

    for peer in range(1, 8):
        @pl.when(j < peer)
        def _():
            kv_copy(j, peer).wait_send()

    for owner in range(7):
        @pl.when(owner < j)
        def _():
            part_copy(owner, j).wait_send()

    for copy in sent + [swap, swap_back]:
        copy.wait_send()


def whole(hidden, tiles, gain_piece, cosine, sine, cot):
    dma = pltpu.SemaphoreType.DMA
    vmem = pl.BlockSpec(memory_space=pltpu.VMEM)
    low, wide = jnp.bfloat16, jnp.float32

    def rings(p):
        dim = ORDERS[p][2]
        return pltpu.VMEM((2, SIZES[dim] // 2, HALVES, *RING_SHAPES[dim]), low)

    def lines(p):
        return pltpu.VMEM((SIZES[ORDERS[p][1]] - 1, *LINE_SHAPES[ORDERS[p][0]]), low)

    return pl.pallas_call(
        whole_kernel,
        out_shape=(
            jax.ShapeDtypeStruct((128, FLAT), low),
            jax.ShapeDtypeStruct((128, WIDTH), low),
            jax.ShapeDtypeStruct((8, TILES * HD), wide),
            jax.ShapeDtypeStruct((1, 128), wide),
        ),
        in_specs=[vmem] * 6,
        out_specs=(vmem,) * 4,
        scratch_shapes=[
            pltpu.VMEM((TILES, 8, 4, 2, 4, 2, 8, HD), low),
            pltpu.VMEM((8, 4, 2, 4, 2, 1, 128), wide),
            pltpu.VMEM((1, WIDTH), wide),
            pltpu.VMEM((128, WIDTH), low),
            pltpu.VMEM((WIDTH, 128), low),
            pltpu.VMEM((WIDTH, 128), low),
            pltpu.VMEM((8, 2, 128, HD), low),
            pltpu.VMEM((CHUNKS, CHUNK, FLAT), wide),
            pltpu.VMEM((8, 2, 128, HD), low),
            pltpu.VMEM((8, 2, 128, HD), low),
            pltpu.VMEM((TILES, 128, HD), low),
            pltpu.VMEM((3, 128, HD), low),
            pltpu.VMEM((128, WIDTH), wide),
            pltpu.VMEM((3, 4, 2, 8, 4, 2, 8, HD), low),
            *[rings(p) for p in range(3)],
            *[lines(p) for p in range(3)],
            pltpu.VMEM((3, 7, 2, 8, HD), low),
            pltpu.VMEM((3, 2, 8, HD), wide),
            pltpu.VMEM((TILES, 8, HD), wide),
            dma((2, 3)),
            dma((2, 3, 7)),
            dma((2, 3, 7)),
            dma((2, 3, 2, 4, HALVES)),
            dma((2, 3, 8)),
            dma((2, 4, 7)),
            dma((4,)),
            dma((2, 8)),
            dma((2, 8)),
            dma((2, 2)),
            dma((2, 3, 2, 4, HALVES)),
            dma((2, 3, 7)),
            dma((2, 3, 7)),
            dma((2, 3)),
        ],
        compiler_params=pltpu.CompilerParams(collective_id=0, has_side_effects=True, vmem_limit_bytes=56 * 2**20),
        name="whole",
    )(hidden, tiles, gain_piece, cosine, sine, cot)


def rope_tables(first_position):
    freqs = rope_base ** (-jnp.arange(HD // 2, dtype=jnp.float32) / (HD // 2))
    positions = first_position + jnp.arange(128, dtype=jnp.int32)
    angles = positions.astype(jnp.float32)[:, None] * freqs[None, :]
    cosine, sine = jnp.cos(angles), jnp.sin(angles)
    return jnp.concatenate([cosine, cosine], axis=1), jnp.concatenate([-sine, sine], axis=1)


def local(hidden_in, norm_gain, qkv_weight, attn_cotangent):
    i, j = lax.axis_index("inter"), lax.axis_index("intra")
    tiles = jnp.moveaxis(qkv_weight.reshape(8, TILES, HD), 1, 0)
    lane = jnp.arange(128)
    gain_piece = jnp.where(lane // 8 == (i * 8 + j) % 16, jnp.tile(norm_gain.astype(jnp.float32), 16), 0.0)[None]
    cosine, sine = rope_tables(j * 128)
    attn, grad_in, weight_grad, gain_grad = whole(hidden_in[0], tiles, gain_piece, cosine, sine, attn_cotangent[0])
    return (attn[None], grad_in[None], weight_grad, gain_grad[0, :8])


def solution(mesh):
    return jax.shard_map(
        local,
        mesh=mesh,
        in_specs=(
            P("inter", "intra", None),
            P(("inter", "intra")),
            P(("inter", "intra"), None),
            P("inter", "intra", None),
        ),
        out_specs=(
            P("inter", "intra", None),
            P("inter", "intra", None),
            P(("intra", "inter"), None),
            P(("intra", "inter")),
        ),
        check_vma=False,
    )
```

```python
import functools

import jax
import jax.numpy as jnp
from jax import lax
from jax.experimental import pallas as pl
from jax.experimental.pallas import tpu as pltpu
from jax.sharding import PartitionSpec as P

HD = 128
HEADS = 4
TILES = HEADS + 2
WIDTH = 4096
MESH = pl.DeviceIdType.MESH
SIZES = {"x": 4, "y": 8, "z": 8}
ORDERS = (
    (("z", "y", "x"), ("y", "z", "x")),
    (("z", "x", "y"), ("z", "x", "y")),
    (("y", "x", "z"), ("y", "x", "z")),
)
RINGS = ("x", "y", "z")
HALVES = 2
GAIN_ORDER = ("z", "y", "x")
CHUNK = 256
CHUNKS = 1024 // CHUNK
BLOCKS = CHUNK // 128
FLAT = HEADS * 128

eps_norm = 1e-05
rope_base = 500000.0


def place():
    i, j = lax.axis_index("inter"), lax.axis_index("intra")
    return {"x": j // 2, "y": i // 8, "z": ((i // 2) % 4) * 2 + j % 2}, i % 2


def device(at, core):
    return ((at["y"] * 4 + at["z"] // 2) * 2 + core, at["x"] * 2 + at["z"] % 2)


def moved(at, dim, step):
    size = SIZES[dim]
    return {**at, dim: (at[dim] + step + size) % size}


def indices(at):
    every = slice(None)
    y, x = at.get("y", every), at.get("x", every)
    high, low = (at["z"] // 2, at["z"] % 2) if "z" in at else (every, every)
    return y, high, x, low


def slab(ref, tile, at, cores=slice(None)):
    y, high, x, low = indices(at)
    return ref.at[tile, y, high, cores, x, low]


def gain_slab(ref, at, cores):
    y, high, x, low = indices(at)
    return ref.at[y, high, cores, x, low]


def out_slab(ref, tile, at, cores=slice(None)):
    y, high, x, low = indices(at)
    return ref.at[tile, x, low, y, high, cores]


def remote(src, dst, send, recv, peer):
    return pltpu.make_async_remote_copy(
        src_ref=src, dst_ref=dst, send_sem=send, recv_sem=recv, device_id=peer, device_id_type=MESH
    )


def across(left, right, left_dim, right_dim):
    return lax.dot_general(
        left, right, (((left_dim,), (right_dim,)), ((), ())), preferred_element_type=jnp.float32
    )


def steps_of(p, way):
    return SIZES[RINGS[p]] // 2 - way


def tiles_of(core):
    return [4 + core, 2 * core, 2 * core + 1]


def settle(spare, count, sem):
    pltpu.make_async_copy(spare.at[pl.ds(0, count)], spare.at[pl.ds(0, count)], sem).wait()


def greet(at, core, barrier):
    i, j = lax.axis_index("inter"), lax.axis_index("intra")
    peers = [device(at, 1 - core)]
    for dim, size in SIZES.items():
        peers += [device(moved(at, dim, step), core) for step in range(1, size)]
    peers += [(i, (j + step) % 8) for step in range(1, 8)]
    for peer in peers:
        pl.semaphore_signal(barrier, inc=1, device_id=peer, device_id_type=MESH)
    return len(peers)


class Gather:
    def __init__(self, at, core, mine_ref, gain_ref, full, gain_full, spare, sems):
        self.at, self.core, self.partner = at, core, device(at, 1 - core)
        self.mine_ref, self.gain_ref, self.full, self.gain_full = mine_ref, gain_ref, full, gain_full
        (self.swap, self.one, self.two, self.ring_out, self.ring, self.passing, self.gains, self.own) = sems
        self.mine, self.theirs = tiles_of(core), tiles_of(1 - core)
        sign = 1 - 2 * core
        self.ways = (sign, -sign)
        self.spare = spare

    def go(self, copy):
        copy.start()

    def begin(self):
        at, core, full = self.at, self.core, self.full
        owns = []
        for p in range(3):
            self.go(
                remote(
                    self.mine_ref.at[self.theirs[p]],
                    slab(full, self.theirs[p], at, core),
                    self.swap.at[0],
                    self.swap.at[1],
                    self.partner,
                )
            )
            owns.append(
                pltpu.make_async_copy(self.mine_ref.at[self.mine[p]], slab(full, self.mine[p], at, core), self.own.at[p])
            )
        owns.append(pltpu.make_async_copy(self.gain_ref, gain_slab(self.gain_full, at, core), self.own.at[3]))
        for own in owns:
            own.start()
        for own in owns:
            own.wait()
        self.gain_out(0)
        settle(self.spare, 3, self.swap.at[1])
        for p in (1, 2, 0):
            for h in range(HALVES):
                self.direct(p, h, 0)

    def direct(self, p, h, phase):
        order = ORDERS[p][h]
        sems = (self.one, self.two)[phase]
        src = slab(self.full, self.mine[p], {d: self.at[d] for d in order[phase:]}, h)
        for step in range(1, SIZES[order[phase]]):
            peer = device(moved(self.at, order[phase], step), self.core)
            self.go(remote(src, src, sems.at[6], sems.at[2 * p + h], peer))

    def arrived(self, p, h, phase):
        order = ORDERS[p][h]
        sems = (self.one, self.two)[phase]
        each = 1 if phase == 0 else SIZES[order[0]]
        settle(self.spare, (SIZES[order[phase]] - 1) * each, sems.at[2 * p + h])

    def gain_out(self, phase):
        dim = GAIN_ORDER[phase]
        src = gain_slab(self.gain_full, {d: self.at[d] for d in GAIN_ORDER[phase:]}, self.core)
        for step in range(1, SIZES[dim]):
            peer = device(moved(self.at, dim, step), self.core)
            self.go(remote(src, src, self.gains.at[0, phase], self.gains.at[1, phase], peer))

    def gain_wait(self, phase, side):
        rows = (
            self.gain_full.at[pl.ds(0, 7), 0, 0, 0, 0],
            self.gain_full.at[pl.ds(0, 7), :, :, 0, 0],
            self.gain_full.at[pl.ds(0, 6), :, :, :, 0],
            self.gain_full.at[:, :, 0],
        )[phase]
        pltpu.make_async_copy(rows, rows, self.gains.at[side, phase]).wait()

    def gain_in(self, phase):
        self.gain_wait(phase, 1)

    def gain_pass(self):
        whole = gain_slab(self.gain_full, {}, self.core)
        self.go(remote(whole, whole, self.gains.at[0, 3], self.gains.at[1, 3], self.partner))

    def gain_passed(self):
        self.gain_wait(3, 1)

    def settled(self):
        settle(self.spare, 3, self.swap.at[0])
        settle(self.spare, 42, self.one.at[6])
        settle(self.spare, 208, self.two.at[6])
        for p in range(3):
            settle(self.spare, 384 if RINGS[p] == "x" else 448, self.ring_out.at[p])
            settle(self.spare, 512, self.passing.at[0, p])
        for phase in range(4):
            self.gain_wait(phase, 0)

    def where(self, p, way, step):
        dim = RINGS[p]
        return moved(self.at, dim, -self.ways[way] * step)[dim]

    def hop(self, p, way, step, h):
        dim = RINGS[p]
        piece = slab(self.full, self.mine[p], {dim: self.where(p, way, step)}, h)
        peer = device(moved(self.at, dim, self.ways[way]), self.core)
        self.go(remote(piece, piece, self.ring_out.at[p], self.ring.at[p, way, step, h], peer))

    def pass_on(self, p, h, where):
        piece = slab(self.full, self.mine[p], {RINGS[p]: where}, h)
        self.go(remote(piece, piece, self.passing.at[0, p], self.passing.at[1, p], self.partner))

    def ring_start(self, p, h):
        for way in range(2):
            self.hop(p, way, 0, h)
        self.pass_on(p, h, self.at[RINGS[p]])

    def ring_step(self, p, h, step):
        dim = RINGS[p]
        for way in range(2):
            if step >= steps_of(p, way):
                continue
            piece = slab(self.full, self.mine[p], {dim: self.where(p, way, step + 1)}, h)
            remote(piece, piece, self.ring_out.at[p], self.ring.at[p, way, step, h], self.partner).wait_recv()
            if step + 1 < steps_of(p, way):
                self.hop(p, way, step + 1, h)
            self.pass_on(p, h, self.where(p, way, step + 1))

    def passed(self, p):
        settle(self.spare, 512, self.passing.at[1, p])


RING_SHAPES = {"x": (2, 8, 4, 8, HD), "y": (4, 2, 4, 8, HD), "z": (4, 8, 8, HD)}
LINE_SHAPES = {"x": (4, 8, HD), "y": (8, 8, HD), "z": (2, 4, 8, HD)}


class Scatter:
    def __init__(self, at, core, part, rings, lines, dot_in, final, total_ref, spare, sems):
        self.at, self.core, self.partner = at, core, device(at, 1 - core)
        self.part, self.rings, self.lines, self.dot_in = part, rings, lines, dot_in
        self.final, self.total_ref = final, total_ref
        self.ring_out, self.ring, self.two, self.three, self.last = sems
        sign = 1 - 2 * core
        self.ways = (sign, -sign)
        self.spare = spare

    def go(self, copy):
        copy.start()

    def target(self, p, way, left):
        dim = RINGS[p]
        return {dim: moved(self.at, dim, self.ways[way] * left)[dim]}

    def copy(self, p, way, step, h):
        dim = RINGS[p]
        return remote(
            out_slab(self.part, p, self.target(p, way, steps_of(p, way) - step), h),
            self.rings[p].at[way, step, h],
            self.ring_out.at[p],
            self.ring.at[p, way, step, h],
            device(moved(self.at, dim, self.ways[way]), self.core),
        )

    def ring_start(self, p):
        for h in range(HALVES):
            for way in range(2):
                self.go(self.copy(p, way, 0, h))

    def ring_step(self, p, h, step):
        for way in range(2):
            if step >= steps_of(p, way):
                continue
            self.copy(p, way, step, h).wait_recv()
            here = out_slab(self.part, p, self.target(p, way, steps_of(p, way) - step - 1), h)
            there = self.rings[p].at[way, step, h]
            here[...] = (here[...].astype(jnp.float32) + there[...].astype(jnp.float32)).astype(jnp.bfloat16)
            if step + 1 < steps_of(p, way):
                self.go(self.copy(p, way, step + 1, h))

    def lines_out(self, p, h):
        a, b, c = ORDERS[p][h]
        for step in range(1, SIZES[b]):
            there = moved(self.at, b, step)
            self.go(
                remote(
                    out_slab(self.part, p, {b: there[b], c: self.at[c]}, h),
                    self.lines[2 * p + h].at[step - 1],
                    self.two.at[6],
                    self.two.at[2 * p + h],
                    device(there, self.core),
                )
            )

    def dots_out(self, p, h):
        a, b, c = ORDERS[p][h]
        lines = self.lines[2 * p + h]
        here = out_slab(self.part, p, {b: self.at[b], c: self.at[c]}, h)
        total = here[...].astype(jnp.float32)
        settle(self.spare, (SIZES[b] - 1) * SIZES[a], self.two.at[2 * p + h])
        for step in range(1, SIZES[b]):
            total = total + lines[step - 1].astype(jnp.float32)
        here[...] = total.astype(jnp.bfloat16)
        for step in range(1, SIZES[a]):
            there = moved(self.at, a, step)
            self.go(
                remote(
                    out_slab(self.part, p, there, h),
                    self.dot_in.at[p, h, step - 1],
                    self.three.at[6],
                    self.three.at[2 * p + h],
                    device(there, self.core),
                )
            )

    def finish(self, p):
        tile = tiles_of(self.core)[p]
        for h in range(HALVES):
            a = ORDERS[p][h][0]
            here = out_slab(self.part, p, self.at, h)
            total = here[...].astype(jnp.float32)
            settle(self.spare, SIZES[a] - 1, self.three.at[2 * p + h])
            for step in range(1, SIZES[a]):
                total = total + self.dot_in[p, h, step - 1].astype(jnp.float32)
            self.final[p, h] = total
        self.total_ref[tile] = self.final[p, self.core]
        self.go(
            remote(
                self.final.at[p, 1 - self.core], self.total_ref.at[tile], self.last.at[0], self.last.at[1], self.partner
            )
        )

    def finished(self, side):
        settle(self.spare, 6, self.last.at[side])

    def settled(self):
        for p in range(3):
            settle(self.spare, 384 if RINGS[p] == "x" else 448, self.ring_out.at[p])
        settle(self.spare, 208, self.two.at[6])
        settle(self.spare, 42, self.three.at[6])
        self.finished(0)


def whole_kernel(
    hidden_ref, mine_ref, gain_ref, cos_ref, sin_ref, cot_ref,
    attn_ref, grad_in_ref, weight_grad_ref, gain_grad_ref,
    full, gain_full, gain_row, normed, turned_own, turned_other,
    kv, probs, part_out, part_in, back, back_other, plain,
    part, ring_0, ring_1, ring_2, line_0, line_1, line_2, line_3, line_4, line_5, dot_in, final, total_ref, mixed, spare,
    g_swap, g_one, g_two, g_out, g_ring, g_pass, g_gain, g_own,
    kv_sem, part_sem, swap_sem, s_out, s_ring, s_two, s_three, s_last,
):
    i, j = lax.axis_index("inter"), lax.axis_index("intra")
    at, core = place()
    partner = device(at, 1 - core)
    barrier = pltpu.get_barrier_semaphore()
    for block in range(8):
        kv[block] = jnp.zeros((2, 128, HD), jnp.bfloat16)
    count = greet(at, core, barrier)
    squares = jnp.zeros((128, 128), jnp.float32)
    for t in range(WIDTH // 128):
        tile = hidden_ref[:, t * 128 : (t + 1) * 128].astype(jnp.float32)
        squares = squares + tile * tile
    inv_rms = lax.rsqrt(jnp.sum(squares, axis=1, keepdims=True) / WIDTH + eps_norm)
    cosine, sine = cos_ref[...], sin_ref[...]
    cots = [cot_ref[:, h * HD : (h + 1) * HD] for h in range(HEADS)]
    pl.semaphore_wait(barrier, count)

    g = Gather(
        at, core, mine_ref, gain_ref, full, gain_full, spare,
        (g_swap, g_one, g_two, g_out, g_ring, g_pass, g_gain, g_own),
    )
    g.begin()
    for p in (1, 2):
        for h in range(HALVES):
            g.arrived(p, h, 0)
            g.direct(p, h, 1)
    g.gain_in(0)
    g.gain_out(1)
    for h in range(HALVES):
        g.arrived(0, h, 0)
        g.direct(0, h, 1)
    for h in range(HALVES):
        for p in (1, 2):
            g.arrived(p, h, 1)
            g.ring_start(p, h)
    g.gain_in(1)
    g.gain_out(2)

    def far(step):
        for h in range(HALVES):
            for p in (1, 2):
                g.ring_step(p, h, step)

    for h in range(HALVES):
        g.arrived(0, h, 1)
        g.ring_start(0, h)
    far(0)
    g.gain_in(2)
    g.gain_pass()
    far(1)
    g.gain_passed()
    for y in range(8):
        for z in range(4):
            t = y * 4 + z
            gain_row[:, t * 128 : (t + 1) * 128] = jnp.sum(gain_full[y, z], axis=(0, 1, 2))
    for t in range(WIDTH // 128):
        cols = slice(t * 128, (t + 1) * 128)
        unit = hidden_ref[:, cols].astype(jnp.float32) * inv_rms * gain_row[:, cols]
        normed[:, cols] = unit.astype(jnp.bfloat16)
    for h in range(HALVES):
        g.ring_step(0, h, 0)
    far(2)
    for t in range(WIDTH // 128):
        cols = slice(t * 128, (t + 1) * 128)
        turned_own[cols, :] = normed[:, cols].T
    for h in range(HALVES):
        g.ring_step(0, h, 1)
    far(3)
    swap = remote(turned_own, turned_other, swap_sem.at[0, 0], swap_sem.at[1, 0], partner)
    swap.start()

    def weight_rows(tiles, y):
        return jnp.concatenate([full[tile, y].reshape(512, HD) for tile in tiles], axis=1)

    def mix(tiles):
        total = jnp.zeros((128, len(tiles) * HD), jnp.float32)
        for y in range(8):
            total = total + across(normed[:, y * 512 : (y + 1) * 512], weight_rows(tiles, y), 1, 0)
        for k, tile in enumerate(tiles):
            mixed[tile] = total[:, k * HD : (k + 1) * HD]

    def rotated(x, sign):
        return x * cosine + sign * (pltpu.roll(x, 64, 1) * sine)

    mix(g.mine[:1])
    g.passed(0)
    mix(g.theirs[:1])
    kv[j, 0] = rotated(mixed[4], 1.0).astype(jnp.bfloat16)
    kv[j, 1] = mixed[5].astype(jnp.bfloat16)

    def kv_copy(owner, peer):
        return remote(kv.at[owner], kv.at[owner], kv_sem.at[0, peer], kv_sem.at[1, owner], (i, peer))

    for peer in range(1, 8):
        @pl.when(j < peer)
        def _():
            kv_copy(j, peer).start()

    scale = HD ** (-0.5)
    mix(g.mine[1:])
    g.passed(1)
    g.passed(2)
    mix(g.theirs[1:])
    queries = [(rotated(mixed[h], 1.0) * scale).astype(jnp.bfloat16) for h in range(HEADS)]
    query = jnp.concatenate(queries, axis=0)
    query_t = jnp.concatenate([q.T for q in queries], axis=1)
    cot = jnp.concatenate(cots, axis=0)
    cot_t = jnp.concatenate([c.T for c in cots], axis=1)
    row_pos = j * 128 + lax.broadcasted_iota(jnp.int32, (CHUNK, FLAT), 1) % 128
    key_pos = lax.broadcasted_iota(jnp.int32, (CHUNK, FLAT), 0)

    def allowed(chunk):
        return key_pos + chunk * CHUNK <= row_pos

    def rows(chunk, which):
        return jnp.concatenate([kv[chunk * BLOCKS + b, which] for b in range(BLOCKS)], axis=0)

    for owner in range(7):
        @pl.when(owner < j)
        def _():
            kv_copy(owner, j).wait_recv()

    top = jnp.full((1, FLAT), -1e30, jnp.float32)
    for chunk in range(CHUNKS):
        scores = jnp.where(allowed(chunk), across(rows(chunk, 0), query_t, 1, 0), -1e30)
        probs[chunk] = scores
        top = jnp.maximum(top, jnp.max(scores, axis=0, keepdims=True))
    total = jnp.zeros((1, FLAT), jnp.float32)
    out_t = jnp.zeros((HD, FLAT), jnp.float32)
    for chunk in range(CHUNKS):
        numbers = jnp.exp(probs[chunk] - top)
        probs[chunk] = numbers
        total = total + jnp.sum(numbers, axis=0, keepdims=True)
        out_t = out_t + across(rows(chunk, 1), numbers.astype(jnp.bfloat16), 0, 0)
    share = 1.0 / total
    attn_t = (out_t * share).astype(jnp.bfloat16)
    delta = jnp.sum(cot_t.astype(jnp.float32) * attn_t.astype(jnp.float32), axis=0, keepdims=True)
    query_grad_t = jnp.zeros((HD, FLAT), jnp.float32)

    def part_copy(owner, maker):
        return remote(part_out.at[owner], part_in.at[maker], part_sem.at[0, owner], part_sem.at[1, maker], (i, owner))

    def send_parts(chunk):
        for b in range(BLOCKS):
            owner = chunk * BLOCKS + b

            @pl.when(owner < j)
            def _():
                part_copy(owner, j).start()

    for chunk in range(CHUNKS):
        probs_t = probs[chunk] * share
        probs_grad = across(rows(chunk, 1), cot_t, 1, 0)
        scores_grad = (probs_t * (probs_grad - delta)).astype(jnp.bfloat16)
        keys_part = across(scores_grad, query, 1, 0).astype(jnp.bfloat16)
        values_part = across(probs_t.astype(jnp.bfloat16), cot, 1, 0).astype(jnp.bfloat16)
        for b in range(BLOCKS):
            part_out[chunk * BLOCKS + b, 0] = keys_part[b * 128 : (b + 1) * 128]
            part_out[chunk * BLOCKS + b, 1] = values_part[b * 128 : (b + 1) * 128]
        query_grad_t = query_grad_t + across(rows(chunk, 0), scores_grad, 0, 0)
        send_parts(chunk)
    for h in range(HEADS):
        grad = query_grad_t[:, h * 128 : (h + 1) * 128].T
        back[h] = (rotated(grad, -1.0) * scale).astype(jnp.bfloat16)

    def swap_back(first, count, slot):
        return remote(
            back.at[pl.ds(first, count)], back_other.at[pl.ds(slot, count)], swap_sem.at[0, 1 + slot],
            swap_sem.at[1, 1 + slot], partner,
        )

    swap_heads = swap_back(2 * (1 - core), 2, 0)
    swap_heads.start()
    for h in range(HEADS):
        attn_ref[:, h * HD : (h + 1) * HD] = attn_t[:, h * 128 : (h + 1) * 128].T
    swap.wait_recv()
    swap_heads.wait_recv()

    def products(ps):
        own = jnp.concatenate([back[g.mine[p]] for p in ps], axis=1)
        other = jnp.concatenate([back_other[(p + 2) % 3] for p in ps], axis=1)
        both = jnp.concatenate([own, other], axis=0)
        for k in range(8):
            chosen = slice(k * 512, (k + 1) * 512)
            left = jnp.concatenate([turned_own[chosen, :], turned_other[chosen, :]], axis=1)
            sums = across(left, both, 1, 0)
            for n, p in enumerate(ps):
                part[p, k // 2, k % 2] = sums[:, n * HD : (n + 1) * HD].reshape(8, 4, 2, 8, HD).astype(jnp.bfloat16)

    s = Scatter(
        at, core, part, (ring_0, ring_1, ring_2), (line_0, line_1, line_2, line_3, line_4, line_5), dot_in, final,
        total_ref, spare, (s_out, s_ring, s_two, s_three, s_last),
    )
    products((1, 2))
    s.ring_start(1)
    s.ring_start(2)
    part_in[j] = part_out[j]
    keys_grad = jnp.zeros((128, HD), jnp.float32)
    values_grad = jnp.zeros((128, HD), jnp.float32)
    for maker in range(8):
        @pl.when(maker > j)
        def _():
            part_copy(j, maker).wait_recv()

        @pl.when(maker < j)
        def _():
            part_in[maker] = jnp.zeros((2, 128, HD), jnp.bfloat16)

        keys_grad = keys_grad + part_in[maker, 0].astype(jnp.float32)
        values_grad = values_grad + part_in[maker, 1].astype(jnp.float32)
    back[4] = rotated(keys_grad, -1.0).astype(jnp.bfloat16)
    back[5] = values_grad.astype(jnp.bfloat16)

    swap_last = swap_back(5 - core, 1, 2)
    swap_last.start()
    pairs = [jnp.concatenate([back[2 * pair], back[2 * pair + 1]], axis=1) for pair in range(3)]
    swap_last.wait_recv()
    products((0,))
    s.ring_start(0)
    g.settled()

    def plain_rows(y, inner):
        cols = slice(y * 512, (y + 1) * 512)
        grad = sum(across(pairs[pair], weight_rows((2 * pair, 2 * pair + 1), y), 1, 1) for pair in range(3))
        grad = grad * gain_row[:, cols]
        plain[:, cols] = grad
        return inner + jnp.sum(grad * hidden_ref[:, cols].astype(jnp.float32), axis=1, keepdims=True)

    inner = jnp.zeros((128, 1), jnp.float32)

    def both(step):
        for h in range(HALVES):
            for p in (1, 2):
                s.ring_step(p, h, step)

    both(0)
    for y in (0, 1, 2, 3):
        inner = plain_rows(y, inner)
    both(1)
    s.ring_step(0, 0, 0)
    for y in (4, 5, 6, 7):
        inner = plain_rows(y, inner)
    both(2)
    s.ring_step(0, 1, 0)
    fall = inv_rms * inv_rms * inv_rms * (1.0 / WIDTH) * inner
    for y in range(8):
        cols = slice(y * 512, (y + 1) * 512)
        grad_in_ref[:, cols] = (
            plain[:, cols] * inv_rms - hidden_ref[:, cols].astype(jnp.float32) * fall
        ).astype(jnp.bfloat16)
    s.ring_step(0, 0, 1)
    s.lines_out(0, 0)
    for h in range(HALVES):
        for p in (1, 2):
            s.ring_step(p, h, 3)
            s.lines_out(p, h)
    s.ring_step(0, 1, 1)
    s.lines_out(0, 1)
    for h in range(HALVES):
        for p in (1, 2):
            s.dots_out(p, h)
    for h in range(HALVES):
        s.dots_out(0, h)
    s.finish(1)
    s.finish(2)
    s.finish(0)
    s.finished(1)
    inside = (j, i // 16, (i // 8) % 2, (i // 2) % 4, i % 2)
    sums = jnp.zeros((8, HD), jnp.float32)
    for n in range(TILES):
        tile = total_ref[n]
        weight_grad_ref[:, n * HD : (n + 1) * HD] = tile
        sums = sums + tile * full[(n, *inside)].astype(jnp.float32)
    lane = lax.broadcasted_iota(jnp.int32, (8, 128), 1)
    row = lax.broadcasted_iota(jnp.int32, (8, 128), 0)
    gains = jnp.sum(jnp.where(lane % 8 == row, gain_full[inside], 0.0), axis=1, keepdims=True)
    answer = jnp.sum(sums, axis=1, keepdims=True) / gains
    gain_grad_ref[...] = jnp.sum(jnp.where(lane == row, answer, 0.0), axis=0, keepdims=True)

    for peer in range(1, 8):
        @pl.when(j < peer)
        def _():
            kv_copy(j, peer).wait_send()

    for owner in range(7):
        @pl.when(owner < j)
        def _():
            part_copy(owner, j).wait_send()

    for copy in (swap, swap_heads, swap_last):
        copy.wait_send()
    s.settled()


def whole(hidden, tiles, gain_piece, cosine, sine, cot):
    dma = pltpu.SemaphoreType.DMA
    vmem = pl.BlockSpec(memory_space=pltpu.VMEM)
    low, wide = jnp.bfloat16, jnp.float32

    def rings(p):
        dim = RINGS[p]
        return pltpu.VMEM((2, SIZES[dim] // 2, HALVES, *RING_SHAPES[dim]), low)

    def lines(p, h):
        return pltpu.VMEM((SIZES[ORDERS[p][h][1]] - 1, *LINE_SHAPES[ORDERS[p][h][0]]), low)

    return pl.pallas_call(
        whole_kernel,
        out_shape=(
            jax.ShapeDtypeStruct((128, FLAT), low),
            jax.ShapeDtypeStruct((128, WIDTH), low),
            jax.ShapeDtypeStruct((8, TILES * HD), wide),
            jax.ShapeDtypeStruct((1, 128), wide),
        ),
        in_specs=[vmem] * 6,
        out_specs=(vmem,) * 4,
        scratch_shapes=[
            pltpu.VMEM((TILES, 8, 4, 2, 4, 2, 8, HD), low),
            pltpu.VMEM((8, 4, 2, 4, 2, 1, 128), wide),
            pltpu.VMEM((1, WIDTH), wide),
            pltpu.VMEM((128, WIDTH), low),
            pltpu.VMEM((WIDTH, 128), low),
            pltpu.VMEM((WIDTH, 128), low),
            pltpu.VMEM((8, 2, 128, HD), low),
            pltpu.VMEM((CHUNKS, CHUNK, FLAT), wide),
            pltpu.VMEM((8, 2, 128, HD), low),
            pltpu.VMEM((8, 2, 128, HD), low),
            pltpu.VMEM((TILES, 128, HD), low),
            pltpu.VMEM((3, 128, HD), low),
            pltpu.VMEM((128, WIDTH), wide),
            pltpu.VMEM((3, 4, 2, 8, 4, 2, 8, HD), low),
            *[rings(p) for p in range(3)],
            *[lines(p, h) for p in range(3) for h in range(HALVES)],
            pltpu.VMEM((3, HALVES, 7, 8, HD), low),
            pltpu.VMEM((3, 2, 8, HD), wide),
            pltpu.VMEM((TILES, 8, HD), wide),
            pltpu.VMEM((TILES, 128, HD), wide),
            pltpu.VMEM((512, 8, HD), low),
            dma((2,)),
            dma((7,)),
            dma((7,)),
            dma((3,)),
            dma((3, 2, 4, HALVES)),
            dma((2, 3)),
            dma((2, 4)),
            dma((4,)),
            dma((2, 8)),
            dma((2, 8)),
            dma((2, 4)),
            dma((3,)),
            dma((3, 2, 4, HALVES)),
            dma((7,)),
            dma((7,)),
            dma((2,)),
        ],
        compiler_params=pltpu.CompilerParams(collective_id=0, has_side_effects=True, vmem_limit_bytes=40 * 2**20),
        name="whole",
    )(hidden, tiles, gain_piece, cosine, sine, cot)


def rope_tables(first_position):
    freqs = rope_base ** (-jnp.arange(HD // 2, dtype=jnp.float32) / (HD // 2))
    positions = first_position + jnp.arange(128, dtype=jnp.int32)
    angles = positions.astype(jnp.float32)[:, None] * freqs[None, :]
    cosine, sine = jnp.cos(angles), jnp.sin(angles)
    return jnp.concatenate([cosine, cosine], axis=1), jnp.concatenate([-sine, sine], axis=1)


def local(hidden_in, norm_gain, qkv_weight, attn_cotangent):
    i, j = lax.axis_index("inter"), lax.axis_index("intra")
    tiles = jnp.moveaxis(qkv_weight.reshape(8, TILES, HD), 1, 0)
    lane = jnp.arange(128)
    gain_piece = jnp.where(lane // 8 == (i * 8 + j) % 16, jnp.tile(norm_gain.astype(jnp.float32), 16), 0.0)[None]
    cosine, sine = rope_tables(j * 128)
    attn, grad_in, weight_grad, gain_grad = whole(hidden_in[0], tiles, gain_piece, cosine, sine, attn_cotangent[0])
    return (attn[None], grad_in[None], weight_grad, gain_grad[0, :8])


def solution(mesh):
    return jax.shard_map(
        local,
        mesh=mesh,
        in_specs=(
            P("inter", "intra", None),
            P(("inter", "intra")),
            P(("inter", "intra"), None),
            P("inter", "intra", None),
        ),
        out_specs=(
            P("inter", "intra", None),
            P("inter", "intra", None),
            P(("intra", "inter"), None),
            P(("intra", "inter")),
        ),
        check_vma=False,
    )
```

```python
import jax
import jax.numpy as jnp
import numpy as np
from jax import lax
from jax.experimental import pallas as pl
from jax.experimental.pallas import tpu as pltpu
from jax.sharding import PartitionSpec as P

HD = 128
HEADS = 4
TILES = HEADS + 2
WIDTH = 4096
MESH = pl.DeviceIdType.MESH
SIZES = {"x": 4, "y": 8, "z": 8}
ORDERS = (
    (("z", "y", "x"), ("y", "z", "x")),
    (("z", "x", "y"), ("z", "x", "y")),
    (("y", "x", "z"), ("y", "x", "z")),
)
RINGS = ("x", "y", "z")
HALVES = 2
GAIN_ORDER = ("z", "y", "x")
CHUNK = 256
CHUNKS = 1024 // CHUNK
BLOCKS = CHUNK // 128
FLAT = HEADS * 128

eps_norm = 1e-05
rope_base = 500000.0


def place():
    i, j = lax.axis_index("inter"), lax.axis_index("intra")
    return {"x": j // 2, "y": i // 8, "z": ((i // 2) % 4) * 2 + j % 2}, i % 2


def device(at, core):
    return ((at["y"] * 4 + at["z"] // 2) * 2 + core, at["x"] * 2 + at["z"] % 2)


def moved(at, dim, step):
    size = SIZES[dim]
    return {**at, dim: (at[dim] + step + size) % size}


def indices(at):
    every = slice(None)
    y, x = at.get("y", every), at.get("x", every)
    high, low = (at["z"] // 2, at["z"] % 2) if "z" in at else (every, every)
    return y, high, x, low


def slab(ref, tile, at, cores=slice(None)):
    y, high, x, low = indices(at)
    return ref.at[tile, y, high, cores, x, low]


def gain_slab(ref, at, cores):
    y, high, x, low = indices(at)
    return ref.at[y, high, cores, x, low]


def out_slab(ref, tile, at, cores=slice(None)):
    y, high, x, low = indices(at)
    return ref.at[tile, x, low, y, high, cores]


def remote(src, dst, send, recv, peer):
    return pltpu.make_async_remote_copy(
        src_ref=src, dst_ref=dst, send_sem=send, recv_sem=recv, device_id=peer, device_id_type=MESH
    )


def across(left, right, left_dim, right_dim):
    return lax.dot_general(
        left, right, (((left_dim,), (right_dim,)), ((), ())), preferred_element_type=jnp.float32
    )


def steps_of(p, way):
    return SIZES[RINGS[p]] // 2 - way


def tiles_of(core):
    return [4 + core, 2 * core, 2 * core + 1]


def settle(spare, count, sem):
    pltpu.make_async_copy(spare.at[pl.ds(0, count)], spare.at[pl.ds(0, count)], sem).wait()


def greet(at, core, barrier):
    i, j = lax.axis_index("inter"), lax.axis_index("intra")
    peers = [device(at, 1 - core)]
    for dim, size in SIZES.items():
        peers += [device(moved(at, dim, step), core) for step in range(1, size)]
    peers += [(i, (j + step) % 8) for step in range(1, 8)]
    for peer in peers:
        pl.semaphore_signal(barrier, inc=1, device_id=peer, device_id_type=MESH)
    return len(peers)


class Gather:
    def __init__(self, at, core, mine_ref, gain_ref, full, gain_full, spare, sems):
        self.at, self.core, self.partner = at, core, device(at, 1 - core)
        self.mine_ref, self.gain_ref, self.full, self.gain_full = mine_ref, gain_ref, full, gain_full
        (self.swap, self.one, self.two, self.item, self.side, self.ring_out, self.ring, self.passing, self.gains, self.own) = sems
        self.mine, self.theirs = tiles_of(core), tiles_of(1 - core)
        sign = 1 - 2 * core
        self.ways = (sign, -sign)
        self.spare = spare

    def go(self, copy):
        copy.start()

    def begin(self):
        at, core, full = self.at, self.core, self.full
        owns = []
        for p in range(3):
            self.go(
                remote(
                    self.mine_ref.at[self.theirs[p]],
                    slab(full, self.theirs[p], at, core),
                    self.swap.at[0],
                    self.swap.at[1],
                    self.partner,
                )
            )
            owns.append(
                pltpu.make_async_copy(self.mine_ref.at[self.mine[p]], slab(full, self.mine[p], at, core), self.own.at[p])
            )
        owns.append(pltpu.make_async_copy(self.gain_ref, gain_slab(self.gain_full, at, core), self.own.at[3]))
        for own in owns:
            own.start()
        for own in owns:
            own.wait()
        self.gain_out(0)
        settle(self.spare, 3, self.swap.at[1])
        for p in (1, 2, 0):
            for h in range(HALVES):
                self.direct(p, h, 0)

    def direct(self, p, h, phase):
        order = ORDERS[p][h]
        sems = (self.one, self.two)[phase]
        src = slab(self.full, self.mine[p], {d: self.at[d] for d in order[phase:]}, h)
        for step in range(1, SIZES[order[phase]]):
            peer = device(moved(self.at, order[phase], step), self.core)
            recv = self.item.at[h, step - 1] if p == 0 and phase == 1 else sems.at[2 * p + h]
            self.go(remote(src, src, sems.at[6], recv, peer))

    def along(self, h, step):
        middle = ORDERS[0][h][1]
        if step:
            settle(self.spare, 8, self.item.at[h, step - 1])
        known = moved({d: self.at[d] for d in (middle, "x")}, middle, -step)
        src = slab(self.full, self.mine[0], known, h)
        for k in (1, 3, 2):
            peer = device(moved(self.at, "x", k), self.core)
            self.go(remote(src, src, self.ring_out.at[0], self.side.at[h, k - 1], peer))

    def beside(self, h):
        for k in (1, 3, 2):
            settle(self.spare, 64, self.side.at[h, k - 1])
            self.pass_on(0, h, moved(self.at, "x", -k)["x"])

    def arrived(self, p, h, phase):
        order = ORDERS[p][h]
        sems = (self.one, self.two)[phase]
        each = 1 if phase == 0 else SIZES[order[0]]
        settle(self.spare, (SIZES[order[phase]] - 1) * each, sems.at[2 * p + h])

    def gain_out(self, phase):
        dim = GAIN_ORDER[phase]
        src = gain_slab(self.gain_full, {d: self.at[d] for d in GAIN_ORDER[phase:]}, self.core)
        for step in range(1, SIZES[dim]):
            peer = device(moved(self.at, dim, step), self.core)
            self.go(remote(src, src, self.gains.at[0, phase], self.gains.at[1, phase], peer))

    def gain_wait(self, phase, side):
        rows = (
            self.gain_full.at[pl.ds(0, 7), 0, 0, 0, 0],
            self.gain_full.at[pl.ds(0, 7), :, :, 0, 0],
            self.gain_full.at[pl.ds(0, 6), :, :, :, 0],
            self.gain_full.at[:, :, 0],
        )[phase]
        pltpu.make_async_copy(rows, rows, self.gains.at[side, phase]).wait()

    def gain_in(self, phase):
        self.gain_wait(phase, 1)

    def gain_pass(self):
        whole = gain_slab(self.gain_full, {}, self.core)
        self.go(remote(whole, whole, self.gains.at[0, 3], self.gains.at[1, 3], self.partner))

    def gain_passed(self):
        self.gain_wait(3, 1)

    def settled(self):
        settle(self.spare, 3, self.swap.at[0])
        settle(self.spare, 42, self.one.at[6])
        settle(self.spare, 208, self.two.at[6])
        for p in range(3):
            settle(self.spare, 384 if RINGS[p] == "x" else 448, self.ring_out.at[p])
            settle(self.spare, 512, self.passing.at[0, p])
        for phase in range(4):
            self.gain_wait(phase, 0)

    def where(self, p, way, step):
        dim = RINGS[p]
        return moved(self.at, dim, -self.ways[way] * step)[dim]

    def hop(self, p, way, step, h):
        dim = RINGS[p]
        piece = slab(self.full, self.mine[p], {dim: self.where(p, way, step)}, h)
        peer = device(moved(self.at, dim, self.ways[way]), self.core)
        self.go(remote(piece, piece, self.ring_out.at[p], self.ring.at[p - 1, way, step, h], peer))

    def pass_on(self, p, h, where):
        piece = slab(self.full, self.mine[p], {RINGS[p]: where}, h)
        self.go(remote(piece, piece, self.passing.at[0, p], self.passing.at[1, p], self.partner))

    def ring_start(self, p, h):
        for way in range(2):
            self.hop(p, way, 0, h)
        self.pass_on(p, h, self.at[RINGS[p]])

    def ring_step(self, p, h, step):
        dim = RINGS[p]
        for way in range(2):
            if step >= steps_of(p, way):
                continue
            piece = slab(self.full, self.mine[p], {dim: self.where(p, way, step + 1)}, h)
            remote(piece, piece, self.ring_out.at[p], self.ring.at[p - 1, way, step, h], self.partner).wait_recv()
            if step + 1 < steps_of(p, way):
                self.hop(p, way, step + 1, h)
            self.pass_on(p, h, self.where(p, way, step + 1))

    def passed(self, p):
        settle(self.spare, 512, self.passing.at[1, p])


RING_SHAPES = {"x": (2, 8, 4, 8, HD), "y": (4, 2, 4, 8, HD), "z": (4, 8, 8, HD)}
LINE_SHAPES = {"x": (4, 8, HD), "y": (8, 8, HD), "z": (2, 4, 8, HD)}


class Scatter:
    def __init__(self, at, core, part, rings, lines, dot_in, final, total_ref, spare, sems):
        self.at, self.core, self.partner = at, core, device(at, 1 - core)
        self.part, self.rings, self.lines, self.dot_in = part, rings, lines, dot_in
        self.final, self.total_ref = final, total_ref
        self.ring_out, self.ring, self.two, self.three, self.last = sems
        sign = 1 - 2 * core
        self.ways = (sign, -sign)
        self.spare = spare

    def go(self, copy):
        copy.start()

    def target(self, p, way, left):
        dim = RINGS[p]
        return {dim: moved(self.at, dim, self.ways[way] * left)[dim]}

    def copy(self, p, way, step, h):
        dim = RINGS[p]
        return remote(
            out_slab(self.part, p, self.target(p, way, steps_of(p, way) - step), h),
            self.rings[p].at[way, step, h],
            self.ring_out.at[p],
            self.ring.at[p, way, step, h],
            device(moved(self.at, dim, self.ways[way]), self.core),
        )

    def ring_start(self, p):
        for h in range(HALVES):
            for way in range(2):
                self.go(self.copy(p, way, 0, h))

    def ring_step(self, p, h, step):
        for way in range(2):
            if step >= steps_of(p, way):
                continue
            self.copy(p, way, step, h).wait_recv()
            here = out_slab(self.part, p, self.target(p, way, steps_of(p, way) - step - 1), h)
            there = self.rings[p].at[way, step, h]
            here[...] = (here[...].astype(jnp.float32) + there[...].astype(jnp.float32)).astype(jnp.bfloat16)
            if step + 1 < steps_of(p, way):
                self.go(self.copy(p, way, step + 1, h))

    def lines_out(self, p, h):
        a, b, c = ORDERS[p][h]
        for step in range(1, SIZES[b]):
            there = moved(self.at, b, step)
            self.go(
                remote(
                    out_slab(self.part, p, {b: there[b], c: self.at[c]}, h),
                    self.lines[2 * p + h].at[step - 1],
                    self.two.at[6],
                    self.two.at[2 * p + h],
                    device(there, self.core),
                )
            )

    def dots_out(self, p, h):
        a, b, c = ORDERS[p][h]
        lines = self.lines[2 * p + h]
        here = out_slab(self.part, p, {b: self.at[b], c: self.at[c]}, h)
        total = here[...].astype(jnp.float32)
        settle(self.spare, (SIZES[b] - 1) * SIZES[a], self.two.at[2 * p + h])
        for step in range(1, SIZES[b]):
            total = total + lines[step - 1].astype(jnp.float32)
        here[...] = total.astype(jnp.bfloat16)
        for step in range(1, SIZES[a]):
            there = moved(self.at, a, step)
            self.go(
                remote(
                    out_slab(self.part, p, there, h),
                    self.dot_in.at[p, h, step - 1],
                    self.three.at[6],
                    self.three.at[2 * p + h],
                    device(there, self.core),
                )
            )

    def finish(self, p):
        tile = tiles_of(self.core)[p]
        for h in range(HALVES):
            a = ORDERS[p][h][0]
            here = out_slab(self.part, p, self.at, h)
            total = here[...].astype(jnp.float32)
            settle(self.spare, SIZES[a] - 1, self.three.at[2 * p + h])
            for step in range(1, SIZES[a]):
                total = total + self.dot_in[p, h, step - 1].astype(jnp.float32)
            self.final[p, h] = total
        self.total_ref[tile] = self.final[p, self.core]
        self.go(
            remote(
                self.final.at[p, 1 - self.core], self.total_ref.at[tile], self.last.at[0], self.last.at[1], self.partner
            )
        )

    def finished(self, side):
        settle(self.spare, 6, self.last.at[side])

    def settled(self):
        for p in range(3):
            settle(self.spare, 384 if RINGS[p] == "x" else 448, self.ring_out.at[p])
        settle(self.spare, 208, self.two.at[6])
        settle(self.spare, 42, self.three.at[6])
        self.finished(0)


def whole_kernel(
    hidden_in, mine_ref, gain_ref, tables_in, cot_in,
    attn_ref, grad_in_ref, weight_grad_ref, gain_grad_ref,
    full, gain_full, gain_row, normed, turned_own, turned_other,
    kv, probs, part_out, part_in, back, back_other, plain,
    part, ring_0, ring_1, ring_2, line_0, line_1, line_2, line_3, line_4, line_5, dot_in, final, total_ref, mixed, spare, hidden_ref, tables, cot_ref, load_sem,
    g_swap, g_one, g_two, g_item, g_side, g_out, g_ring, g_pass, g_gain, g_own,
    kv_sem, part_sem, swap_sem, s_out, s_ring, s_two, s_three, s_last,
):
    i, j = lax.axis_index("inter"), lax.axis_index("intra")
    at, core = place()
    partner = device(at, 1 - core)
    barrier = pltpu.get_barrier_semaphore()
    loads = [
        pltpu.make_async_copy(hidden_in, hidden_ref, load_sem.at[0]),
        pltpu.make_async_copy(cot_in, cot_ref, load_sem.at[1]),
        pltpu.make_async_copy(tables_in.at[j], tables, load_sem.at[2]),
    ]
    for load in loads:
        load.start()
    for block in range(8):
        kv[block] = jnp.zeros((2, 128, HD), jnp.bfloat16)
    count = greet(at, core, barrier)
    for load in loads:
        load.wait()
    squares = jnp.zeros((128, 128), jnp.float32)
    for t in range(WIDTH // 128):
        tile = hidden_ref[:, t * 128 : (t + 1) * 128].astype(jnp.float32)
        squares = squares + tile * tile
    inv_rms = lax.rsqrt(jnp.sum(squares, axis=1, keepdims=True) / WIDTH + eps_norm)
    cosine, sine = tables[0], tables[1]
    cots = [cot_ref[:, h * HD : (h + 1) * HD] for h in range(HEADS)]
    pl.semaphore_wait(barrier, count)

    g = Gather(
        at, core, mine_ref, gain_ref, full, gain_full, spare,
        (g_swap, g_one, g_two, g_item, g_side, g_out, g_ring, g_pass, g_gain, g_own),
    )
    g.begin()
    for p in (1, 2):
        for h in range(HALVES):
            g.arrived(p, h, 0)
            g.direct(p, h, 1)
    g.gain_in(0)
    g.gain_out(1)
    for h in range(HALVES):
        g.arrived(0, h, 0)
        g.direct(0, h, 1)
    for h in range(HALVES):
        g.along(h, 0)

    def along(*steps):
        for step in steps:
            for h in range(HALVES):
                g.along(h, step)

    def begin_far(h):
        for p in (1, 2):
            g.arrived(p, h, 1)
            g.ring_start(p, h)

    def far(step):
        for h in range(HALVES):
            for p in (1, 2):
                g.ring_step(p, h, step)

    begin_far(0)
    along(1, 7)
    begin_far(1)
    along(2, 6)
    g.gain_in(1)
    g.gain_out(2)
    along(3, 5, 4)
    for h in range(HALVES):
        g.pass_on(0, h, at["x"])
    far(0)
    g.gain_in(2)
    g.gain_pass()
    far(1)
    g.gain_passed()
    for y in range(8):
        for z in range(4):
            t = y * 4 + z
            gain_row[:, t * 128 : (t + 1) * 128] = jnp.sum(gain_full[y, z], axis=(0, 1, 2))
    for t in range(WIDTH // 128):
        cols = slice(t * 128, (t + 1) * 128)
        unit = hidden_ref[:, cols].astype(jnp.float32) * inv_rms * gain_row[:, cols]
        normed[:, cols] = unit.astype(jnp.bfloat16)
    far(2)
    for h in range(HALVES):
        g.beside(h)

    def weight_rows(tiles, y):
        return jnp.concatenate([full[tile, y].reshape(512, HD) for tile in tiles], axis=1)

    def mix(tiles):
        total = jnp.zeros((128, len(tiles) * HD), jnp.float32)
        for y in range(8):
            total = total + across(normed[:, y * 512 : (y + 1) * 512], weight_rows(tiles, y), 1, 0)
        for k, tile in enumerate(tiles):
            mixed[tile] = total[:, k * HD : (k + 1) * HD]

    def rotated(x, sign):
        return x * cosine + sign * (pltpu.roll(x, 64, 1) * sine)

    mix(g.mine[:1])
    g.passed(0)
    mix(g.theirs[:1])
    kv[j, 0] = rotated(mixed[4], 1.0).astype(jnp.bfloat16)
    kv[j, 1] = mixed[5].astype(jnp.bfloat16)

    def kv_copy(owner, peer):
        return remote(kv.at[owner], kv.at[owner], kv_sem.at[0, peer], kv_sem.at[1, owner], (i, peer))

    for peer in range(1, 8):
        @pl.when(j < peer)
        def _():
            kv_copy(j, peer).start()

    scale = HD ** (-0.5)
    far(3)
    for t in range(WIDTH // 128):
        cols = slice(t * 128, (t + 1) * 128)
        turned_own[cols, :] = normed[:, cols].T
    swap = remote(turned_own, turned_other, swap_sem.at[0, 0], swap_sem.at[1, 0], partner)
    swap.start()
    mix(g.mine[1:])
    g.passed(1)
    g.passed(2)
    mix(g.theirs[1:])
    queries = [(rotated(mixed[h], 1.0) * scale).astype(jnp.bfloat16) for h in range(HEADS)]
    query = jnp.concatenate(queries, axis=0)
    query_t = jnp.concatenate([q.T for q in queries], axis=1)
    cot = jnp.concatenate(cots, axis=0)
    cot_t = jnp.concatenate([c.T for c in cots], axis=1)
    row_pos = j * 128 + lax.broadcasted_iota(jnp.int32, (CHUNK, FLAT), 1) % 128
    key_pos = lax.broadcasted_iota(jnp.int32, (CHUNK, FLAT), 0)

    def allowed(chunk):
        return key_pos + chunk * CHUNK <= row_pos

    def rows(chunk, which):
        return jnp.concatenate([kv[chunk * BLOCKS + b, which] for b in range(BLOCKS)], axis=0)

    for owner in range(7):
        @pl.when(owner < j)
        def _():
            kv_copy(owner, j).wait_recv()

    top = jnp.full((1, FLAT), -1e30, jnp.float32)
    for chunk in range(CHUNKS):
        scores = jnp.where(allowed(chunk), across(rows(chunk, 0), query_t, 1, 0), -1e30)
        probs[chunk] = scores
        top = jnp.maximum(top, jnp.max(scores, axis=0, keepdims=True))
    total = jnp.zeros((1, FLAT), jnp.float32)
    out_t = jnp.zeros((HD, FLAT), jnp.float32)
    for chunk in range(CHUNKS):
        numbers = jnp.exp(probs[chunk] - top)
        probs[chunk] = numbers
        total = total + jnp.sum(numbers, axis=0, keepdims=True)
        out_t = out_t + across(rows(chunk, 1), numbers.astype(jnp.bfloat16), 0, 0)
    share = 1.0 / total
    attn_t = (out_t * share).astype(jnp.bfloat16)
    delta = jnp.sum(cot_t.astype(jnp.float32) * attn_t.astype(jnp.float32), axis=0, keepdims=True)
    query_grad_t = jnp.zeros((HD, FLAT), jnp.float32)

    def part_copy(owner, maker):
        return remote(part_out.at[owner], part_in.at[maker], part_sem.at[0, owner], part_sem.at[1, maker], (i, owner))

    def send_parts(chunk):
        for b in range(BLOCKS):
            owner = chunk * BLOCKS + b

            @pl.when(owner < j)
            def _():
                part_copy(owner, j).start()

    for chunk in range(CHUNKS):
        probs_t = probs[chunk] * share
        probs_grad = across(rows(chunk, 1), cot_t, 1, 0)
        scores_grad = (probs_t * (probs_grad - delta)).astype(jnp.bfloat16)
        keys_part = across(scores_grad, query, 1, 0).astype(jnp.bfloat16)
        values_part = across(probs_t.astype(jnp.bfloat16), cot, 1, 0).astype(jnp.bfloat16)
        for b in range(BLOCKS):
            part_out[chunk * BLOCKS + b, 0] = keys_part[b * 128 : (b + 1) * 128]
            part_out[chunk * BLOCKS + b, 1] = values_part[b * 128 : (b + 1) * 128]
        query_grad_t = query_grad_t + across(rows(chunk, 0), scores_grad, 0, 0)
        send_parts(chunk)
    for h in range(HEADS):
        grad = query_grad_t[:, h * 128 : (h + 1) * 128].T
        back[h] = (rotated(grad, -1.0) * scale).astype(jnp.bfloat16)

    def swap_back(first, count, slot):
        return remote(
            back.at[pl.ds(first, count)], back_other.at[pl.ds(slot, count)], swap_sem.at[0, 1 + slot],
            swap_sem.at[1, 1 + slot], partner,
        )

    swap_heads = swap_back(2 * (1 - core), 2, 0)
    swap_heads.start()
    for h in range(HEADS):
        attn_ref[:, h * HD : (h + 1) * HD] = attn_t[:, h * 128 : (h + 1) * 128].T
    swap.wait_recv()
    swap_heads.wait_recv()

    def products(ps):
        own = jnp.concatenate([back[g.mine[p]] for p in ps], axis=1)
        other = jnp.concatenate([back_other[(p + 2) % 3] for p in ps], axis=1)
        both = jnp.concatenate([own, other], axis=0)
        for k in range(8):
            chosen = slice(k * 512, (k + 1) * 512)
            left = jnp.concatenate([turned_own[chosen, :], turned_other[chosen, :]], axis=1)
            sums = across(left, both, 1, 0)
            for n, p in enumerate(ps):
                part[p, k // 2, k % 2] = sums[:, n * HD : (n + 1) * HD].reshape(8, 4, 2, 8, HD).astype(jnp.bfloat16)

    s = Scatter(
        at, core, part, (ring_0, ring_1, ring_2), (line_0, line_1, line_2, line_3, line_4, line_5), dot_in, final,
        total_ref, spare, (s_out, s_ring, s_two, s_three, s_last),
    )
    products((1, 2))
    s.ring_start(1)
    s.ring_start(2)
    part_in[j] = part_out[j]
    keys_grad = jnp.zeros((128, HD), jnp.float32)
    values_grad = jnp.zeros((128, HD), jnp.float32)
    for maker in range(8):
        @pl.when(maker > j)
        def _():
            part_copy(j, maker).wait_recv()

        @pl.when(maker < j)
        def _():
            part_in[maker] = jnp.zeros((2, 128, HD), jnp.bfloat16)

        keys_grad = keys_grad + part_in[maker, 0].astype(jnp.float32)
        values_grad = values_grad + part_in[maker, 1].astype(jnp.float32)
    back[4] = rotated(keys_grad, -1.0).astype(jnp.bfloat16)
    back[5] = values_grad.astype(jnp.bfloat16)

    def both(step):
        for h in range(HALVES):
            for p in (1, 2):
                s.ring_step(p, h, step)

    swap_last = swap_back(5 - core, 1, 2)
    swap_last.start()
    pairs = [jnp.concatenate([back[2 * pair], back[2 * pair + 1]], axis=1) for pair in range(3)]
    both(0)
    swap_last.wait_recv()
    products((0,))
    s.ring_start(0)
    g.settled()

    def plain_rows(y, inner):
        cols = slice(y * 512, (y + 1) * 512)
        grad = sum(across(pairs[pair], weight_rows((2 * pair, 2 * pair + 1), y), 1, 1) for pair in range(3))
        grad = grad * gain_row[:, cols]
        plain[:, cols] = grad
        return inner + jnp.sum(grad * hidden_ref[:, cols].astype(jnp.float32), axis=1, keepdims=True)

    inner = jnp.zeros((128, 1), jnp.float32)

    for y in (0, 1, 2, 3):
        inner = plain_rows(y, inner)
    both(1)
    s.ring_step(0, 0, 0)
    for y in (4, 5, 6, 7):
        inner = plain_rows(y, inner)
    both(2)
    s.ring_step(0, 1, 0)
    fall = inv_rms * inv_rms * inv_rms * (1.0 / WIDTH) * inner
    for y in range(8):
        cols = slice(y * 512, (y + 1) * 512)
        grad_in_ref[:, cols] = (
            plain[:, cols] * inv_rms - hidden_ref[:, cols].astype(jnp.float32) * fall
        ).astype(jnp.bfloat16)
    s.ring_step(0, 0, 1)
    s.lines_out(0, 0)
    for h in range(HALVES):
        for p in (1, 2):
            s.ring_step(p, h, 3)
            s.lines_out(p, h)
    s.ring_step(0, 1, 1)
    s.lines_out(0, 1)
    for h in range(HALVES):
        for p in (1, 2):
            s.dots_out(p, h)
    for h in range(HALVES):
        s.dots_out(0, h)
    s.finish(1)
    s.finish(2)
    s.finish(0)
    s.finished(1)
    inside = (j, i // 16, (i // 8) % 2, (i // 2) % 4, i % 2)
    sums = jnp.zeros((8, HD), jnp.float32)
    for n in range(TILES):
        tile = total_ref[n]
        weight_grad_ref[:, n * HD : (n + 1) * HD] = tile
        sums = sums + tile * full[(n, *inside)].astype(jnp.float32)
    lane = lax.broadcasted_iota(jnp.int32, (8, 128), 1)
    row = lax.broadcasted_iota(jnp.int32, (8, 128), 0)
    gains = jnp.sum(jnp.where(lane % 8 == row, gain_full[inside], 0.0), axis=1, keepdims=True)
    answer = jnp.sum(sums, axis=1, keepdims=True) / gains
    gain_grad_ref[...] = jnp.sum(jnp.where(lane == row, answer, 0.0), axis=0, keepdims=True)

    for peer in range(1, 8):
        @pl.when(j < peer)
        def _():
            kv_copy(j, peer).wait_send()

    for owner in range(7):
        @pl.when(owner < j)
        def _():
            part_copy(owner, j).wait_send()

    for copy in (swap, swap_heads, swap_last):
        copy.wait_send()
    s.settled()


def whole(hidden, tiles, gain_piece, tables, cot):
    dma = pltpu.SemaphoreType.DMA
    vmem = pl.BlockSpec(memory_space=pltpu.VMEM)
    hbm = pl.BlockSpec(memory_space=pltpu.HBM)
    low, wide = jnp.bfloat16, jnp.float32

    def rings(p):
        dim = RINGS[p]
        return pltpu.VMEM((2, SIZES[dim] // 2, HALVES, *RING_SHAPES[dim]), low)

    def lines(p, h):
        return pltpu.VMEM((SIZES[ORDERS[p][h][1]] - 1, *LINE_SHAPES[ORDERS[p][h][0]]), low)

    return pl.pallas_call(
        whole_kernel,
        out_shape=(
            jax.ShapeDtypeStruct((128, FLAT), low),
            jax.ShapeDtypeStruct((128, WIDTH), low),
            jax.ShapeDtypeStruct((8, TILES * HD), wide),
            jax.ShapeDtypeStruct((1, 128), wide),
        ),
        in_specs=[hbm, vmem, vmem, hbm, hbm],
        out_specs=(vmem,) * 4,
        scratch_shapes=[
            pltpu.VMEM((TILES, 8, 4, 2, 4, 2, 8, HD), low),
            pltpu.VMEM((8, 4, 2, 4, 2, 1, 128), wide),
            pltpu.VMEM((1, WIDTH), wide),
            pltpu.VMEM((128, WIDTH), low),
            pltpu.VMEM((WIDTH, 128), low),
            pltpu.VMEM((WIDTH, 128), low),
            pltpu.VMEM((8, 2, 128, HD), low),
            pltpu.VMEM((CHUNKS, CHUNK, FLAT), wide),
            pltpu.VMEM((8, 2, 128, HD), low),
            pltpu.VMEM((8, 2, 128, HD), low),
            pltpu.VMEM((TILES, 128, HD), low),
            pltpu.VMEM((3, 128, HD), low),
            pltpu.VMEM((128, WIDTH), wide),
            pltpu.VMEM((3, 4, 2, 8, 4, 2, 8, HD), low),
            *[rings(p) for p in range(3)],
            *[lines(p, h) for p in range(3) for h in range(HALVES)],
            pltpu.VMEM((3, HALVES, 7, 8, HD), low),
            pltpu.VMEM((3, 2, 8, HD), wide),
            pltpu.VMEM((TILES, 8, HD), wide),
            pltpu.VMEM((TILES, 128, HD), wide),
            pltpu.VMEM((512, 8, HD), low),
            pltpu.VMEM((128, WIDTH), low),
            pltpu.VMEM((2, 128, HD), wide),
            pltpu.VMEM((128, FLAT), low),
            dma((3,)),
            dma((2,)),
            dma((7,)),
            dma((7,)),
            dma((HALVES, 7)),
            dma((HALVES, 3)),
            dma((3,)),
            dma((2, 2, 4, HALVES)),
            dma((2, 3)),
            dma((2, 4)),
            dma((4,)),
            dma((2, 8)),
            dma((2, 8)),
            dma((2, 4)),
            dma((3,)),
            dma((3, 2, 4, HALVES)),
            dma((7,)),
            dma((7,)),
            dma((2,)),
        ],
        compiler_params=pltpu.CompilerParams(collective_id=0, has_side_effects=True, vmem_limit_bytes=40 * 2**20),
        name="whole",
    )(hidden, tiles, gain_piece, tables, cot)


def rope_tables():
    freqs = np.float32(rope_base) ** (-np.arange(HD // 2, dtype=np.float32) / np.float32(HD // 2))
    angles = (np.arange(1024, dtype=np.float32)[:, None] * freqs.astype(np.float32)[None, :]).astype(np.float64)
    cosine, sine = np.cos(angles), np.sin(angles)
    both = np.stack([np.concatenate([cosine, cosine], axis=1), np.concatenate([-sine, sine], axis=1)])
    return np.moveaxis(both.reshape(2, 8, 128, HD), 1, 0).astype(np.float32)


def write_kernel(*refs):
    sems = refs[-1]
    copies = [pltpu.make_async_copy(refs[k], refs[3 + k], sems.at[k]) for k in range(3)]
    for copy in copies:
        copy.start()
    for copy in copies:
        copy.wait()


def written(*arrays):
    return pl.pallas_call(
        write_kernel,
        out_shape=tuple(jax.ShapeDtypeStruct(a.shape, a.dtype) for a in arrays),
        in_specs=[pl.BlockSpec(memory_space=pltpu.VMEM)] * 3,
        out_specs=(pl.BlockSpec(memory_space=pltpu.HBM),) * 3,
        scratch_shapes=[pltpu.SemaphoreType.DMA((3,))],
        compiler_params=pltpu.CompilerParams(vmem_limit_bytes=16 * 2**20),
        name="written",
    )(*arrays)


def local(hidden_in, norm_gain, qkv_weight, attn_cotangent):
    i, j = lax.axis_index("inter"), lax.axis_index("intra")
    tiles = jnp.moveaxis(qkv_weight.reshape(8, TILES, HD), 1, 0)
    lane = jnp.arange(128)
    gain_piece = jnp.where(lane // 8 == (i * 8 + j) % 16, jnp.tile(norm_gain.astype(jnp.float32), 16), 0.0)[None]
    tables = jnp.asarray(rope_tables())
    kept = [pltpu.with_memory_space_constraint(v, pltpu.HBM) for v in (hidden_in[0], attn_cotangent[0], tables)]
    attn, grad_in, weight_grad, gain_grad = whole(kept[0], tiles, gain_piece, kept[2], kept[1])
    attn, grad_in, weight_grad = written(attn, grad_in, weight_grad)
    return (attn[None], grad_in[None], weight_grad, gain_grad[0, :8])


def solution(mesh):
    return jax.shard_map(
        local,
        mesh=mesh,
        in_specs=(
            P("inter", "intra", None),
            P(("inter", "intra")),
            P(("inter", "intra"), None),
            P("inter", "intra", None),
        ),
        out_specs=(
            P("inter", "intra", None),
            P("inter", "intra", None),
            P(("intra", "inter"), None),
            P(("intra", "inter")),
        ),
        check_vma=False,
    )
```

```python
import jax
import jax.numpy as jnp
import numpy as np
from jax import lax
from jax.experimental import pallas as pl
from jax.experimental.pallas import tpu as pltpu
from jax.sharding import PartitionSpec as P

HD = 128
HEADS = 4
TILES = HEADS + 2
WIDTH = 4096
MESH = pl.DeviceIdType.MESH
SIZES = {"x": 4, "y": 8, "z": 8}
ORDERS = (
    (("z", "y", "x"), ("y", "z", "x")),
    (("z", "x", "y"), ("z", "x", "y")),
    (("y", "x", "z"), ("y", "x", "z")),
)
RINGS = ("x", "y", "z")
HALVES = 2
CHUNK = 256
CHUNKS = 1024 // CHUNK
BLOCKS = CHUNK // 128
FLAT = HEADS * 128

eps_norm = 1e-05
rope_base = 500000.0


def place():
    i, j = lax.axis_index("inter"), lax.axis_index("intra")
    return {"x": j // 2, "y": i // 8, "z": ((i // 2) % 4) * 2 + j % 2}, i % 2


def device(at, core):
    return ((at["y"] * 4 + at["z"] // 2) * 2 + core, at["x"] * 2 + at["z"] % 2)


def moved(at, dim, step):
    size = SIZES[dim]
    return {**at, dim: (at[dim] + step + size) % size}


def indices(at):
    every = slice(None)
    y, x = at.get("y", every), at.get("x", every)
    high, low = (at["z"] // 2, at["z"] % 2) if "z" in at else (every, every)
    return y, high, x, low


def slab(ref, tile, at, cores=slice(None)):
    y, high, x, low = indices(at)
    return ref.at[tile, y, high, cores, x, low]


def out_slab(ref, tile, at, cores=slice(None)):
    y, high, x, low = indices(at)
    return ref.at[tile, x, low, y, high, cores]


def remote(src, dst, send, recv, peer):
    return pltpu.make_async_remote_copy(
        src_ref=src, dst_ref=dst, send_sem=send, recv_sem=recv, device_id=peer, device_id_type=MESH
    )


def across(left, right, left_dim, right_dim):
    return lax.dot_general(
        left, right, (((left_dim,), (right_dim,)), ((), ())), preferred_element_type=jnp.float32
    )


def steps_of(p, way):
    return SIZES[RINGS[p]] // 2 - way


def tiles_of(core):
    return [4 + core, 2 * core, 2 * core + 1]


def settle(spare, count, sem):
    pltpu.make_async_copy(spare.at[pl.ds(0, count)], spare.at[pl.ds(0, count)], sem).wait()


def greet(at, core, barrier):
    i, j = lax.axis_index("inter"), lax.axis_index("intra")
    peers = [device(at, 1 - core)]
    for dim, size in SIZES.items():
        peers += [device(moved(at, dim, step), core) for step in range(1, size)]
    peers += [(i, (j + step) % 8) for step in range(1, 8)]
    for peer in peers:
        pl.semaphore_signal(barrier, inc=1, device_id=peer, device_id_type=MESH)
    return len(peers)


class Gather:
    def __init__(self, at, core, mine_ref, gain_ref, full, gain_pair, gain_near, gain_far, spare, sems):
        self.at, self.core, self.partner = at, core, device(at, 1 - core)
        self.mine_ref, self.gain_ref, self.full = mine_ref, gain_ref, full
        self.pair, self.near, self.far = gain_pair, gain_near, gain_far
        (self.swap, self.one, self.two, self.item, self.side, self.ring_out, self.ring, self.passing, self.gains, self.own) = sems
        self.mine, self.theirs = tiles_of(core), tiles_of(1 - core)
        sign = 1 - 2 * core
        self.ways = (sign, -sign)
        self.spare = spare

    def go(self, copy):
        copy.start()

    def begin(self):
        at, core, full = self.at, self.core, self.full
        owns = []
        for p in range(3):
            self.go(
                remote(
                    self.mine_ref.at[self.theirs[p]],
                    slab(full, self.theirs[p], at, core),
                    self.swap.at[0],
                    self.swap.at[1],
                    self.partner,
                )
            )
            owns.append(
                pltpu.make_async_copy(self.mine_ref.at[self.mine[p]], slab(full, self.mine[p], at, core), self.own.at[p])
            )
        self.go(remote(self.gain_ref, self.pair, self.gains.at[0, 0], self.gains.at[1, 0], self.partner))
        for own in owns:
            own.start()
        for own in owns:
            own.wait()
        settle(self.spare, 3, self.swap.at[1])
        for p in (1, 2, 0):
            for h in range(HALVES):
                self.direct(p, h, 0)
        self.gain_wait(0, 1)
        self.near[0] = self.gain_ref[...] + self.pair[...]

    def direct(self, p, h, phase):
        order = ORDERS[p][h]
        sems = (self.one, self.two)[phase]
        src = slab(self.full, self.mine[p], {d: self.at[d] for d in order[phase:]}, h)
        for step in range(1, SIZES[order[phase]]):
            peer = device(moved(self.at, order[phase], step), self.core)
            recv = self.item.at[h, step - 1] if p == 0 and phase == 1 else sems.at[2 * p + h]
            self.go(remote(src, src, sems.at[6], recv, peer))

    def along(self, h, step):
        middle = ORDERS[0][h][1]
        if step:
            settle(self.spare, 8, self.item.at[h, step - 1])
        known = moved({d: self.at[d] for d in (middle, "x")}, middle, -step)
        src = slab(self.full, self.mine[0], known, h)
        for k in (1, 3, 2):
            peer = device(moved(self.at, "x", k), self.core)
            self.go(remote(src, src, self.ring_out.at[0], self.side.at[h, k - 1], peer))

    def beside(self, h):
        for k in (1, 3, 2):
            settle(self.spare, 64, self.side.at[h, k - 1])
            self.pass_on(0, h, moved(self.at, "x", -k)["x"])

    def arrived(self, p, h, phase):
        order = ORDERS[p][h]
        sems = (self.one, self.two)[phase]
        each = 1 if phase == 0 else SIZES[order[0]]
        settle(self.spare, (SIZES[order[phase]] - 1) * each, sems.at[2 * p + h])

    def gain_wait(self, phase, side):
        rows = (self.pair, self.near.at[pl.ds(0, 7)], self.far.at[0, pl.ds(0, 3)], self.far.at[pl.ds(0, 7)])[phase]
        pltpu.make_async_copy(rows, rows, self.gains.at[side, phase]).wait()

    def gain_group(self):
        i, j = lax.axis_index("inter"), lax.axis_index("intra")
        for step in range(1, 8):
            self.go(
                remote(
                    self.near.at[0], self.near.at[step], self.gains.at[0, 1], self.gains.at[1, 1], (i, (j + step) % 8)
                )
            )

    def gain_high(self):
        at = self.at
        self.gain_wait(1, 1)
        self.far[at["y"], at["z"] // 2] = sum(self.near[k] for k in range(8))
        here = self.far.at[at["y"], at["z"] // 2]
        for step in (1, 3, 2):
            peer = device(moved(at, "z", 2 * step), self.core)
            self.go(remote(here, here, self.gains.at[0, 2], self.gains.at[1, 2], peer))

    def gain_all(self):
        self.gain_wait(2, 1)
        here = self.far.at[self.at["y"]]
        for step in range(1, 8):
            peer = device(moved(self.at, "y", step), self.core)
            self.go(remote(here, here, self.gains.at[0, 3], self.gains.at[1, 3], peer))

    def settled(self):
        settle(self.spare, 3, self.swap.at[0])
        settle(self.spare, 42, self.one.at[6])
        settle(self.spare, 208, self.two.at[6])
        for p in range(3):
            settle(self.spare, 384 if RINGS[p] == "x" else 448, self.ring_out.at[p])
            settle(self.spare, 512, self.passing.at[0, p])
        for phase in range(4):
            self.gain_wait(phase, 0)

    def where(self, p, way, step):
        dim = RINGS[p]
        return moved(self.at, dim, -self.ways[way] * step)[dim]

    def hop(self, p, way, step, h):
        dim = RINGS[p]
        piece = slab(self.full, self.mine[p], {dim: self.where(p, way, step)}, h)
        peer = device(moved(self.at, dim, self.ways[way]), self.core)
        self.go(remote(piece, piece, self.ring_out.at[p], self.ring.at[p - 1, way, step, h], peer))

    def pass_on(self, p, h, where):
        piece = slab(self.full, self.mine[p], {RINGS[p]: where}, h)
        self.go(remote(piece, piece, self.passing.at[0, p], self.passing.at[1, p], self.partner))

    def ring_start(self, p, h):
        for way in range(2):
            self.hop(p, way, 0, h)
        self.pass_on(p, h, self.at[RINGS[p]])

    def ring_step(self, p, h, step):
        dim = RINGS[p]
        for way in range(2):
            if step >= steps_of(p, way):
                continue
            piece = slab(self.full, self.mine[p], {dim: self.where(p, way, step + 1)}, h)
            remote(piece, piece, self.ring_out.at[p], self.ring.at[p - 1, way, step, h], self.partner).wait_recv()
            if step + 1 < steps_of(p, way):
                self.hop(p, way, step + 1, h)
            self.pass_on(p, h, self.where(p, way, step + 1))

    def passed(self, p):
        settle(self.spare, 512, self.passing.at[1, p])


RING_SHAPES = {"x": (2, 8, 4, 8, HD), "y": (4, 2, 4, 8, HD), "z": (4, 8, 8, HD)}
LINE_SHAPES = {"x": (4, 8, HD), "y": (8, 8, HD), "z": (2, 4, 8, HD)}


class Scatter:
    def __init__(self, at, core, part, rings, lines, dot_in, final, total_ref, spare, sems):
        self.at, self.core, self.partner = at, core, device(at, 1 - core)
        self.part, self.rings, self.lines, self.dot_in = part, rings, lines, dot_in
        self.final, self.total_ref = final, total_ref
        self.ring_out, self.ring, self.two, self.three, self.last = sems
        sign = 1 - 2 * core
        self.ways = (sign, -sign)
        self.spare = spare

    def go(self, copy):
        copy.start()

    def target(self, p, way, left):
        dim = RINGS[p]
        return {dim: moved(self.at, dim, self.ways[way] * left)[dim]}

    def copy(self, p, way, step, h):
        dim = RINGS[p]
        return remote(
            out_slab(self.part, p, self.target(p, way, steps_of(p, way) - step), h),
            self.rings[p].at[way, step, h],
            self.ring_out.at[p],
            self.ring.at[p, way, step, h],
            device(moved(self.at, dim, self.ways[way]), self.core),
        )

    def ring_start(self, p):
        for h in range(HALVES):
            for way in range(2):
                self.go(self.copy(p, way, 0, h))

    def ring_step(self, p, h, step):
        for way in range(2):
            if step >= steps_of(p, way):
                continue
            self.copy(p, way, step, h).wait_recv()
            here = out_slab(self.part, p, self.target(p, way, steps_of(p, way) - step - 1), h)
            there = self.rings[p].at[way, step, h]
            here[...] = (here[...].astype(jnp.float32) + there[...].astype(jnp.float32)).astype(jnp.bfloat16)
            if step + 1 < steps_of(p, way):
                self.go(self.copy(p, way, step + 1, h))

    def lines_out(self, p, h):
        a, b, c = ORDERS[p][h]
        for step in range(1, SIZES[b]):
            there = moved(self.at, b, step)
            self.go(
                remote(
                    out_slab(self.part, p, {b: there[b], c: self.at[c]}, h),
                    self.lines[2 * p + h].at[step - 1],
                    self.two.at[6],
                    self.two.at[2 * p + h],
                    device(there, self.core),
                )
            )

    def dots_out(self, p, h):
        a, b, c = ORDERS[p][h]
        lines = self.lines[2 * p + h]
        here = out_slab(self.part, p, {b: self.at[b], c: self.at[c]}, h)
        total = here[...].astype(jnp.float32)
        settle(self.spare, (SIZES[b] - 1) * SIZES[a], self.two.at[2 * p + h])
        for step in range(1, SIZES[b]):
            total = total + lines[step - 1].astype(jnp.float32)
        here[...] = total.astype(jnp.bfloat16)
        for step in range(1, SIZES[a]):
            there = moved(self.at, a, step)
            self.go(
                remote(
                    out_slab(self.part, p, there, h),
                    self.dot_in.at[p, h, step - 1],
                    self.three.at[6],
                    self.three.at[2 * p + h],
                    device(there, self.core),
                )
            )

    def finish(self, p):
        tile = tiles_of(self.core)[p]
        for h in range(HALVES):
            a = ORDERS[p][h][0]
            here = out_slab(self.part, p, self.at, h)
            total = here[...].astype(jnp.float32)
            settle(self.spare, SIZES[a] - 1, self.three.at[2 * p + h])
            for step in range(1, SIZES[a]):
                total = total + self.dot_in[p, h, step - 1].astype(jnp.float32)
            self.final[p, h] = total
        self.total_ref[tile] = self.final[p, self.core]
        self.go(
            remote(
                self.final.at[p, 1 - self.core], self.total_ref.at[tile], self.last.at[0], self.last.at[1], self.partner
            )
        )

    def finished(self, side):
        settle(self.spare, 6, self.last.at[side])

    def settled(self):
        for p in range(3):
            settle(self.spare, 384 if RINGS[p] == "x" else 448, self.ring_out.at[p])
        settle(self.spare, 208, self.two.at[6])
        settle(self.spare, 42, self.three.at[6])
        self.finished(0)


def whole_kernel(
    hidden_in, mine_ref, gain_ref, tables_in, cot_in,
    attn_ref, grad_in_ref, weight_grad_ref, gain_grad_ref,
    full, gain_pair, gain_near, gain_far, gain_row, normed, turned_own, turned_other,
    kv, probs, part_out, part_in, back, back_other, plain,
    part, ring_0, ring_1, ring_2, line_0, line_1, line_2, line_3, line_4, line_5, dot_in, final, total_ref, mixed, spare, hidden_ref, tables, cot_ref, load_sem,
    g_swap, g_one, g_two, g_item, g_side, g_out, g_ring, g_pass, g_gain, g_own,
    kv_sem, part_sem, swap_sem, s_out, s_ring, s_two, s_three, s_last,
):
    i, j = lax.axis_index("inter"), lax.axis_index("intra")
    at, core = place()
    partner = device(at, 1 - core)
    barrier = pltpu.get_barrier_semaphore()
    loads = [
        pltpu.make_async_copy(hidden_in, hidden_ref, load_sem.at[0]),
        pltpu.make_async_copy(cot_in, cot_ref, load_sem.at[1]),
        pltpu.make_async_copy(tables_in.at[j], tables, load_sem.at[2]),
    ]
    for load in loads:
        load.start()
    for block in range(8):
        kv[block] = jnp.zeros((2, 128, HD), jnp.bfloat16)
    count = greet(at, core, barrier)
    for load in loads:
        load.wait()
    squares = jnp.zeros((128, 128), jnp.float32)
    for t in range(WIDTH // 128):
        tile = hidden_ref[:, t * 128 : (t + 1) * 128].astype(jnp.float32)
        squares = squares + tile * tile
    inv_rms = lax.rsqrt(jnp.sum(squares, axis=1, keepdims=True) / WIDTH + eps_norm)
    cosine, sine = tables[0], tables[1]
    cots = [cot_ref[:, h * HD : (h + 1) * HD] for h in range(HEADS)]
    pl.semaphore_wait(barrier, count)

    g = Gather(
        at, core, mine_ref, gain_ref, full, gain_pair, gain_near, gain_far, spare,
        (g_swap, g_one, g_two, g_item, g_side, g_out, g_ring, g_pass, g_gain, g_own),
    )
    g.begin()
    g.gain_group()
    for p in (1, 2):
        for h in range(HALVES):
            g.arrived(p, h, 0)
            g.direct(p, h, 1)
    for h in range(HALVES):
        g.arrived(0, h, 0)
        g.direct(0, h, 1)
    for h in range(HALVES):
        g.along(h, 0)
    g.gain_high()

    def along(*steps):
        for step in steps:
            for h in range(HALVES):
                g.along(h, step)

    def begin_far(h):
        for p in (1, 2):
            g.arrived(p, h, 1)
            g.ring_start(p, h)

    def far(step):
        for h in range(HALVES):
            for p in (1, 2):
                g.ring_step(p, h, step)

    begin_far(0)
    along(1, 7)
    begin_far(1)
    along(2, 6)
    g.gain_all()
    along(3, 5, 4)
    for h in range(HALVES):
        g.pass_on(0, h, at["x"])
    far(0)
    far(1)
    g.gain_wait(3, 1)
    for y in range(8):
        for z in range(4):
            t = y * 4 + z
            gain_row[:, t * 128 : (t + 1) * 128] = gain_far[y, z]
    for t in range(WIDTH // 128):
        cols = slice(t * 128, (t + 1) * 128)
        unit = hidden_ref[:, cols].astype(jnp.float32) * inv_rms * gain_row[:, cols]
        normed[:, cols] = unit.astype(jnp.bfloat16)
    g.beside(0)
    far(2)
    g.beside(1)

    def weight_rows(tiles, y):
        return jnp.concatenate([full[tile, y].reshape(512, HD) for tile in tiles], axis=1)

    def mix(tiles):
        total = jnp.zeros((128, len(tiles) * HD), jnp.float32)
        for y in range(8):
            total = total + across(normed[:, y * 512 : (y + 1) * 512], weight_rows(tiles, y), 1, 0)
        for k, tile in enumerate(tiles):
            mixed[tile] = total[:, k * HD : (k + 1) * HD]

    def rotated(x, sign):
        return x * cosine + sign * (pltpu.roll(x, 64, 1) * sine)

    mix(g.mine[:1])
    g.passed(0)
    mix(g.theirs[:1])
    kv[j, 0] = rotated(mixed[4], 1.0).astype(jnp.bfloat16)
    kv[j, 1] = mixed[5].astype(jnp.bfloat16)

    def kv_copy(owner, peer):
        return remote(kv.at[owner], kv.at[owner], kv_sem.at[0, peer], kv_sem.at[1, owner], (i, peer))

    for peer in range(1, 8):
        @pl.when(j < peer)
        def _():
            kv_copy(j, peer).start()

    scale = HD ** (-0.5)
    far(3)
    for t in range(WIDTH // 128):
        cols = slice(t * 128, (t + 1) * 128)
        turned_own[cols, :] = normed[:, cols].T
    swap = remote(turned_own, turned_other, swap_sem.at[0, 0], swap_sem.at[1, 0], partner)
    swap.start()
    mix(g.mine[1:])
    g.passed(1)
    g.passed(2)
    mix(g.theirs[1:])
    queries = [(rotated(mixed[h], 1.0) * scale).astype(jnp.bfloat16) for h in range(HEADS)]
    query = jnp.concatenate(queries, axis=0)
    query_t = jnp.concatenate([q.T for q in queries], axis=1)
    cot = jnp.concatenate(cots, axis=0)
    cot_t = jnp.concatenate([c.T for c in cots], axis=1)
    row_pos = j * 128 + lax.broadcasted_iota(jnp.int32, (CHUNK, FLAT), 1) % 128
    key_pos = lax.broadcasted_iota(jnp.int32, (CHUNK, FLAT), 0)

    def allowed(chunk):
        return key_pos + chunk * CHUNK <= row_pos

    def rows(chunk, which):
        return jnp.concatenate([kv[chunk * BLOCKS + b, which] for b in range(BLOCKS)], axis=0)

    for owner in range(7):
        @pl.when(owner < j)
        def _():
            kv_copy(owner, j).wait_recv()

    top = jnp.full((1, FLAT), -1e30, jnp.float32)
    for chunk in range(CHUNKS):
        scores = jnp.where(allowed(chunk), across(rows(chunk, 0), query_t, 1, 0), -1e30)
        probs[chunk] = scores
        top = jnp.maximum(top, jnp.max(scores, axis=0, keepdims=True))
    total = jnp.zeros((1, FLAT), jnp.float32)
    out_t = jnp.zeros((HD, FLAT), jnp.float32)
    for chunk in range(CHUNKS):
        numbers = jnp.exp(probs[chunk] - top)
        probs[chunk] = numbers
        total = total + jnp.sum(numbers, axis=0, keepdims=True)
        out_t = out_t + across(rows(chunk, 1), numbers.astype(jnp.bfloat16), 0, 0)
    share = 1.0 / total
    attn_t = (out_t * share).astype(jnp.bfloat16)
    delta = jnp.sum(cot_t.astype(jnp.float32) * attn_t.astype(jnp.float32), axis=0, keepdims=True)
    query_grad_t = jnp.zeros((HD, FLAT), jnp.float32)

    def part_copy(owner, maker):
        return remote(part_out.at[owner], part_in.at[maker], part_sem.at[0, owner], part_sem.at[1, maker], (i, owner))

    def send_parts(chunk):
        for b in range(BLOCKS):
            owner = chunk * BLOCKS + b

            @pl.when(owner < j)
            def _():
                part_copy(owner, j).start()

    for chunk in range(CHUNKS):
        probs_t = probs[chunk] * share
        probs_grad = across(rows(chunk, 1), cot_t, 1, 0)
        scores_grad = (probs_t * (probs_grad - delta)).astype(jnp.bfloat16)
        keys_part = across(scores_grad, query, 1, 0).astype(jnp.bfloat16)
        values_part = across(probs_t.astype(jnp.bfloat16), cot, 1, 0).astype(jnp.bfloat16)
        for b in range(BLOCKS):
            part_out[chunk * BLOCKS + b, 0] = keys_part[b * 128 : (b + 1) * 128]
            part_out[chunk * BLOCKS + b, 1] = values_part[b * 128 : (b + 1) * 128]
        query_grad_t = query_grad_t + across(rows(chunk, 0), scores_grad, 0, 0)
        send_parts(chunk)
    for h in range(HEADS):
        grad = query_grad_t[:, h * 128 : (h + 1) * 128].T
        back[h] = (rotated(grad, -1.0) * scale).astype(jnp.bfloat16)

    def swap_back(first, count, slot):
        return remote(
            back.at[pl.ds(first, count)], back_other.at[pl.ds(slot, count)], swap_sem.at[0, 1 + slot],
            swap_sem.at[1, 1 + slot], partner,
        )

    swap_heads = swap_back(2 * (1 - core), 2, 0)
    swap_heads.start()
    for h in range(HEADS):
        attn_ref[:, h * HD : (h + 1) * HD] = attn_t[:, h * 128 : (h + 1) * 128].T
    swap.wait_recv()
    swap_heads.wait_recv()

    def products(ps):
        own = jnp.concatenate([back[g.mine[p]] for p in ps], axis=1)
        other = jnp.concatenate([back_other[(p + 2) % 3] for p in ps], axis=1)
        both = jnp.concatenate([own, other], axis=0)
        for k in range(8):
            chosen = slice(k * 512, (k + 1) * 512)
            left = jnp.concatenate([turned_own[chosen, :], turned_other[chosen, :]], axis=1)
            sums = across(left, both, 1, 0)
            for n, p in enumerate(ps):
                part[p, k // 2, k % 2] = sums[:, n * HD : (n + 1) * HD].reshape(8, 4, 2, 8, HD).astype(jnp.bfloat16)

    s = Scatter(
        at, core, part, (ring_0, ring_1, ring_2), (line_0, line_1, line_2, line_3, line_4, line_5), dot_in, final,
        total_ref, spare, (s_out, s_ring, s_two, s_three, s_last),
    )
    products((1, 2))
    s.ring_start(1)
    s.ring_start(2)
    pairs = [jnp.concatenate([back[2 * pair], back[2 * pair + 1]], axis=1) for pair in range(2)]
    for y in range(8):
        plain[:, y * 512 : (y + 1) * 512] = sum(
            across(pairs[pair], weight_rows((2 * pair, 2 * pair + 1), y), 1, 1) for pair in range(2)
        )
    part_in[j] = part_out[j]
    keys_grad = jnp.zeros((128, HD), jnp.float32)
    values_grad = jnp.zeros((128, HD), jnp.float32)
    for maker in range(8):
        @pl.when(maker > j)
        def _():
            part_copy(j, maker).wait_recv()

        @pl.when(maker < j)
        def _():
            part_in[maker] = jnp.zeros((2, 128, HD), jnp.bfloat16)

        keys_grad = keys_grad + part_in[maker, 0].astype(jnp.float32)
        values_grad = values_grad + part_in[maker, 1].astype(jnp.float32)
    back[4] = rotated(keys_grad, -1.0).astype(jnp.bfloat16)
    back[5] = values_grad.astype(jnp.bfloat16)

    def both(step):
        for h in range(HALVES):
            for p in (1, 2):
                s.ring_step(p, h, step)

    swap_last = swap_back(5 - core, 1, 2)
    swap_last.start()
    last_pair = jnp.concatenate([back[4], back[5]], axis=1)
    both(0)
    swap_last.wait_recv()
    products((0,))
    s.ring_start(0)
    g.settled()

    def plain_rows(y, inner):
        cols = slice(y * 512, (y + 1) * 512)
        grad = plain[:, cols] + across(last_pair, weight_rows((4, 5), y), 1, 1)
        grad = grad * gain_row[:, cols]
        plain[:, cols] = grad
        return inner + jnp.sum(grad * hidden_ref[:, cols].astype(jnp.float32), axis=1, keepdims=True)

    inner = jnp.zeros((128, 1), jnp.float32)

    for y in range(8):
        inner = plain_rows(y, inner)
    both(1)
    fall = inv_rms * inv_rms * inv_rms * (1.0 / WIDTH) * inner
    for y in range(8):
        cols = slice(y * 512, (y + 1) * 512)
        grad_in_ref[:, cols] = (
            plain[:, cols] * inv_rms - hidden_ref[:, cols].astype(jnp.float32) * fall
        ).astype(jnp.bfloat16)
    s.ring_step(0, 0, 0)
    both(2)
    s.ring_step(0, 1, 0)
    s.ring_step(0, 0, 1)
    s.lines_out(0, 0)
    for h in range(HALVES):
        for p in (1, 2):
            s.ring_step(p, h, 3)
            s.lines_out(p, h)
    s.ring_step(0, 1, 1)
    s.lines_out(0, 1)
    for h in range(HALVES):
        for p in (1, 2):
            s.dots_out(p, h)
    for h in range(HALVES):
        s.dots_out(0, h)
    s.finish(1)
    s.finish(2)
    s.finish(0)
    s.finished(1)
    inside = (j, i // 16, (i // 8) % 2, (i // 2) % 4, i % 2)
    sums = jnp.zeros((8, HD), jnp.float32)
    for n in range(TILES):
        tile = total_ref[n]
        weight_grad_ref[:, n * HD : (n + 1) * HD] = tile
        sums = sums + tile * full[(n, *inside)].astype(jnp.float32)
    lane = lax.broadcasted_iota(jnp.int32, (8, 128), 1)
    row = lax.broadcasted_iota(jnp.int32, (8, 128), 0)
    gains = jnp.sum(jnp.where(lane == (i % 16) * 8 + row, gain_far[j, i // 16], 0.0), axis=1, keepdims=True)
    answer = jnp.sum(sums, axis=1, keepdims=True) / gains
    gain_grad_ref[...] = jnp.sum(jnp.where(lane == row, answer, 0.0), axis=0, keepdims=True)

    for peer in range(1, 8):
        @pl.when(j < peer)
        def _():
            kv_copy(j, peer).wait_send()

    for owner in range(7):
        @pl.when(owner < j)
        def _():
            part_copy(owner, j).wait_send()

    for copy in (swap, swap_heads, swap_last):
        copy.wait_send()
    s.settled()


def whole(hidden, tiles, gain_piece, tables, cot):
    dma = pltpu.SemaphoreType.DMA
    vmem = pl.BlockSpec(memory_space=pltpu.VMEM)
    hbm = pl.BlockSpec(memory_space=pltpu.HBM)
    low, wide = jnp.bfloat16, jnp.float32

    def rings(p):
        dim = RINGS[p]
        return pltpu.VMEM((2, SIZES[dim] // 2, HALVES, *RING_SHAPES[dim]), low)

    def lines(p, h):
        return pltpu.VMEM((SIZES[ORDERS[p][h][1]] - 1, *LINE_SHAPES[ORDERS[p][h][0]]), low)

    return pl.pallas_call(
        whole_kernel,
        out_shape=(
            jax.ShapeDtypeStruct((128, FLAT), low),
            jax.ShapeDtypeStruct((128, WIDTH), low),
            jax.ShapeDtypeStruct((8, TILES * HD), wide),
            jax.ShapeDtypeStruct((1, 128), wide),
        ),
        in_specs=[hbm, vmem, vmem, hbm, hbm],
        out_specs=(vmem,) * 4,
        scratch_shapes=[
            pltpu.VMEM((TILES, 8, 4, 2, 4, 2, 8, HD), low),
            pltpu.VMEM((1, 128), wide),
            pltpu.VMEM((8, 1, 128), wide),
            pltpu.VMEM((8, 4, 1, 128), wide),
            pltpu.VMEM((1, WIDTH), wide),
            pltpu.VMEM((128, WIDTH), low),
            pltpu.VMEM((WIDTH, 128), low),
            pltpu.VMEM((WIDTH, 128), low),
            pltpu.VMEM((8, 2, 128, HD), low),
            pltpu.VMEM((CHUNKS, CHUNK, FLAT), wide),
            pltpu.VMEM((8, 2, 128, HD), low),
            pltpu.VMEM((8, 2, 128, HD), low),
            pltpu.VMEM((TILES, 128, HD), low),
            pltpu.VMEM((3, 128, HD), low),
            pltpu.VMEM((128, WIDTH), wide),
            pltpu.VMEM((3, 4, 2, 8, 4, 2, 8, HD), low),
            *[rings(p) for p in range(3)],
            *[lines(p, h) for p in range(3) for h in range(HALVES)],
            pltpu.VMEM((3, HALVES, 7, 8, HD), low),
            pltpu.VMEM((3, 2, 8, HD), wide),
            pltpu.VMEM((TILES, 8, HD), wide),
            pltpu.VMEM((TILES, 128, HD), wide),
            pltpu.VMEM((512, 8, HD), low),
            pltpu.VMEM((128, WIDTH), low),
            pltpu.VMEM((2, 128, HD), wide),
            pltpu.VMEM((128, FLAT), low),
            dma((3,)),
            dma((2,)),
            dma((7,)),
            dma((7,)),
            dma((HALVES, 7)),
            dma((HALVES, 3)),
            dma((3,)),
            dma((2, 2, 4, HALVES)),
            dma((2, 3)),
            dma((2, 4)),
            dma((4,)),
            dma((2, 8)),
            dma((2, 8)),
            dma((2, 4)),
            dma((3,)),
            dma((3, 2, 4, HALVES)),
            dma((7,)),
            dma((7,)),
            dma((2,)),
        ],
        compiler_params=pltpu.CompilerParams(collective_id=0, has_side_effects=True, vmem_limit_bytes=40 * 2**20),
        name="whole",
    )(hidden, tiles, gain_piece, tables, cot)


def rope_tables():
    freqs = np.float32(rope_base) ** (-np.arange(HD // 2, dtype=np.float32) / np.float32(HD // 2))
    angles = (np.arange(1024, dtype=np.float32)[:, None] * freqs.astype(np.float32)[None, :]).astype(np.float64)
    cosine, sine = np.cos(angles), np.sin(angles)
    both = np.stack([np.concatenate([cosine, cosine], axis=1), np.concatenate([-sine, sine], axis=1)])
    return np.moveaxis(both.reshape(2, 8, 128, HD), 1, 0).astype(np.float32)


def write_kernel(*refs):
    sems = refs[-1]
    copies = [pltpu.make_async_copy(refs[k], refs[3 + k], sems.at[k]) for k in range(3)]
    for copy in copies:
        copy.start()
    for copy in copies:
        copy.wait()


def written(*arrays):
    return pl.pallas_call(
        write_kernel,
        out_shape=tuple(jax.ShapeDtypeStruct(a.shape, a.dtype) for a in arrays),
        in_specs=[pl.BlockSpec(memory_space=pltpu.VMEM)] * 3,
        out_specs=(pl.BlockSpec(memory_space=pltpu.HBM),) * 3,
        scratch_shapes=[pltpu.SemaphoreType.DMA((3,))],
        compiler_params=pltpu.CompilerParams(vmem_limit_bytes=16 * 2**20),
        name="written",
    )(*arrays)


def local(hidden_in, norm_gain, qkv_weight, attn_cotangent):
    i, j = lax.axis_index("inter"), lax.axis_index("intra")
    tiles = jnp.moveaxis(qkv_weight.reshape(8, TILES, HD), 1, 0)
    lane = jnp.arange(128)
    gain_piece = jnp.where(lane // 8 == (i * 8 + j) % 16, jnp.tile(norm_gain.astype(jnp.float32), 16), 0.0)[None]
    tables = jnp.asarray(rope_tables())
    kept = [pltpu.with_memory_space_constraint(v, pltpu.HBM) for v in (hidden_in[0], attn_cotangent[0], tables)]
    attn, grad_in, weight_grad, gain_grad = whole(kept[0], tiles, gain_piece, kept[2], kept[1])
    attn, grad_in, weight_grad = written(attn, grad_in, weight_grad)
    return (attn[None], grad_in[None], weight_grad, gain_grad[0, :8])


def solution(mesh):
    return jax.shard_map(
        local,
        mesh=mesh,
        in_specs=(
            P("inter", "intra", None),
            P(("inter", "intra")),
            P(("inter", "intra"), None),
            P("inter", "intra", None),
        ),
        out_specs=(
            P("inter", "intra", None),
            P("inter", "intra", None),
            P(("intra", "inter"), None),
            P(("intra", "inter")),
        ),
        check_vma=False,
    )
```

```python
import jax
import jax.numpy as jnp
import numpy as np
from jax import lax
from jax.experimental import pallas as pl
from jax.experimental.pallas import tpu as pltpu
from jax.sharding import PartitionSpec as P

HD = 128
HEADS = 4
TILES = HEADS + 2
WIDTH = 4096
MESH = pl.DeviceIdType.MESH
SIZES = {"x": 4, "y": 8, "z": 8}
ORDERS = (
    (("z", "y", "x"), ("y", "z", "x")),
    (("z", "x", "y"), ("z", "x", "y")),
    (("y", "x", "z"), ("y", "x", "z")),
)
RINGS = ("x", "y", "z")
HALVES = 2
QUARTERS = 2
CHUNK = 256
CHUNKS = 1024 // CHUNK
BLOCKS = CHUNK // 128
FLAT = HEADS * 128

eps_norm = 1e-05
rope_base = 500000.0


def place():
    i, j = lax.axis_index("inter"), lax.axis_index("intra")
    return {"x": j // 2, "y": i // 8, "z": ((i // 2) % 4) * 2 + j % 2}, i % 2


def device(at, core):
    return ((at["y"] * 4 + at["z"] // 2) * 2 + core, at["x"] * 2 + at["z"] % 2)


def moved(at, dim, step):
    size = SIZES[dim]
    return {**at, dim: (at[dim] + step + size) % size}


def indices(at):
    every = slice(None)
    y, x = at.get("y", every), at.get("x", every)
    high, low = (at["z"] // 2, at["z"] % 2) if "z" in at else (every, every)
    return y, high, x, low


def slab(ref, tile, at, cores=slice(None)):
    y, high, x, low = indices(at)
    return ref.at[tile, y, high, cores, x, low]


def out_slab(ref, tile, at, cores=slice(None)):
    y, high, x, low = indices(at)
    return ref.at[tile, x, low, y, high, cores]


def shares(dim, q):
    if dim == "y":
        return slice(None), slice(q * 2, q * 2 + 2)
    return slice(q * 4, q * 4 + 4), slice(None)


def ring_slab(ref, tile, dim, where, h, q):
    y, high, x, low = indices({dim: where})
    cut_y, cut_high = shares(dim, q)
    y, high = (y, cut_high) if dim == "y" else (cut_y, high)
    return ref.at[tile, y, high, h, x, low]


def ring_out_slab(ref, tile, dim, where, h, q):
    y, high, x, low = indices({dim: where})
    cut_y, cut_high = shares(dim, q)
    y, high = (y, cut_high) if dim == "y" else (cut_y, high)
    return ref.at[tile, x, low, y, high, h]


def remote(src, dst, send, recv, peer):
    return pltpu.make_async_remote_copy(
        src_ref=src, dst_ref=dst, send_sem=send, recv_sem=recv, device_id=peer, device_id_type=MESH
    )


def across(left, right, left_dim, right_dim):
    return lax.dot_general(
        left, right, (((left_dim,), (right_dim,)), ((), ())), preferred_element_type=jnp.float32
    )


def steps_of(p, way):
    return SIZES[RINGS[p]] // 2 - way


def ring_sem(sems, p, way, step, h, q):
    return sems.at[7 * p - 4 * (p > 0) + way * (2 if p == 0 else 4) + step, h, q]


def tiles_of(core):
    return [4 + core, 2 * core, 2 * core + 1]


def settle(spare, count, sem):
    pltpu.make_async_copy(spare.at[pl.ds(0, count)], spare.at[pl.ds(0, count)], sem).wait()


def greet(at, core, barrier):
    i, j = lax.axis_index("inter"), lax.axis_index("intra")
    peers = [device(at, 1 - core)]
    for dim, size in SIZES.items():
        peers += [device(moved(at, dim, step), core) for step in range(1, size)]
        if dim != "x":
            peers += [device(moved(at, dim, step), 1 - core) for step in range(1, size)]
    peers += [(i, (j + step) % 8) for step in range(1, 8)]
    for peer in peers:
        pl.semaphore_signal(barrier, inc=1, device_id=peer, device_id_type=MESH)
    return len(peers)


class Gather:
    def __init__(self, at, core, mine_ref, gain_ref, full, gain_pair, gain_near, gain_far, spare, sems):
        self.at, self.core, self.partner = at, core, device(at, 1 - core)
        self.mine_ref, self.gain_ref, self.full = mine_ref, gain_ref, full
        self.pair, self.near, self.far = gain_pair, gain_near, gain_far
        (self.swap, self.one, self.two, self.item, self.side, self.ring_out, self.ring, self.passing, self.gains, self.own) = sems
        self.mine, self.theirs = tiles_of(core), tiles_of(1 - core)
        sign = 1 - 2 * core
        self.ways = (sign, -sign)
        self.spare = spare

    def go(self, copy):
        copy.start()

    def begin(self):
        at, core, full = self.at, self.core, self.full
        owns = []
        for p in range(3):
            self.go(
                remote(
                    self.mine_ref.at[self.theirs[p]],
                    slab(full, self.theirs[p], at, core),
                    self.swap.at[0],
                    self.swap.at[1],
                    self.partner,
                )
            )
            owns.append(
                pltpu.make_async_copy(self.mine_ref.at[self.mine[p]], slab(full, self.mine[p], at, core), self.own.at[p])
            )
        self.go(remote(self.gain_ref, self.pair, self.gains.at[0, 0], self.gains.at[1, 0], self.partner))
        for own in owns:
            own.start()
        for own in owns:
            own.wait()
        settle(self.spare, 3, self.swap.at[1])
        for p in (1, 2, 0):
            for h in range(HALVES):
                self.direct(p, h, 0)
        self.gain_wait(0, 1)
        self.near[0] = self.gain_ref[...] + self.pair[...]

    def direct(self, p, h, phase):
        order = ORDERS[p][h]
        sems = (self.one, self.two)[phase]
        src = slab(self.full, self.mine[p], {d: self.at[d] for d in order[phase:]}, h)
        for step in range(1, SIZES[order[phase]]):
            peer = device(moved(self.at, order[phase], step), self.core)
            recv = self.item.at[h, step - 1] if p == 0 and phase == 1 else sems.at[2 * p + h]
            self.go(remote(src, src, sems.at[6], recv, peer))

    def along(self, h, step):
        middle = ORDERS[0][h][1]
        if step:
            settle(self.spare, 8, self.item.at[h, step - 1])
        known = moved({d: self.at[d] for d in (middle, "x")}, middle, -step)
        src = slab(self.full, self.mine[0], known, h)
        for k in (2, 1, 3):
            peer = device(moved(self.at, "x", k), self.core)
            self.go(remote(src, src, self.ring_out.at[0], self.side.at[h, k - 1], peer))

    def beside(self, h):
        for k in (1, 3, 2):
            settle(self.spare, 64, self.side.at[h, k - 1])
            self.pass_on(0, h, moved(self.at, "x", -k)["x"])

    def arrived(self, p, h, phase):
        order = ORDERS[p][h]
        sems = (self.one, self.two)[phase]
        each = 1 if phase == 0 else SIZES[order[0]]
        settle(self.spare, (SIZES[order[phase]] - 1) * each, sems.at[2 * p + h])

    def gain_wait(self, phase, side):
        rows = (self.pair, self.near.at[pl.ds(0, 7)], self.far.at[0, pl.ds(0, 3)], self.far.at[pl.ds(0, 7)])[phase]
        pltpu.make_async_copy(rows, rows, self.gains.at[side, phase]).wait()

    def gain_group(self):
        i, j = lax.axis_index("inter"), lax.axis_index("intra")
        for step in range(1, 8):
            self.go(
                remote(
                    self.near.at[0], self.near.at[step], self.gains.at[0, 1], self.gains.at[1, 1], (i, (j + step) % 8)
                )
            )

    def gain_high(self):
        at = self.at
        self.gain_wait(1, 1)
        self.far[at["y"], at["z"] // 2] = sum(self.near[k] for k in range(8))
        here = self.far.at[at["y"], at["z"] // 2]
        for step in (1, 3, 2):
            peer = device(moved(at, "z", 2 * step), self.core)
            self.go(remote(here, here, self.gains.at[0, 2], self.gains.at[1, 2], peer))

    def gain_all(self):
        self.gain_wait(2, 1)
        here = self.far.at[self.at["y"]]
        for step in range(1, 8):
            peer = device(moved(self.at, "y", step), self.core)
            self.go(remote(here, here, self.gains.at[0, 3], self.gains.at[1, 3], peer))

    def settled(self):
        settle(self.spare, 3, self.swap.at[0])
        settle(self.spare, 42, self.one.at[6])
        settle(self.spare, 208, self.two.at[6])
        for p in range(3):
            settle(self.spare, 384 if RINGS[p] == "x" else 448, self.ring_out.at[p])
            settle(self.spare, 512, self.passing.at[0, p])
        for phase in range(4):
            self.gain_wait(phase, 0)

    def where(self, p, way, step):
        dim = RINGS[p]
        return moved(self.at, dim, -self.ways[way] * step)[dim]

    def hop(self, p, way, step, h, q):
        dim = RINGS[p]
        piece = ring_slab(self.full, self.mine[p], dim, self.where(p, way, step), h, q)
        peer = device(moved(self.at, dim, self.ways[way]), self.core)
        self.go(remote(piece, piece, self.ring_out.at[p], self.ring.at[7 * (p - 1) + 4 * way + step, h, q], peer))

    def pass_on(self, p, h, where):
        piece = slab(self.full, self.mine[p], {RINGS[p]: where}, h)
        self.go(remote(piece, piece, self.passing.at[0, p], self.passing.at[1, p], self.partner))

    def ring_start(self, p, h):
        for q in range(QUARTERS):
            for way in range(2):
                self.hop(p, way, 0, h, q)
        self.pass_on(p, h, self.at[RINGS[p]])

    def ring_step(self, p, h, step, q):
        dim = RINGS[p]
        for way in range(2):
            if step >= steps_of(p, way):
                continue
            piece = ring_slab(self.full, self.mine[p], dim, self.where(p, way, step + 1), h, q)
            remote(piece, piece, self.ring_out.at[p], self.ring.at[7 * (p - 1) + 4 * way + step, h, q], self.partner).wait_recv()
            if step + 1 < steps_of(p, way):
                self.hop(p, way, step + 1, h, q)
            if q == QUARTERS - 1:
                self.pass_on(p, h, self.where(p, way, step + 1))

    def passed(self, p):
        settle(self.spare, 512, self.passing.at[1, p])


RING_SHAPES = {"x": (2, 4, 4, 8, HD), "y": (4, 2, 2, 8, HD), "z": (4, 4, 8, HD)}
LINE_SHAPES = {"x": (4, 8, HD), "y": (8, 8, HD), "z": (2, 4, 8, HD)}


class Scatter:
    def __init__(self, at, core, part, rings, lines, dot_in, total_ref, spare, sems):
        self.at, self.core, self.partner = at, core, device(at, 1 - core)
        self.part, self.rings, self.lines, self.dot_in = part, rings, lines, dot_in
        self.total_ref = total_ref
        self.ring_out, self.ring, self.two, self.three, self.last = sems
        sign = 1 - 2 * core
        self.ways = (sign, -sign)
        self.spare = spare

    def go(self, copy):
        copy.start()

    def target(self, p, way, left):
        dim = RINGS[p]
        return moved(self.at, dim, self.ways[way] * left)[dim]

    def copy(self, p, way, step, h, q):
        dim = RINGS[p]
        return remote(
            ring_out_slab(self.part, p, dim, self.target(p, way, steps_of(p, way) - step), h, q),
            self.rings[p].at[way, step, h, q],
            self.ring_out.at[p],
            ring_sem(self.ring, p, way, step, h, q),
            device(moved(self.at, dim, self.ways[way]), self.core),
        )

    def ring_start(self, p):
        for h in range(HALVES):
            for q in range(QUARTERS):
                for way in range(2):
                    self.go(self.copy(p, way, 0, h, q))

    def ring_step(self, p, h, step, q):
        for way in range(2):
            if step >= steps_of(p, way):
                continue
            self.copy(p, way, step, h, q).wait_recv()
            dim = RINGS[p]
            here = ring_out_slab(self.part, p, dim, self.target(p, way, steps_of(p, way) - step - 1), h, q)
            there = self.rings[p].at[way, step, h, q]
            here[...] = (here[...].astype(jnp.float32) + there[...].astype(jnp.float32)).astype(jnp.bfloat16)
            if step + 1 < steps_of(p, way):
                self.go(self.copy(p, way, step + 1, h, q))

    def lines_out(self, p, h):
        a, b, c = ORDERS[p][h]
        for step in range(1, SIZES[b]):
            there = moved(self.at, b, step)
            self.go(
                remote(
                    out_slab(self.part, p, {b: there[b], c: self.at[c]}, h),
                    self.lines[2 * p + h].at[step - 1],
                    self.two.at[6],
                    self.two.at[2 * p + h],
                    device(there, self.core),
                )
            )

    def dots_out(self, p, h):
        a, b, c = ORDERS[p][h]
        lines = self.lines[2 * p + h]
        here = out_slab(self.part, p, {b: self.at[b], c: self.at[c]}, h)
        total = here[...].astype(jnp.float32)
        settle(self.spare, (SIZES[b] - 1) * SIZES[a], self.two.at[2 * p + h])
        for step in range(1, SIZES[b]):
            total = total + lines[step - 1].astype(jnp.float32)
        here[...] = total.astype(jnp.bfloat16)
        tile = tiles_of(self.core)[p]
        for step in range(1, SIZES[a]):
            there = moved(self.at, a, step)
            self.go(
                remote(
                    out_slab(self.part, p, there, h),
                    self.dot_in.at[tile, step - 1],
                    self.three.at[6],
                    self.three.at[tile],
                    device(there, h),
                )
            )
        own = out_slab(self.part, p, self.at, h)

        @pl.when(self.core == h)
        def _():
            self.dot_in[tile, 7] = own[...]

        @pl.when(self.core != h)
        def _():
            self.go(remote(own, self.dot_in.at[tile, 7], self.three.at[6], self.last.at[p], self.partner))

    def finish(self, p, mine):
        tile = tiles_of(self.core if mine else 1 - self.core)[p]
        settle(self.spare, 7, self.three.at[tile])
        if not mine:
            settle(self.spare, 1, self.last.at[p])
        self.total_ref[tile] = sum(self.dot_in[tile, k].astype(jnp.float32) for k in range(8))

    def settled(self):
        for p in range(3):
            settle(self.spare, 384 if RINGS[p] == "x" else 448, self.ring_out.at[p])
        settle(self.spare, 208, self.two.at[6])
        settle(self.spare, 45, self.three.at[6])


def whole_kernel(
    hidden_in, mine_ref, gain_ref, tables_in, cot_in,
    attn_ref, grad_in_ref, weight_grad_ref, gain_grad_ref,
    full, gain_pair, gain_near, gain_far, gain_row, normed, turned_own, turned_other,
    kv, probs, part_out, part_in, back, back_other, plain,
    part, ring_0, ring_1, ring_2, line_0, line_1, line_2, line_3, line_4, line_5, dot_in, total_ref, mixed, spare, hidden_ref, tables, cot_ref, load_sem,
    g_swap, g_one, g_two, g_item, g_side, g_out, g_ring, g_pass, g_gain, g_own,
    kv_sem, part_sem, swap_sem, s_out, s_ring, s_two, s_three, s_last,
):
    i, j = lax.axis_index("inter"), lax.axis_index("intra")
    at, core = place()
    partner = device(at, 1 - core)
    barrier = pltpu.get_barrier_semaphore()
    loads = [
        pltpu.make_async_copy(hidden_in, hidden_ref, load_sem.at[0]),
        pltpu.make_async_copy(cot_in, cot_ref, load_sem.at[1]),
        pltpu.make_async_copy(tables_in.at[j], tables, load_sem.at[2]),
    ]
    for load in loads:
        load.start()
    for block in range(8):
        kv[block] = jnp.zeros((2, 128, HD), jnp.bfloat16)
    count = greet(at, core, barrier)
    for load in loads:
        load.wait()
    squares = jnp.zeros((128, 128), jnp.float32)
    for t in range(WIDTH // 128):
        tile = hidden_ref[:, t * 128 : (t + 1) * 128].astype(jnp.float32)
        squares = squares + tile * tile
    inv_rms = lax.rsqrt(jnp.sum(squares, axis=1, keepdims=True) / WIDTH + eps_norm)
    cosine, sine = tables[0], tables[1]
    cots = [cot_ref[:, h * HD : (h + 1) * HD] for h in range(HEADS)]
    pl.semaphore_wait(barrier, count)

    g = Gather(
        at, core, mine_ref, gain_ref, full, gain_pair, gain_near, gain_far, spare,
        (g_swap, g_one, g_two, g_item, g_side, g_out, g_ring, g_pass, g_gain, g_own),
    )
    g.begin()
    g.gain_group()
    for p in (1, 2):
        for h in range(HALVES):
            g.arrived(p, h, 0)
            g.direct(p, h, 1)
    for h in range(HALVES):
        g.arrived(0, h, 0)
        g.direct(0, h, 1)
    for h in range(HALVES):
        g.along(h, 0)
    g.gain_high()

    def along(*steps):
        for step in steps:
            for h in range(HALVES):
                g.along(h, step)

    def begin_far(h):
        for p in (1, 2):
            g.arrived(p, h, 1)
            g.ring_start(p, h)

    def far(step):
        for h in range(HALVES):
            for q in range(QUARTERS):
                for p in (1, 2):
                    g.ring_step(p, h, step, q)

    begin_far(0)
    along(1, 7)
    begin_far(1)
    along(2, 6)
    g.gain_all()
    along(3, 5, 4)
    for h in range(HALVES):
        g.pass_on(0, h, at["x"])
    far(0)
    far(1)
    g.gain_wait(3, 1)
    for y in range(8):
        for z in range(4):
            t = y * 4 + z
            gain_row[:, t * 128 : (t + 1) * 128] = gain_far[y, z]
    for t in range(WIDTH // 128):
        cols = slice(t * 128, (t + 1) * 128)
        unit = hidden_ref[:, cols].astype(jnp.float32) * inv_rms * gain_row[:, cols]
        normed[:, cols] = unit.astype(jnp.bfloat16)
    g.beside(0)
    g.beside(1)
    far(2)

    def weight_rows(tiles, y):
        return jnp.concatenate([full[tile, y].reshape(512, HD) for tile in tiles], axis=1)

    def mix(tiles):
        total = jnp.zeros((128, len(tiles) * HD), jnp.float32)
        for y in range(8):
            total = total + across(normed[:, y * 512 : (y + 1) * 512], weight_rows(tiles, y), 1, 0)
        for k, tile in enumerate(tiles):
            mixed[tile] = total[:, k * HD : (k + 1) * HD]

    def rotated(x, sign):
        return x * cosine + sign * (pltpu.roll(x, 64, 1) * sine)

    mix(g.mine[:1])
    g.passed(0)
    mix(g.theirs[:1])
    kv[j, 0] = rotated(mixed[4], 1.0).astype(jnp.bfloat16)
    kv[j, 1] = mixed[5].astype(jnp.bfloat16)

    def kv_copy(owner, peer):
        return remote(kv.at[owner], kv.at[owner], kv_sem.at[0, peer], kv_sem.at[1, owner], (i, peer))

    for peer in range(1, 8):
        @pl.when(j < peer)
        def _():
            kv_copy(j, peer).start()

    scale = HD ** (-0.5)
    far(3)
    for t in range(WIDTH // 128):
        cols = slice(t * 128, (t + 1) * 128)
        turned_own[cols, :] = normed[:, cols].T
    swap = remote(turned_own, turned_other, swap_sem.at[0, 0], swap_sem.at[1, 0], partner)
    swap.start()
    mix(g.mine[1:])
    g.passed(1)
    g.passed(2)
    mix(g.theirs[1:])
    queries = [(rotated(mixed[h], 1.0) * scale).astype(jnp.bfloat16) for h in range(HEADS)]
    query = jnp.concatenate(queries, axis=0)
    query_t = jnp.concatenate([q.T for q in queries], axis=1)
    cot = jnp.concatenate(cots, axis=0)
    cot_t = jnp.concatenate([c.T for c in cots], axis=1)
    row_pos = j * 128 + lax.broadcasted_iota(jnp.int32, (CHUNK, FLAT), 1) % 128
    key_pos = lax.broadcasted_iota(jnp.int32, (CHUNK, FLAT), 0)

    def allowed(chunk):
        return key_pos + chunk * CHUNK <= row_pos

    def rows(chunk, which):
        return jnp.concatenate([kv[chunk * BLOCKS + b, which] for b in range(BLOCKS)], axis=0)

    for owner in range(7):
        @pl.when(owner < j)
        def _():
            kv_copy(owner, j).wait_recv()

    top = jnp.full((1, FLAT), -1e30, jnp.float32)
    for chunk in range(CHUNKS):
        scores = jnp.where(allowed(chunk), across(rows(chunk, 0), query_t, 1, 0), -1e30)
        probs[chunk] = scores
        top = jnp.maximum(top, jnp.max(scores, axis=0, keepdims=True))
    total = jnp.zeros((1, FLAT), jnp.float32)
    out_t = jnp.zeros((HD, FLAT), jnp.float32)
    for chunk in range(CHUNKS):
        numbers = jnp.exp(probs[chunk] - top)
        probs[chunk] = numbers
        total = total + jnp.sum(numbers, axis=0, keepdims=True)
        out_t = out_t + across(rows(chunk, 1), numbers.astype(jnp.bfloat16), 0, 0)
    share = 1.0 / total
    attn_t = (out_t * share).astype(jnp.bfloat16)
    delta = jnp.sum(cot_t.astype(jnp.float32) * attn_t.astype(jnp.float32), axis=0, keepdims=True)
    query_grad_t = jnp.zeros((HD, FLAT), jnp.float32)

    def part_copy(owner, maker):
        return remote(part_out.at[owner], part_in.at[maker], part_sem.at[0, owner], part_sem.at[1, maker], (i, owner))

    def send_parts(chunk):
        for b in range(BLOCKS):
            owner = chunk * BLOCKS + b

            @pl.when(owner < j)
            def _():
                part_copy(owner, j).start()

    for chunk in range(CHUNKS):
        probs_t = probs[chunk] * share
        probs_grad = across(rows(chunk, 1), cot_t, 1, 0)
        scores_grad = (probs_t * (probs_grad - delta)).astype(jnp.bfloat16)
        keys_part = across(scores_grad, query, 1, 0).astype(jnp.bfloat16)
        values_part = across(probs_t.astype(jnp.bfloat16), cot, 1, 0).astype(jnp.bfloat16)
        for b in range(BLOCKS):
            part_out[chunk * BLOCKS + b, 0] = keys_part[b * 128 : (b + 1) * 128]
            part_out[chunk * BLOCKS + b, 1] = values_part[b * 128 : (b + 1) * 128]
        query_grad_t = query_grad_t + across(rows(chunk, 0), scores_grad, 0, 0)
        send_parts(chunk)
    for h in range(HEADS):
        grad = query_grad_t[:, h * 128 : (h + 1) * 128].T
        back[h] = (rotated(grad, -1.0) * scale).astype(jnp.bfloat16)

    def swap_back(first, count, slot):
        return remote(
            back.at[pl.ds(first, count)], back_other.at[pl.ds(slot, count)], swap_sem.at[0, 1 + slot],
            swap_sem.at[1, 1 + slot], partner,
        )

    swap_heads = swap_back(2 * (1 - core), 2, 0)
    swap_heads.start()
    for h in range(HEADS):
        attn_ref[:, h * HD : (h + 1) * HD] = attn_t[:, h * 128 : (h + 1) * 128].T
    swap.wait_recv()
    swap_heads.wait_recv()

    def products(ps):
        own = jnp.concatenate([back[g.mine[p]] for p in ps], axis=1)
        other = jnp.concatenate([back_other[(p + 2) % 3] for p in ps], axis=1)
        both = jnp.concatenate([own, other], axis=0)
        for k in range(8):
            chosen = slice(k * 512, (k + 1) * 512)
            left = jnp.concatenate([turned_own[chosen, :], turned_other[chosen, :]], axis=1)
            sums = across(left, both, 1, 0)
            for n, p in enumerate(ps):
                part[p, k // 2, k % 2] = sums[:, n * HD : (n + 1) * HD].reshape(8, 4, 2, 8, HD).astype(jnp.bfloat16)

    s = Scatter(
        at, core, part, (ring_0, ring_1, ring_2), (line_0, line_1, line_2, line_3, line_4, line_5), dot_in, total_ref, spare, (s_out, s_ring, s_two, s_three, s_last),
    )
    products((1, 2))
    s.ring_start(1)
    s.ring_start(2)
    pairs = [jnp.concatenate([back[2 * pair], back[2 * pair + 1]], axis=1) for pair in range(2)]
    for y in range(8):
        plain[:, y * 512 : (y + 1) * 512] = sum(
            across(pairs[pair], weight_rows((2 * pair, 2 * pair + 1), y), 1, 1) for pair in range(2)
        )
    part_in[j] = part_out[j]
    keys_grad = jnp.zeros((128, HD), jnp.float32)
    values_grad = jnp.zeros((128, HD), jnp.float32)
    for maker in range(8):
        @pl.when(maker > j)
        def _():
            part_copy(j, maker).wait_recv()

        @pl.when(maker < j)
        def _():
            part_in[maker] = jnp.zeros((2, 128, HD), jnp.bfloat16)

        keys_grad = keys_grad + part_in[maker, 0].astype(jnp.float32)
        values_grad = values_grad + part_in[maker, 1].astype(jnp.float32)
    back[4] = rotated(keys_grad, -1.0).astype(jnp.bfloat16)
    back[5] = values_grad.astype(jnp.bfloat16)

    def both(step):
        for h in range(HALVES):
            for q in range(QUARTERS):
                for p in (1, 2):
                    s.ring_step(p, h, step, q)

    swap_last = swap_back(5 - core, 1, 2)
    swap_last.start()
    last_pair = jnp.concatenate([back[4], back[5]], axis=1)
    both(0)
    swap_last.wait_recv()
    products((0,))
    s.ring_start(0)
    g.settled()

    def plain_rows(y, inner):
        cols = slice(y * 512, (y + 1) * 512)
        grad = plain[:, cols] + across(last_pair, weight_rows((4, 5), y), 1, 1)
        grad = grad * gain_row[:, cols]
        plain[:, cols] = grad
        return inner + jnp.sum(grad * hidden_ref[:, cols].astype(jnp.float32), axis=1, keepdims=True)

    inner = jnp.zeros((128, 1), jnp.float32)

    for y in range(8):
        inner = plain_rows(y, inner)
    both(1)
    fall = inv_rms * inv_rms * inv_rms * (1.0 / WIDTH) * inner
    for y in range(8):
        cols = slice(y * 512, (y + 1) * 512)
        grad_in_ref[:, cols] = (
            plain[:, cols] * inv_rms - hidden_ref[:, cols].astype(jnp.float32) * fall
        ).astype(jnp.bfloat16)
    def late(h, step):
        for q in range(QUARTERS):
            s.ring_step(0, h, step, q)

    late(0, 0)
    both(2)
    late(1, 0)
    late(0, 1)
    s.lines_out(0, 0)
    for h in range(HALVES):
        for q in range(QUARTERS):
            for p in (1, 2):
                s.ring_step(p, h, 3, q)
                if q == QUARTERS - 1:
                    s.lines_out(p, h)
    late(1, 1)
    s.lines_out(0, 1)
    for h in range(HALVES):
        for p in (1, 2):
            s.dots_out(p, h)
    for h in range(HALVES):
        s.dots_out(0, h)
    for p in (1, 2, 0):
        s.finish(p, True)
        s.finish(p, False)
    inside = (j, i // 16, (i // 8) % 2, (i // 2) % 4, i % 2)
    sums = jnp.zeros((8, HD), jnp.float32)
    for n in range(TILES):
        tile = total_ref[n]
        weight_grad_ref[:, n * HD : (n + 1) * HD] = tile
        sums = sums + tile * full[(n, *inside)].astype(jnp.float32)
    lane = lax.broadcasted_iota(jnp.int32, (8, 128), 1)
    row = lax.broadcasted_iota(jnp.int32, (8, 128), 0)
    gains = jnp.sum(jnp.where(lane == (i % 16) * 8 + row, gain_far[j, i // 16], 0.0), axis=1, keepdims=True)
    answer = jnp.sum(sums, axis=1, keepdims=True) / gains
    gain_grad_ref[...] = jnp.sum(jnp.where(lane == row, answer, 0.0), axis=0, keepdims=True)

    for peer in range(1, 8):
        @pl.when(j < peer)
        def _():
            kv_copy(j, peer).wait_send()

    for owner in range(7):
        @pl.when(owner < j)
        def _():
            part_copy(owner, j).wait_send()

    for copy in (swap, swap_heads, swap_last):
        copy.wait_send()
    s.settled()


def whole(hidden, tiles, gain_piece, tables, cot):
    dma = pltpu.SemaphoreType.DMA
    vmem = pl.BlockSpec(memory_space=pltpu.VMEM)
    hbm = pl.BlockSpec(memory_space=pltpu.HBM)
    low, wide = jnp.bfloat16, jnp.float32

    def rings(p):
        dim = RINGS[p]
        return pltpu.VMEM((2, SIZES[dim] // 2, HALVES, QUARTERS, *RING_SHAPES[dim]), low)

    def lines(p, h):
        return pltpu.VMEM((SIZES[ORDERS[p][h][1]] - 1, *LINE_SHAPES[ORDERS[p][h][0]]), low)

    return pl.pallas_call(
        whole_kernel,
        out_shape=(
            jax.ShapeDtypeStruct((128, FLAT), low),
            jax.ShapeDtypeStruct((128, WIDTH), low),
            jax.ShapeDtypeStruct((8, TILES * HD), wide),
            jax.ShapeDtypeStruct((1, 128), wide),
        ),
        in_specs=[hbm, vmem, vmem, hbm, hbm],
        out_specs=(vmem,) * 4,
        scratch_shapes=[
            pltpu.VMEM((TILES, 8, 4, 2, 4, 2, 8, HD), low),
            pltpu.VMEM((1, 128), wide),
            pltpu.VMEM((8, 1, 128), wide),
            pltpu.VMEM((8, 4, 1, 128), wide),
            pltpu.VMEM((1, WIDTH), wide),
            pltpu.VMEM((128, WIDTH), low),
            pltpu.VMEM((WIDTH, 128), low),
            pltpu.VMEM((WIDTH, 128), low),
            pltpu.VMEM((8, 2, 128, HD), low),
            pltpu.VMEM((CHUNKS, CHUNK, FLAT), wide),
            pltpu.VMEM((8, 2, 128, HD), low),
            pltpu.VMEM((8, 2, 128, HD), low),
            pltpu.VMEM((TILES, 128, HD), low),
            pltpu.VMEM((3, 128, HD), low),
            pltpu.VMEM((128, WIDTH), wide),
            pltpu.VMEM((3, 4, 2, 8, 4, 2, 8, HD), low),
            *[rings(p) for p in range(3)],
            *[lines(p, h) for p in range(3) for h in range(HALVES)],
            pltpu.VMEM((TILES, 8, 8, HD), low),
            pltpu.VMEM((TILES, 8, HD), wide),
            pltpu.VMEM((TILES, 128, HD), wide),
            pltpu.VMEM((512, 8, HD), low),
            pltpu.VMEM((128, WIDTH), low),
            pltpu.VMEM((2, 128, HD), wide),
            pltpu.VMEM((128, FLAT), low),
            dma((3,)),
            dma((2,)),
            dma((7,)),
            dma((7,)),
            dma((HALVES, 7)),
            dma((HALVES, 3)),
            dma((3,)),
            dma((14, HALVES, QUARTERS)),
            dma((2, 3)),
            dma((2, 4)),
            dma((4,)),
            dma((2, 8)),
            dma((2, 8)),
            dma((2, 4)),
            dma((3,)),
            dma((17, HALVES, QUARTERS)),
            dma((7,)),
            dma((7,)),
            dma((3,)),
        ],
        compiler_params=pltpu.CompilerParams(collective_id=0, has_side_effects=True, vmem_limit_bytes=40 * 2**20),
        name="whole",
    )(hidden, tiles, gain_piece, tables, cot)


def rope_tables():
    freqs = np.float32(rope_base) ** (-np.arange(HD // 2, dtype=np.float32) / np.float32(HD // 2))
    angles = (np.arange(1024, dtype=np.float32)[:, None] * freqs.astype(np.float32)[None, :]).astype(np.float64)
    cosine, sine = np.cos(angles), np.sin(angles)
    both = np.stack([np.concatenate([cosine, cosine], axis=1), np.concatenate([-sine, sine], axis=1)])
    return np.moveaxis(both.reshape(2, 8, 128, HD), 1, 0).astype(np.float32)


def write_kernel(*refs):
    sems = refs[-1]
    copies = [pltpu.make_async_copy(refs[k], refs[3 + k], sems.at[k]) for k in range(3)]
    for copy in copies:
        copy.start()
    for copy in copies:
        copy.wait()


def written(*arrays):
    return pl.pallas_call(
        write_kernel,
        out_shape=tuple(jax.ShapeDtypeStruct(a.shape, a.dtype) for a in arrays),
        in_specs=[pl.BlockSpec(memory_space=pltpu.VMEM)] * 3,
        out_specs=(pl.BlockSpec(memory_space=pltpu.HBM),) * 3,
        scratch_shapes=[pltpu.SemaphoreType.DMA((3,))],
        compiler_params=pltpu.CompilerParams(vmem_limit_bytes=16 * 2**20),
        name="written",
    )(*arrays)


def local(hidden_in, norm_gain, qkv_weight, attn_cotangent):
    i, j = lax.axis_index("inter"), lax.axis_index("intra")
    tiles = jnp.moveaxis(qkv_weight.reshape(8, TILES, HD), 1, 0)
    lane = jnp.arange(128)
    gain_piece = jnp.where(lane // 8 == (i * 8 + j) % 16, jnp.tile(norm_gain.astype(jnp.float32), 16), 0.0)[None]
    tables = jnp.asarray(rope_tables())
    kept = [pltpu.with_memory_space_constraint(v, pltpu.HBM) for v in (hidden_in[0], attn_cotangent[0], tables)]
    attn, grad_in, weight_grad, gain_grad = whole(kept[0], tiles, gain_piece, kept[2], kept[1])
    attn, grad_in, weight_grad = written(attn, grad_in, weight_grad)
    return (attn[None], grad_in[None], weight_grad, gain_grad[0, :8])


def solution(mesh):
    return jax.shard_map(
        local,
        mesh=mesh,
        in_specs=(
            P("inter", "intra", None),
            P(("inter", "intra")),
            P(("inter", "intra"), None),
            P("inter", "intra", None),
        ),
        out_specs=(
            P("inter", "intra", None),
            P("inter", "intra", None),
            P(("intra", "inter"), None),
            P(("intra", "inter")),
        ),
        check_vma=False,
    )
```

```python
import jax
import jax.numpy as jnp
import numpy as np
from jax import lax
from jax.experimental import pallas as pl
from jax.experimental.pallas import tpu as pltpu
from jax.sharding import PartitionSpec as P

HD = 128
HEADS = 4
TILES = HEADS + 2
WIDTH = 4096
MESH = pl.DeviceIdType.MESH
SIZES = {"x": 4, "y": 8, "z": 8}
ORDERS = (
    (("z", "y", "x"), ("y", "z", "x")),
    (("z", "x", "y"), ("z", "x", "y")),
    (("y", "x", "z"), ("y", "x", "z")),
)
RINGS = ("x", "y", "z")
HALVES = 2
QUARTERS = 2
CHUNK = 256
CHUNKS = 1024 // CHUNK
BLOCKS = CHUNK // 128
FLAT = HEADS * 128

eps_norm = 1e-05
rope_base = 500000.0


def place():
    i, j = lax.axis_index("inter"), lax.axis_index("intra")
    return {"x": j // 2, "y": i // 8, "z": ((i // 2) % 4) * 2 + j % 2}, i % 2


def device(at, core):
    return ((at["y"] * 4 + at["z"] // 2) * 2 + core, at["x"] * 2 + at["z"] % 2)


def moved(at, dim, step):
    size = SIZES[dim]
    return {**at, dim: (at[dim] + step + size) % size}


def indices(at):
    every = slice(None)
    y, x = at.get("y", every), at.get("x", every)
    high, low = (at["z"] // 2, at["z"] % 2) if "z" in at else (every, every)
    return y, high, x, low


def slab(ref, tile, at, cores=slice(None)):
    y, high, x, low = indices(at)
    return ref.at[tile, y, high, cores, x, low]


def out_slab(ref, tile, at, cores=slice(None)):
    y, high, x, low = indices(at)
    return ref.at[tile, x, low, y, high, cores]


def shares(dim, q):
    if dim == "y":
        return slice(None), slice(q * 2, q * 2 + 2)
    return slice(q * 4, q * 4 + 4), slice(None)


def ring_slab(ref, tile, dim, where, h, q):
    y, high, x, low = indices({dim: where})
    cut_y, cut_high = shares(dim, q)
    y, high = (y, cut_high) if dim == "y" else (cut_y, high)
    return ref.at[tile, y, high, h, x, low]


def ring_out_slab(ref, tile, dim, where, h, q):
    y, high, x, low = indices({dim: where})
    cut_y, cut_high = shares(dim, q)
    y, high = (y, cut_high) if dim == "y" else (cut_y, high)
    return ref.at[tile, x, low, y, high, h]


def remote(src, dst, send, recv, peer):
    return pltpu.make_async_remote_copy(
        src_ref=src, dst_ref=dst, send_sem=send, recv_sem=recv, device_id=peer, device_id_type=MESH
    )


def across(left, right, left_dim, right_dim):
    return lax.dot_general(
        left, right, (((left_dim,), (right_dim,)), ((), ())), preferred_element_type=jnp.float32
    )


def steps_of(p, way):
    return SIZES[RINGS[p]] // 2 - way


def ring_sem(sems, p, way, step, h, q):
    return sems.at[7 * p - 4 * (p > 0) + way * (2 if p == 0 else 4) + step, h, q]


def tiles_of(core):
    return [4 + core, 2 * core, 2 * core + 1]


def settle(spare, count, sem):
    pltpu.make_async_copy(spare.at[pl.ds(0, count)], spare.at[pl.ds(0, count)], sem).wait()


def greet(at, core, barrier):
    i, j = lax.axis_index("inter"), lax.axis_index("intra")
    peers = [device(at, 1 - core)]
    for dim, size in SIZES.items():
        peers += [device(moved(at, dim, step), core) for step in range(1, size)]
        if dim != "x":
            peers += [device(moved(at, dim, step), 1 - core) for step in range(1, size)]
    peers += [(i, (j + step) % 8) for step in range(1, 8)]
    for peer in peers:
        pl.semaphore_signal(barrier, inc=1, device_id=peer, device_id_type=MESH)
    return len(peers)


class Gather:
    def __init__(self, at, core, mine_ref, gain_ref, full, gain_pair, gain_near, gain_far, spare, sems):
        self.at, self.core, self.partner = at, core, device(at, 1 - core)
        self.mine_ref, self.gain_ref, self.full = mine_ref, gain_ref, full
        self.pair, self.near, self.far = gain_pair, gain_near, gain_far
        (self.swap, self.one, self.two, self.item, self.side, self.ring_out, self.ring, self.passing, self.gains, self.own) = sems
        self.mine, self.theirs = tiles_of(core), tiles_of(1 - core)
        sign = 1 - 2 * core
        self.ways = (sign, -sign)
        self.spare = spare

    def go(self, copy):
        copy.start()

    def begin(self):
        at, core, full = self.at, self.core, self.full
        owns = []
        for p in range(3):
            self.go(
                remote(
                    self.mine_ref.at[self.theirs[p]],
                    slab(full, self.theirs[p], at, core),
                    self.swap.at[0],
                    self.swap.at[1],
                    self.partner,
                )
            )
            owns.append(
                pltpu.make_async_copy(self.mine_ref.at[self.mine[p]], slab(full, self.mine[p], at, core), self.own.at[p])
            )
        self.go(remote(self.gain_ref, self.pair, self.gains.at[0, 0], self.gains.at[1, 0], self.partner))
        for own in owns:
            own.start()
        for own in owns:
            own.wait()
        settle(self.spare, 3, self.swap.at[1])
        for p in (1, 2, 0):
            for h in range(HALVES):
                self.direct(p, h, 0)
        self.gain_wait(0, 1)
        self.near[0] = self.gain_ref[...] + self.pair[...]

    def direct(self, p, h, phase):
        order = ORDERS[p][h]
        sems = (self.one, self.two)[phase]
        src = slab(self.full, self.mine[p], {d: self.at[d] for d in order[phase:]}, h)
        for step in range(1, SIZES[order[phase]]):
            peer = device(moved(self.at, order[phase], step), self.core)
            recv = self.item.at[h, step - 1] if p == 0 and phase == 1 else sems.at[2 * p + h]
            self.go(remote(src, src, sems.at[6], recv, peer))

    def along(self, h, step):
        middle = ORDERS[0][h][1]
        if step:
            settle(self.spare, 8, self.item.at[h, step - 1])
        known = moved({d: self.at[d] for d in (middle, "x")}, middle, -step)
        src = slab(self.full, self.mine[0], known, h)
        for k in (2, 1, 3):
            peer = device(moved(self.at, "x", k), self.core)
            self.go(remote(src, src, self.ring_out.at[0], self.side.at[h, k - 1], peer))

    def beside(self, h):
        for k in (1, 3, 2):
            settle(self.spare, 64, self.side.at[h, k - 1])
            self.pass_on(0, h, moved(self.at, "x", -k)["x"])

    def arrived(self, p, h, phase):
        order = ORDERS[p][h]
        sems = (self.one, self.two)[phase]
        each = 1 if phase == 0 else SIZES[order[0]]
        settle(self.spare, (SIZES[order[phase]] - 1) * each, sems.at[2 * p + h])

    def gain_wait(self, phase, side):
        rows = (self.pair, self.near.at[pl.ds(0, 7)], self.far.at[0, pl.ds(0, 3)], self.far.at[pl.ds(0, 7)])[phase]
        pltpu.make_async_copy(rows, rows, self.gains.at[side, phase]).wait()

    def gain_group(self):
        i, j = lax.axis_index("inter"), lax.axis_index("intra")
        for step in range(1, 8):
            self.go(
                remote(
                    self.near.at[0], self.near.at[step], self.gains.at[0, 1], self.gains.at[1, 1], (i, (j + step) % 8)
                )
            )

    def gain_high(self):
        at = self.at
        self.gain_wait(1, 1)
        self.far[at["y"], at["z"] // 2] = sum(self.near[k] for k in range(8))
        here = self.far.at[at["y"], at["z"] // 2]
        for step in (1, 3, 2):
            peer = device(moved(at, "z", 2 * step), self.core)
            self.go(remote(here, here, self.gains.at[0, 2], self.gains.at[1, 2], peer))

    def gain_all(self):
        self.gain_wait(2, 1)
        here = self.far.at[self.at["y"]]
        for step in range(1, 8):
            peer = device(moved(self.at, "y", step), self.core)
            self.go(remote(here, here, self.gains.at[0, 3], self.gains.at[1, 3], peer))

    def settled(self):
        settle(self.spare, 3, self.swap.at[0])
        settle(self.spare, 42, self.one.at[6])
        settle(self.spare, 208, self.two.at[6])
        for p in range(3):
            settle(self.spare, 384 if RINGS[p] == "x" else 448, self.ring_out.at[p])
            settle(self.spare, 512, self.passing.at[0, p])
        for phase in range(4):
            self.gain_wait(phase, 0)

    def where(self, p, way, step):
        dim = RINGS[p]
        return moved(self.at, dim, -self.ways[way] * step)[dim]

    def hop(self, p, way, step, h, q):
        dim = RINGS[p]
        piece = ring_slab(self.full, self.mine[p], dim, self.where(p, way, step), h, q)
        peer = device(moved(self.at, dim, self.ways[way]), self.core)
        self.go(remote(piece, piece, self.ring_out.at[p], self.ring.at[7 * (p - 1) + 4 * way + step, h, q], peer))

    def pass_on(self, p, h, where):
        piece = slab(self.full, self.mine[p], {RINGS[p]: where}, h)
        self.go(remote(piece, piece, self.passing.at[0, p], self.passing.at[1, p], self.partner))

    def ring_start(self, p, h):
        for q in range(QUARTERS):
            for way in range(2):
                self.hop(p, way, 0, h, q)
        self.pass_on(p, h, self.at[RINGS[p]])

    def ring_step(self, p, h, step, q):
        dim = RINGS[p]
        for way in range(2):
            if step >= steps_of(p, way):
                continue
            piece = ring_slab(self.full, self.mine[p], dim, self.where(p, way, step + 1), h, q)
            remote(piece, piece, self.ring_out.at[p], self.ring.at[7 * (p - 1) + 4 * way + step, h, q], self.partner).wait_recv()
            if step + 1 < steps_of(p, way):
                self.hop(p, way, step + 1, h, q)
            if q == QUARTERS - 1:
                self.pass_on(p, h, self.where(p, way, step + 1))

    def passed(self, p):
        settle(self.spare, 512, self.passing.at[1, p])


RING_SHAPES = {"x": (2, 4, 4, 8, HD), "y": (4, 2, 2, 8, HD), "z": (4, 4, 8, HD)}
LINE_SHAPES = {"x": (4, 8, HD), "y": (8, 8, HD), "z": (2, 4, 8, HD)}


class Scatter:
    def __init__(self, at, core, part, rings, lines, dot_in, total_ref, spare, sems):
        self.at, self.core, self.partner = at, core, device(at, 1 - core)
        self.part, self.rings, self.lines, self.dot_in = part, rings, lines, dot_in
        self.total_ref = total_ref
        self.ring_out, self.ring, self.two, self.three, self.last = sems
        sign = 1 - 2 * core
        self.ways = (sign, -sign)
        self.spare = spare

    def go(self, copy):
        copy.start()

    def target(self, p, way, left):
        dim = RINGS[p]
        return moved(self.at, dim, self.ways[way] * left)[dim]

    def copy(self, p, way, step, h, q):
        dim = RINGS[p]
        return remote(
            ring_out_slab(self.part, p, dim, self.target(p, way, steps_of(p, way) - step), h, q),
            self.rings[p].at[way, step, h, q],
            self.ring_out.at[p],
            ring_sem(self.ring, p, way, step, h, q),
            device(moved(self.at, dim, self.ways[way]), self.core),
        )

    def ring_start(self, p):
        for h in range(HALVES):
            for q in range(QUARTERS):
                for way in range(2):
                    self.go(self.copy(p, way, 0, h, q))

    def ring_step(self, p, h, step, q):
        for way in range(2):
            if step >= steps_of(p, way):
                continue
            self.copy(p, way, step, h, q).wait_recv()
            dim = RINGS[p]
            here = ring_out_slab(self.part, p, dim, self.target(p, way, steps_of(p, way) - step - 1), h, q)
            there = self.rings[p].at[way, step, h, q]
            here[...] = (here[...].astype(jnp.float32) + there[...].astype(jnp.float32)).astype(jnp.bfloat16)
            if step + 1 < steps_of(p, way):
                self.go(self.copy(p, way, step + 1, h, q))

    def lines_out(self, p, h):
        a, b, c = ORDERS[p][h]
        for step in range(1, SIZES[b]):
            there = moved(self.at, b, step)
            self.go(
                remote(
                    out_slab(self.part, p, {b: there[b], c: self.at[c]}, h),
                    self.lines[2 * p + h].at[step - 1],
                    self.two.at[6],
                    self.two.at[2 * p + h],
                    device(there, self.core),
                )
            )

    def dots_out(self, p, h):
        a, b, c = ORDERS[p][h]
        lines = self.lines[2 * p + h]
        here = out_slab(self.part, p, {b: self.at[b], c: self.at[c]}, h)
        total = here[...].astype(jnp.float32)
        settle(self.spare, (SIZES[b] - 1) * SIZES[a], self.two.at[2 * p + h])
        for step in range(1, SIZES[b]):
            total = total + lines[step - 1].astype(jnp.float32)
        here[...] = total.astype(jnp.bfloat16)
        tile = tiles_of(self.core)[p]
        for step in range(1, SIZES[a]):
            there = moved(self.at, a, step)
            self.go(
                remote(
                    out_slab(self.part, p, there, h),
                    self.dot_in.at[tile, step - 1],
                    self.three.at[6],
                    self.three.at[tile],
                    device(there, h),
                )
            )
        own = out_slab(self.part, p, self.at, h)

        @pl.when(self.core == h)
        def _():
            self.dot_in[tile, 7] = own[...]

        @pl.when(self.core != h)
        def _():
            self.go(remote(own, self.dot_in.at[tile, 7], self.three.at[6], self.last.at[p], self.partner))

    def finish(self, p, mine):
        tile = tiles_of(self.core if mine else 1 - self.core)[p]
        settle(self.spare, 7, self.three.at[tile])
        if not mine:
            settle(self.spare, 1, self.last.at[p])
        self.total_ref[tile] = sum(self.dot_in[tile, k].astype(jnp.float32) for k in range(8))

    def settled(self):
        for p in range(3):
            settle(self.spare, 384 if RINGS[p] == "x" else 448, self.ring_out.at[p])
        settle(self.spare, 208, self.two.at[6])
        settle(self.spare, 45, self.three.at[6])


def whole_kernel(
    hidden_in, mine_ref, gain_ref, tables_in, cot_in,
    attn_ref, grad_in_ref, weight_grad_ref, gain_grad_ref,
    full, gain_pair, gain_near, gain_far, gain_row, normed, turned_own, turned_other,
    kv, probs, part_out, part_in, back, back_other, plain,
    part, ring_0, ring_1, ring_2, line_0, line_1, line_2, line_3, line_4, line_5, dot_in, total_ref, mixed, spare, hidden_ref, tables, cot_ref, load_sem,
    g_swap, g_one, g_two, g_item, g_side, g_out, g_ring, g_pass, g_gain, g_own,
    kv_sem, part_sem, swap_sem, s_out, s_ring, s_two, s_three, s_last,
):
    i, j = lax.axis_index("inter"), lax.axis_index("intra")
    at, core = place()
    partner = device(at, 1 - core)
    barrier = pltpu.get_barrier_semaphore()
    loads = [
        pltpu.make_async_copy(hidden_in, hidden_ref, load_sem.at[0]),
        pltpu.make_async_copy(cot_in, cot_ref, load_sem.at[1]),
        pltpu.make_async_copy(tables_in.at[j], tables, load_sem.at[2]),
    ]
    for load in loads:
        load.start()
    for block in range(8):
        kv[block] = jnp.zeros((2, 128, HD), jnp.bfloat16)
    count = greet(at, core, barrier)
    for load in loads:
        load.wait()
    squares = jnp.zeros((128, 128), jnp.float32)
    for t in range(WIDTH // 128):
        tile = hidden_ref[:, t * 128 : (t + 1) * 128].astype(jnp.float32)
        squares = squares + tile * tile
    inv_rms = lax.rsqrt(jnp.sum(squares, axis=1, keepdims=True) / WIDTH + eps_norm)
    cosine, sine = tables[0], tables[1]
    cots = [cot_ref[:, h * HD : (h + 1) * HD] for h in range(HEADS)]
    pl.semaphore_wait(barrier, count)

    g = Gather(
        at, core, mine_ref, gain_ref, full, gain_pair, gain_near, gain_far, spare,
        (g_swap, g_one, g_two, g_item, g_side, g_out, g_ring, g_pass, g_gain, g_own),
    )
    g.begin()
    g.gain_group()
    for p in (1, 2):
        for h in range(HALVES):
            g.arrived(p, h, 0)
            g.direct(p, h, 1)
    for h in range(HALVES):
        g.arrived(0, h, 0)
        g.direct(0, h, 1)
    for h in range(HALVES):
        g.along(h, 0)
    g.gain_high()

    def along(*steps):
        for step in steps:
            for h in range(HALVES):
                g.along(h, step)

    def begin_far(h):
        for p in (1, 2):
            g.arrived(p, h, 1)
            g.ring_start(p, h)

    def far(step):
        for h in range(HALVES):
            for q in range(QUARTERS):
                for p in (1, 2):
                    g.ring_step(p, h, step, q)

    begin_far(0)
    along(1, 7)
    begin_far(1)
    along(2, 6)
    g.gain_all()
    along(3, 5, 4)
    for h in range(HALVES):
        g.pass_on(0, h, at["x"])
    far(0)
    far(1)
    g.gain_wait(3, 1)
    for y in range(8):
        for z in range(4):
            t = y * 4 + z
            gain_row[:, t * 128 : (t + 1) * 128] = gain_far[y, z]
    for t in range(WIDTH // 128):
        cols = slice(t * 128, (t + 1) * 128)
        unit = hidden_ref[:, cols].astype(jnp.float32) * inv_rms * gain_row[:, cols]
        normed[:, cols] = unit.astype(jnp.bfloat16)
    g.beside(0)
    g.beside(1)

    def weight_rows(tiles, y):
        return jnp.concatenate([full[tile, y].reshape(512, HD) for tile in tiles], axis=1)

    def mix(tiles):
        total = jnp.zeros((128, len(tiles) * HD), jnp.float32)
        for y in range(8):
            total = total + across(normed[:, y * 512 : (y + 1) * 512], weight_rows(tiles, y), 1, 0)
        for k, tile in enumerate(tiles):
            mixed[tile] = total[:, k * HD : (k + 1) * HD]

    def rotated(x, sign):
        return x * cosine + sign * (pltpu.roll(x, 64, 1) * sine)

    mix(g.mine[:1])

    @pl.when(core == 1)
    def _():
        far(2)

    g.passed(0)
    mix(g.theirs[:1])
    kv[j, 0] = rotated(mixed[4], 1.0).astype(jnp.bfloat16)
    kv[j, 1] = mixed[5].astype(jnp.bfloat16)

    def kv_copy(owner, peer):
        return remote(kv.at[owner], kv.at[owner], kv_sem.at[0, peer], kv_sem.at[1, owner], (i, peer))

    for peer in range(7, 0, -1):
        @pl.when(j < peer)
        def _():
            kv_copy(j, peer).start()

    scale = HD ** (-0.5)

    @pl.when(core == 0)
    def _():
        far(2)

    far(3)
    for t in range(WIDTH // 128):
        cols = slice(t * 128, (t + 1) * 128)
        turned_own[cols, :] = normed[:, cols].T
    swap = remote(turned_own, turned_other, swap_sem.at[0, 0], swap_sem.at[1, 0], partner)
    swap.start()
    mix(g.mine[1:])
    g.passed(1)
    g.passed(2)
    mix(g.theirs[1:])
    queries = [(rotated(mixed[h], 1.0) * scale).astype(jnp.bfloat16) for h in range(HEADS)]
    query = jnp.concatenate(queries, axis=0)
    query_t = jnp.concatenate([q.T for q in queries], axis=1)
    cot = jnp.concatenate(cots, axis=0)
    cot_t = jnp.concatenate([c.T for c in cots], axis=1)
    row_pos = j * 128 + lax.broadcasted_iota(jnp.int32, (CHUNK, FLAT), 1) % 128
    key_pos = lax.broadcasted_iota(jnp.int32, (CHUNK, FLAT), 0)

    def allowed(chunk):
        return key_pos + chunk * CHUNK <= row_pos

    def rows(chunk, which):
        return jnp.concatenate([kv[chunk * BLOCKS + b, which] for b in range(BLOCKS)], axis=0)

    for owner in range(7):
        @pl.when(owner < j)
        def _():
            kv_copy(owner, j).wait_recv()

    top = jnp.full((1, FLAT), -1e30, jnp.float32)
    for chunk in range(CHUNKS):
        scores = jnp.where(allowed(chunk), across(rows(chunk, 0), query_t, 1, 0), -1e30)
        probs[chunk] = scores
        top = jnp.maximum(top, jnp.max(scores, axis=0, keepdims=True))
    total = jnp.zeros((1, FLAT), jnp.float32)
    out_t = jnp.zeros((HD, FLAT), jnp.float32)
    for chunk in range(CHUNKS):
        numbers = jnp.exp(probs[chunk] - top)
        probs[chunk] = numbers
        total = total + jnp.sum(numbers, axis=0, keepdims=True)
        out_t = out_t + across(rows(chunk, 1), numbers.astype(jnp.bfloat16), 0, 0)
    share = 1.0 / total
    attn_t = (out_t * share).astype(jnp.bfloat16)
    delta = jnp.sum(cot_t.astype(jnp.float32) * attn_t.astype(jnp.float32), axis=0, keepdims=True)
    query_grad_t = jnp.zeros((HD, FLAT), jnp.float32)

    def part_copy(owner, maker):
        return remote(part_out.at[owner], part_in.at[maker], part_sem.at[0, owner], part_sem.at[1, maker], (i, owner))

    def send_parts(chunk):
        for b in range(BLOCKS):
            owner = chunk * BLOCKS + b

            @pl.when(owner < j)
            def _():
                part_copy(owner, j).start()

    for chunk in range(CHUNKS):
        probs_t = probs[chunk] * share
        probs_grad = across(rows(chunk, 1), cot_t, 1, 0)
        scores_grad = (probs_t * (probs_grad - delta)).astype(jnp.bfloat16)
        keys_part = across(scores_grad, query, 1, 0).astype(jnp.bfloat16)
        values_part = across(probs_t.astype(jnp.bfloat16), cot, 1, 0).astype(jnp.bfloat16)
        for b in range(BLOCKS):
            part_out[chunk * BLOCKS + b, 0] = keys_part[b * 128 : (b + 1) * 128]
            part_out[chunk * BLOCKS + b, 1] = values_part[b * 128 : (b + 1) * 128]
        query_grad_t = query_grad_t + across(rows(chunk, 0), scores_grad, 0, 0)
        send_parts(chunk)
    for h in range(HEADS):
        grad = query_grad_t[:, h * 128 : (h + 1) * 128].T
        back[h] = (rotated(grad, -1.0) * scale).astype(jnp.bfloat16)

    def swap_back(first, count, slot):
        return remote(
            back.at[pl.ds(first, count)], back_other.at[pl.ds(slot, count)], swap_sem.at[0, 1 + slot],
            swap_sem.at[1, 1 + slot], partner,
        )

    swap_heads = swap_back(2 * (1 - core), 2, 0)
    swap_heads.start()
    for h in range(HEADS):
        attn_ref[:, h * HD : (h + 1) * HD] = attn_t[:, h * 128 : (h + 1) * 128].T
    swap.wait_recv()
    swap_heads.wait_recv()

    def products(ps):
        own = jnp.concatenate([back[g.mine[p]] for p in ps], axis=1)
        other = jnp.concatenate([back_other[(p + 2) % 3] for p in ps], axis=1)
        both = jnp.concatenate([own, other], axis=0)
        for k in range(8):
            chosen = slice(k * 512, (k + 1) * 512)
            left = jnp.concatenate([turned_own[chosen, :], turned_other[chosen, :]], axis=1)
            sums = across(left, both, 1, 0)
            for n, p in enumerate(ps):
                part[p, k // 2, k % 2] = sums[:, n * HD : (n + 1) * HD].reshape(8, 4, 2, 8, HD).astype(jnp.bfloat16)

    s = Scatter(
        at, core, part, (ring_0, ring_1, ring_2), (line_0, line_1, line_2, line_3, line_4, line_5), dot_in, total_ref, spare, (s_out, s_ring, s_two, s_three, s_last),
    )
    products((1, 2))
    s.ring_start(1)
    s.ring_start(2)
    pairs = [jnp.concatenate([back[2 * pair], back[2 * pair + 1]], axis=1) for pair in range(2)]
    for y in range(8):
        plain[:, y * 512 : (y + 1) * 512] = sum(
            across(pairs[pair], weight_rows((2 * pair, 2 * pair + 1), y), 1, 1) for pair in range(2)
        )
    part_in[j] = part_out[j]
    keys_grad = jnp.zeros((128, HD), jnp.float32)
    values_grad = jnp.zeros((128, HD), jnp.float32)
    for maker in range(8):
        @pl.when(maker > j)
        def _():
            part_copy(j, maker).wait_recv()

        @pl.when(maker < j)
        def _():
            part_in[maker] = jnp.zeros((2, 128, HD), jnp.bfloat16)

        keys_grad = keys_grad + part_in[maker, 0].astype(jnp.float32)
        values_grad = values_grad + part_in[maker, 1].astype(jnp.float32)
    back[4] = rotated(keys_grad, -1.0).astype(jnp.bfloat16)
    back[5] = values_grad.astype(jnp.bfloat16)

    def both(step, halves=(0, 1)):
        for h in halves:
            for q in range(QUARTERS):
                for p in (1, 2):
                    s.ring_step(p, h, step, q)

    swap_last = swap_back(5 - core, 1, 2)
    swap_last.start()
    last_pair = jnp.concatenate([back[4], back[5]], axis=1)
    both(0, (0,))
    swap_last.wait_recv()
    products((0,))
    s.ring_start(0)
    both(0, (1,))
    g.settled()

    def plain_rows(y, inner):
        cols = slice(y * 512, (y + 1) * 512)
        grad = plain[:, cols] + across(last_pair, weight_rows((4, 5), y), 1, 1)
        grad = grad * gain_row[:, cols]
        plain[:, cols] = grad
        return inner + jnp.sum(grad * hidden_ref[:, cols].astype(jnp.float32), axis=1, keepdims=True)

    inner = jnp.zeros((128, 1), jnp.float32)

    for y in range(8):
        inner = plain_rows(y, inner)
    both(1)
    fall = inv_rms * inv_rms * inv_rms * (1.0 / WIDTH) * inner
    for y in range(8):
        cols = slice(y * 512, (y + 1) * 512)
        grad_in_ref[:, cols] = (
            plain[:, cols] * inv_rms - hidden_ref[:, cols].astype(jnp.float32) * fall
        ).astype(jnp.bfloat16)
    def late(h, step):
        for q in range(QUARTERS):
            s.ring_step(0, h, step, q)

    late(0, 0)
    both(2)
    late(1, 0)
    late(0, 1)
    s.lines_out(0, 0)
    for h in range(HALVES):
        for q in range(QUARTERS):
            for p in (1, 2):
                s.ring_step(p, h, 3, q)
                if q == QUARTERS - 1:
                    s.lines_out(p, h)
    late(1, 1)
    s.lines_out(0, 1)
    for h in range(HALVES):
        for p in (1, 2):
            s.dots_out(p, h)
    for h in range(HALVES):
        s.dots_out(0, h)
    for p in (1, 2, 0):
        s.finish(p, True)
        s.finish(p, False)
    inside = (j, i // 16, (i // 8) % 2, (i // 2) % 4, i % 2)
    sums = jnp.zeros((8, HD), jnp.float32)
    for n in range(TILES):
        tile = total_ref[n]
        weight_grad_ref[:, n * HD : (n + 1) * HD] = tile
        sums = sums + tile * full[(n, *inside)].astype(jnp.float32)
    lane = lax.broadcasted_iota(jnp.int32, (8, 128), 1)
    row = lax.broadcasted_iota(jnp.int32, (8, 128), 0)
    gains = jnp.sum(jnp.where(lane == (i % 16) * 8 + row, gain_far[j, i // 16], 0.0), axis=1, keepdims=True)
    answer = jnp.sum(sums, axis=1, keepdims=True) / gains
    gain_grad_ref[...] = jnp.sum(jnp.where(lane == row, answer, 0.0), axis=0, keepdims=True)

    for peer in range(1, 8):
        @pl.when(j < peer)
        def _():
            kv_copy(j, peer).wait_send()

    for owner in range(7):
        @pl.when(owner < j)
        def _():
            part_copy(owner, j).wait_send()

    for copy in (swap, swap_heads, swap_last):
        copy.wait_send()
    s.settled()


def whole(hidden, tiles, gain_piece, tables, cot):
    dma = pltpu.SemaphoreType.DMA
    vmem = pl.BlockSpec(memory_space=pltpu.VMEM)
    hbm = pl.BlockSpec(memory_space=pltpu.HBM)
    low, wide = jnp.bfloat16, jnp.float32

    def rings(p):
        dim = RINGS[p]
        return pltpu.VMEM((2, SIZES[dim] // 2, HALVES, QUARTERS, *RING_SHAPES[dim]), low)

    def lines(p, h):
        return pltpu.VMEM((SIZES[ORDERS[p][h][1]] - 1, *LINE_SHAPES[ORDERS[p][h][0]]), low)

    return pl.pallas_call(
        whole_kernel,
        out_shape=(
            jax.ShapeDtypeStruct((128, FLAT), low),
            jax.ShapeDtypeStruct((128, WIDTH), low),
            jax.ShapeDtypeStruct((8, TILES * HD), wide),
            jax.ShapeDtypeStruct((1, 128), wide),
        ),
        in_specs=[hbm, vmem, vmem, hbm, hbm],
        out_specs=(vmem,) * 4,
        scratch_shapes=[
            pltpu.VMEM((TILES, 8, 4, 2, 4, 2, 8, HD), low),
            pltpu.VMEM((1, 128), wide),
            pltpu.VMEM((8, 1, 128), wide),
            pltpu.VMEM((8, 4, 1, 128), wide),
            pltpu.VMEM((1, WIDTH), wide),
            pltpu.VMEM((128, WIDTH), low),
            pltpu.VMEM((WIDTH, 128), low),
            pltpu.VMEM((WIDTH, 128), low),
            pltpu.VMEM((8, 2, 128, HD), low),
            pltpu.VMEM((CHUNKS, CHUNK, FLAT), wide),
            pltpu.VMEM((8, 2, 128, HD), low),
            pltpu.VMEM((8, 2, 128, HD), low),
            pltpu.VMEM((TILES, 128, HD), low),
            pltpu.VMEM((3, 128, HD), low),
            pltpu.VMEM((128, WIDTH), wide),
            pltpu.VMEM((3, 4, 2, 8, 4, 2, 8, HD), low),
            *[rings(p) for p in range(3)],
            *[lines(p, h) for p in range(3) for h in range(HALVES)],
            pltpu.VMEM((TILES, 8, 8, HD), low),
            pltpu.VMEM((TILES, 8, HD), wide),
            pltpu.VMEM((TILES, 128, HD), wide),
            pltpu.VMEM((512, 8, HD), low),
            pltpu.VMEM((128, WIDTH), low),
            pltpu.VMEM((2, 128, HD), wide),
            pltpu.VMEM((128, FLAT), low),
            dma((3,)),
            dma((2,)),
            dma((7,)),
            dma((7,)),
            dma((HALVES, 7)),
            dma((HALVES, 3)),
            dma((3,)),
            dma((14, HALVES, QUARTERS)),
            dma((2, 3)),
            dma((2, 4)),
            dma((4,)),
            dma((2, 8)),
            dma((2, 8)),
            dma((2, 4)),
            dma((3,)),
            dma((17, HALVES, QUARTERS)),
            dma((7,)),
            dma((7,)),
            dma((3,)),
        ],
        compiler_params=pltpu.CompilerParams(collective_id=0, has_side_effects=True, vmem_limit_bytes=40 * 2**20),
        name="whole",
    )(hidden, tiles, gain_piece, tables, cot)


def rope_tables():
    freqs = np.float32(rope_base) ** (-np.arange(HD // 2, dtype=np.float32) / np.float32(HD // 2))
    angles = (np.arange(1024, dtype=np.float32)[:, None] * freqs.astype(np.float32)[None, :]).astype(np.float64)
    cosine, sine = np.cos(angles), np.sin(angles)
    both = np.stack([np.concatenate([cosine, cosine], axis=1), np.concatenate([-sine, sine], axis=1)])
    return np.moveaxis(both.reshape(2, 8, 128, HD), 1, 0).astype(np.float32)


def write_kernel(*refs):
    sems = refs[-1]
    copies = [pltpu.make_async_copy(refs[k], refs[3 + k], sems.at[k]) for k in range(3)]
    for copy in copies:
        copy.start()
    for copy in copies:
        copy.wait()


def written(*arrays):
    return pl.pallas_call(
        write_kernel,
        out_shape=tuple(jax.ShapeDtypeStruct(a.shape, a.dtype) for a in arrays),
        in_specs=[pl.BlockSpec(memory_space=pltpu.VMEM)] * 3,
        out_specs=(pl.BlockSpec(memory_space=pltpu.HBM),) * 3,
        scratch_shapes=[pltpu.SemaphoreType.DMA((3,))],
        compiler_params=pltpu.CompilerParams(vmem_limit_bytes=16 * 2**20),
        name="written",
    )(*arrays)


def local(hidden_in, norm_gain, qkv_weight, attn_cotangent):
    i, j = lax.axis_index("inter"), lax.axis_index("intra")
    tiles = jnp.moveaxis(qkv_weight.reshape(8, TILES, HD), 1, 0)
    lane = jnp.arange(128)
    gain_piece = jnp.where(lane // 8 == (i * 8 + j) % 16, jnp.tile(norm_gain.astype(jnp.float32), 16), 0.0)[None]
    tables = jnp.asarray(rope_tables())
    kept = [pltpu.with_memory_space_constraint(v, pltpu.HBM) for v in (hidden_in[0], attn_cotangent[0], tables)]
    attn, grad_in, weight_grad, gain_grad = whole(kept[0], tiles, gain_piece, kept[2], kept[1])
    attn, grad_in, weight_grad = written(attn, grad_in, weight_grad)
    return (attn[None], grad_in[None], weight_grad, gain_grad[0, :8])


def solution(mesh):
    return jax.shard_map(
        local,
        mesh=mesh,
        in_specs=(
            P("inter", "intra", None),
            P(("inter", "intra")),
            P(("inter", "intra"), None),
            P("inter", "intra", None),
        ),
        out_specs=(
            P("inter", "intra", None),
            P("inter", "intra", None),
            P(("intra", "inter"), None),
            P(("intra", "inter")),
        ),
        check_vma=False,
    )
```
